128 devices in a mesh: sec: 2 (over z_lo), tile: 64 (over y, z_hi, x, core).
Axes of the slice: x: 4, y: 4, z: 4 (z_hi: 2, z_lo: 2; z = z_hi * 2 + z_lo), core: 2. Of those that a mesh axis runs over, the one named last changes fastest.
Arguments:
- atmosphere: bfloat16 [128, 360, 384], P(('sec', 'tile')), may hold values from -6 to 6
- ocean_state: bfloat16 [512, 1440, 128], P('tile', 'sec'), may hold values from -6 to 6
- land_mask: int32 [512, 1440], P('tile', 'sec'), may hold values 0 or 1
- crossing_bands: int32 [64, 4], P('tile'), may hold values from 0 to 127, as said below
- ocean_regrid: float32 [64, 4, 8, 1], P('tile'), may hold values from 0 to 1, as said below
- atmosphere_regrid: float32 [64, 4, 1, 8], P('tile'), may hold values from 0 to 1, as said below
- surface_read: bfloat16 [128], replicated, may hold values from -0.5 to 0.5
- surface_embed: float32 [384], replicated, may hold values from -4 to 4
- flux_read: bfloat16 [384, 8], replicated, may hold values from -0.3125 to 0.3125
- flux_embed: bfloat16 [8, 128], replicated, may hold values from -2 to 2
- legendre_forward: bfloat16 [128, 128, 128], P(('sec', 'tile')), may hold values from -0.5 to 0.5
- legendre_inverse: bfloat16 [128, 128, 128], P(('sec', 'tile')), may hold values from -0.5 to 0.5
- spectral_mix: bfloat16 [2, 384, 384], replicated, may hold values from -0.3125 to 0.3125
- conv_kernel: bfloat16 [2, 7, 7, 128], replicated, may hold values from -0.875 to 0.875
- norm_gain: float32 [2, 128], replicated, may hold values from 0.1 to 1.9
- expand_weight: bfloat16 [2, 128, 512], replicated, may hold values from -0.5 to 0.5
- project_weight: bfloat16 [2, 512, 128], replicated, may hold values from -0.25 to 0.25
- atmosphere_cotangent: bfloat16 [128, 360, 384], P(('sec', 'tile')), may hold values from -6 to 6
- ocean_cotangent: bfloat16 [512, 1440, 128], P('tile', 'sec'), may hold values from -6 to 6
Outputs:
- atmosphere_next: bfloat16 [128, 360, 384], P(('sec', 'tile'))
- ocean_next: bfloat16 [512, 1440, 128], P('tile', 'sec')
- atmosphere_grad: float32 [128, 360, 384], P(('sec', 'tile'))
- ocean_grad: float32 [512, 1440, 128], P('tile', 'sec')
The draws below stay inside these ranges and needn't reach their ends.
Inputs may be any that keep to these rules, and one draw needn't show every extreme that they name: `crossing_bands`: row j lists between 1 and 4 consecutive distinct atmosphere bands, then repeats its last band; some row lists 4. Its first band is j * 2 - 1, j * 2 or j * 2 + 1, raised to 0 or lowered as far as needed for the list to end at band 128 - 1 at most. `ocean_regrid`: zero in the repeated slots of crossing_bands; the entries of each ocean row sum to one. `atmosphere_regrid`: zero in the repeated slots of crossing_bands.
All inputs are finite; a program needn't handle non-finite values. No bound on the sum of `land_mask` on one device may be relied on, other than what follows from the above.
Results may differ from the reference program's by a relative error of at most 0.008.
Values may be sent and summed in bfloat16 or wider, within the bound.
A program may use at most 128 MiB of HBM per device.

```python
import jax
import jax.numpy as jnp
from jax import lax

C = 384
ALON = 360
MODES = 128
F = 8
OC = 128
OHID = 512
KS = 7
LAYERS = 2
PEERS = 4
ALAT_DEV = 1
OLAT_DEV = 8
BANDS = 128
GROUPS = 64
ALAT = 128
OLAT = 512
OLON = 1440


def crossing_layout(key):
    base = jax.random.fold_in(key, 17)
    count_key, step_key = jax.random.split(base)
    group_index = jnp.arange(GROUPS, dtype=jnp.int32)
    counts = jax.random.randint(count_key, (GROUPS,), 1, PEERS + 1).astype(jnp.int32)
    counts = jnp.where(group_index == GROUPS // 2, PEERS, counts)
    wiggle = jax.random.randint(step_key, (GROUPS,), -1, 2).astype(jnp.int32)
    first = group_index * (BANDS // GROUPS) + wiggle
    first = jnp.minimum(jnp.maximum(first, 0), BANDS - counts)
    slot = jnp.arange(PEERS, dtype=jnp.int32)
    listed = first[:, None] + jnp.minimum(slot[None, :], counts[:, None] - 1)
    valid = (slot[None, :] < counts[:, None]).astype(jnp.float32)
    return (listed.astype(jnp.int32), valid)


def positive_weights(key, shape):
    raw = jax.random.uniform(key, shape, jnp.float32, 0.2, 1.0)
    return raw


def draw_crossing_bands(key, part):
    return crossing_layout(key)[0]


def draw_ocean_regrid(key, part):
    listed, valid = crossing_layout(key)
    raw = positive_weights(jax.random.fold_in(key, 29), (GROUPS, PEERS, OLAT_DEV, ALAT_DEV))
    raw = raw * valid[:, :, None, None]
    return raw / jnp.sum(raw, axis=(1, 3), keepdims=True)


def draw_atmosphere_regrid(key, part):
    listed, valid = crossing_layout(key)
    raw = positive_weights(jax.random.fold_in(key, 31), (GROUPS, PEERS, ALAT_DEV, OLAT_DEV))
    return raw * valid[:, :, None, None] / OLAT_DEV


def touch_ends(array, own_key, smallest, largest):
    place = [jax.random.randint(jax.random.fold_in(own_key, axis), (), 0, length) for axis, length in enumerate(array.shape)]
    widest = array.shape.index(max(array.shape))
    beside = place[:widest] + [(place[widest] + 1) % array.shape[widest]] + place[widest + 1:]
    return array.at[tuple(place)].set(smallest).at[tuple(beside)].set(largest)


def shard_levels(rng, shape, cuts, least, high):
    def one(axis_at, shards_of):
        steps = jax.random.uniform(jax.random.fold_in(jax.random.fold_in(rng, 6), axis_at), (shards_of,), jnp.float32, least / len(cuts), high / len(cuts))
        return jnp.repeat(jnp.exp(steps), shape[axis_at] // shards_of).reshape((-1,) + (1,) * (len(shape) - axis_at - 1))

    loudness = one(*cuts[0])
    for cut in cuts[1:]:
        loudness = loudness * one(*cut)
    return loudness


def centred(stream_key, shape, deviation, limit, cuts=(), kind=jnp.bfloat16):
    entries = jax.random.normal(stream_key, shape, jnp.float32) * deviation
    if len(cuts) > 0:
        entries = shard_levels(stream_key, shape, cuts, -0.22, 0.18) * entries
    return jnp.clip(entries, min=-limit, max=limit).astype(kind)


def setup_inputs(seed: int = 0) -> dict:
    arg_keys = jax.random.split(jax.random.key(seed), 20)
    return {
        "atmosphere": centred(arg_keys[0], (ALAT, ALON, C), 1.0, 6.0, ((0, 128),)),
        "ocean_state": centred(arg_keys[1], (OLAT, OLON, OC), 1.0, 6.0, ((0, 64), (1, 2))),
        "land_mask": touch_ends((jax.random.randint(arg_keys[2], (OLAT, OLON), 0, 10) < 7).astype(jnp.int32), jax.random.fold_in(arg_keys[2], 1), 0, 1),
        "crossing_bands": draw_crossing_bands(jax.random.fold_in(arg_keys[19], 71), 0),
        "ocean_regrid": draw_ocean_regrid(jax.random.fold_in(arg_keys[19], 71), 0),
        "atmosphere_regrid": draw_atmosphere_regrid(jax.random.fold_in(arg_keys[19], 71), 0),
        "surface_read": centred(arg_keys[6], (OC,), OC ** -0.5, 0.5),
        "surface_embed": centred(arg_keys[7], (C,), 1.0, 4.0, (), jnp.float32),
        "flux_read": centred(arg_keys[8], (C, F), C ** -0.5, 0.3125),
        "flux_embed": centred(arg_keys[9], (F, OC), F ** -0.5, 2.0),
        "legendre_forward": centred(arg_keys[10], (MODES, ALAT, ALAT), ALAT ** -0.5, 0.5, ((0, 128),)),
        "legendre_inverse": centred(arg_keys[11], (MODES, ALAT, ALAT), ALAT ** -0.5, 0.5, ((0, 128),)),
        "spectral_mix": centred(arg_keys[12], (2, C, C), C ** -0.5, 0.3125),
        "conv_kernel": centred(arg_keys[13], (LAYERS, KS, KS, OC), (KS * KS) ** -0.5, 0.875),
        "norm_gain": jnp.clip(1.0 + 0.18 * jax.random.normal(arg_keys[14], (LAYERS, OC), jnp.float32), 0.1, 1.9),
        "expand_weight": centred(arg_keys[15], (LAYERS, OC, OHID), OC ** -0.5, 0.5),
        "project_weight": centred(arg_keys[16], (LAYERS, OHID, OC), OHID ** -0.5, 0.25),
        "atmosphere_cotangent": centred(arg_keys[17], (ALAT, ALON, C), 1.0, 6.0, ((0, 128),)),
        "ocean_cotangent": centred(arg_keys[18], (OLAT, OLON, OC), 1.0, 6.0, ((0, 64), (1, 2))),
    }


def wave_table(lon_count, mode_count):
    longitude = jnp.arange(lon_count, dtype=jnp.int32)
    wavenumber = jnp.arange(mode_count, dtype=jnp.int32)
    phase = (longitude[:, None] * wavenumber[None, :] % lon_count).astype(jnp.float32) * (2.0 * jnp.pi / lon_count)
    scaled = jnp.stack([jnp.cos(phase), -jnp.sin(phase)], axis=2) * jnp.sqrt(jnp.float32(2.0 / lon_count))
    return scaled.reshape(lon_count, 2 * mode_count).astype(jnp.bfloat16)

def depthwise(window, kernel):
    radius = kernel.shape[0] // 2
    height = window.shape[0] - 2 * radius
    extent = window.shape[1]
    wide = jnp.concatenate([window[:, extent - radius:], window, window[:, :radius]], axis=1).astype(jnp.float32)
    weights = kernel.astype(jnp.float32)
    total = jnp.zeros((height, extent, window.shape[2]), jnp.float32)
    for shift_row in range(kernel.shape[0]):
        for shift_col in range(kernel.shape[1]):
            total = total + wide[shift_row:shift_row + height, shift_col:shift_col + extent] * weights[shift_row, shift_col]
    return total

def cell_forward(hidden, gain, expand, project):
    center = hidden - lax.optimization_barrier(jnp.mean(hidden, axis=-1, keepdims=True))
    inverse_std = lax.rsqrt(lax.optimization_barrier(jnp.mean(center * center, axis=-1, keepdims=True)) + 1e-06)
    normed = (center * inverse_std * gain).astype(jnp.bfloat16)
    before = jnp.dot(normed, expand, preferred_element_type=jnp.float32)
    active = jax.nn.gelu(before).astype(jnp.bfloat16)
    return jnp.dot(active, project, preferred_element_type=jnp.float32)

def cell_backward(hidden, gain, expand, project, mask_value, cotangent):
    center = hidden - lax.optimization_barrier(jnp.mean(hidden, axis=-1, keepdims=True))
    inverse_std = lax.rsqrt(lax.optimization_barrier(jnp.mean(center * center, axis=-1, keepdims=True)) + 1e-06)
    unit = center * inverse_std
    normed = (unit * gain).astype(jnp.bfloat16)
    before = jnp.dot(normed, expand, preferred_element_type=jnp.float32)
    masked = (mask_value[:, :, None] * cotangent).astype(jnp.bfloat16)
    active_adjoint = jnp.dot(masked, project.T, preferred_element_type=jnp.float32)
    _, gelu_back = jax.vjp(jax.nn.gelu, before)
    before_adjoint = gelu_back(active_adjoint)[0].astype(jnp.bfloat16)
    normed_adjoint = jnp.dot(before_adjoint, expand.T, preferred_element_type=jnp.float32)
    scaled = normed_adjoint * gain
    result = inverse_std * (scaled - lax.optimization_barrier(jnp.mean(scaled, axis=-1, keepdims=True)) - unit * lax.optimization_barrier(jnp.mean(scaled * unit, axis=-1, keepdims=True)))
    return result.astype(jnp.bfloat16)

def ocean_matrix(bands_row, blocks, lat_count):
    lat_band = blocks.shape[2]
    index = bands_row[:, None] * lat_band + jnp.arange(lat_band, dtype=jnp.int32)[None, :]
    onehot = (index[:, :, None] == jnp.arange(lat_count, dtype=jnp.int32)[None, None, :]).astype(jnp.float32)
    return jnp.einsum('poi,pia->oa', blocks, onehot, precision=lax.Precision.HIGHEST)

def atmosphere_matrix(bands_row, blocks, lat_count):
    lat_band = blocks.shape[1]
    index = bands_row[:, None] * lat_band + jnp.arange(lat_band, dtype=jnp.int32)[None, :]
    onehot = (index[:, :, None] == jnp.arange(lat_count, dtype=jnp.int32)[None, None, :]).astype(jnp.float32)
    return jnp.einsum('pio,pia->ao', blocks, onehot, precision=lax.Precision.HIGHEST)

def mix_complex(coefficient, mix_real, mix_imag):
    real_part = coefficient[:, :, 0].astype(jnp.float32)
    imag_part = coefficient[:, :, 1].astype(jnp.float32)
    first = mix_real.astype(jnp.float32)
    second = mix_imag.astype(jnp.float32)
    out_real = jnp.einsum('lmc,cd->lmd', real_part, first) - jnp.einsum('lmc,cd->lmd', imag_part, second)
    out_imag = jnp.einsum('lmc,cd->lmd', imag_part, first) + jnp.einsum('lmc,cd->lmd', real_part, second)
    return jnp.stack([out_real, out_imag], axis=2).astype(jnp.bfloat16)

def spectral_block(spectrum, forward, inverse, mixing):
    lat_count, columns, channels = spectrum.shape
    split = spectrum.reshape(lat_count, columns // 2, 2, channels).astype(jnp.float32)
    coefficient = jnp.einsum('mla,amrc->lmrc', forward.astype(jnp.float32), split).astype(jnp.bfloat16)
    mixed = mix_complex(coefficient, mixing[0], mixing[1])
    returned = jnp.einsum('mal,lmrc->amrc', inverse.astype(jnp.float32), mixed.astype(jnp.float32)).astype(jnp.bfloat16)
    return returned.reshape(lat_count, columns, channels)

def spectral_adjoint(returned_adjoint, forward, inverse, mixing):
    lat_count, columns, channels = returned_adjoint.shape
    split = returned_adjoint.reshape(lat_count, columns // 2, 2, channels).astype(jnp.float32)
    mixed_adjoint = jnp.einsum('mal,amrc->lmrc', inverse.astype(jnp.float32), split).astype(jnp.bfloat16)
    real_part = mixed_adjoint[:, :, 0].astype(jnp.float32)
    imag_part = mixed_adjoint[:, :, 1].astype(jnp.float32)
    first = mixing[0].astype(jnp.float32)
    second = mixing[1].astype(jnp.float32)
    back_real = jnp.einsum('lmd,cd->lmc', real_part, first) + jnp.einsum('lmd,cd->lmc', imag_part, second)
    back_imag = jnp.einsum('lmd,cd->lmc', imag_part, first) - jnp.einsum('lmd,cd->lmc', real_part, second)
    coefficient_adjoint = jnp.stack([back_real, back_imag], axis=2).astype(jnp.bfloat16)
    spectrum_adjoint = jnp.einsum('mla,lmrc->amrc', forward.astype(jnp.float32), coefficient_adjoint.astype(jnp.float32)).astype(jnp.bfloat16)
    return spectrum_adjoint.reshape(lat_count, columns, channels)

def ocean_layer(state, mask_value, kernel, gain, expand, project, band):
    radius = kernel.shape[0] // 2
    padded = jnp.pad(state, ((radius, radius), (0, 0), (0, 0)))
    band_count = state.shape[0] // band

    def one_band(index):
        start = index * band
        window = lax.dynamic_slice_in_dim(padded, start, band + 2 * radius, 0)
        update = cell_forward(depthwise(window, kernel), gain, expand, project)
        own = lax.dynamic_slice_in_dim(state, start, band, 0).astype(jnp.float32)
        weight = lax.dynamic_slice_in_dim(mask_value, start, band, 0)
        return (own + weight[:, :, None] * update).astype(jnp.bfloat16)
    result = lax.map(one_band, jnp.arange(band_count, dtype=jnp.int32))
    return result.reshape(state.shape)

def ocean_layer_adjoint(state, mask_value, kernel, gain, expand, project, cotangent, band):
    radius = kernel.shape[0] // 2
    padded = jnp.pad(state, ((radius, radius), (0, 0), (0, 0)))
    band_count = state.shape[0] // band

    def local_adjoint(index):
        start = index * band
        window = lax.dynamic_slice_in_dim(padded, start, band + 2 * radius, 0)
        hidden = depthwise(window, kernel)
        local_cotangent = lax.dynamic_slice_in_dim(cotangent, start, band, 0)
        weight = lax.dynamic_slice_in_dim(mask_value, start, band, 0)
        return cell_backward(hidden, gain, expand, project, weight, local_cotangent)
    hidden_adjoint = lax.map(local_adjoint, jnp.arange(band_count, dtype=jnp.int32)).reshape(state.shape)
    padded_adjoint = jnp.pad(hidden_adjoint, ((radius, radius), (0, 0), (0, 0)))
    flipped = kernel[::-1, ::-1]

    def spread(index):
        start = index * band
        window = lax.dynamic_slice_in_dim(padded_adjoint, start, band + 2 * radius, 0)
        return depthwise(window, flipped)
    spreads = lax.map(spread, jnp.arange(band_count, dtype=jnp.int32)).reshape(state.shape)
    return cotangent + spreads

def reference(atmosphere, ocean_state, land_mask, crossing_bands, ocean_regrid, atmosphere_regrid, surface_read, surface_embed, flux_read, flux_embed, legendre_forward, legendre_inverse, spectral_mix, conv_kernel, norm_gain, expand_weight, project_weight, atmosphere_cotangent, ocean_cotangent):
    group_total = crossing_bands.shape[0]
    lat_count, lon_count, channels = atmosphere.shape
    ocean_rows, ocean_lon, ocean_channels = ocean_state.shape
    band = ocean_rows // group_total
    ratio = ocean_lon // lon_count
    flux_count = flux_read.shape[1]
    highest = lax.Precision.HIGHEST
    to_ocean = jax.vmap(lambda row, blocks: ocean_matrix(row, blocks, lat_count))(crossing_bands, ocean_regrid)
    to_ocean = to_ocean.reshape(ocean_rows, lat_count)
    to_atmosphere = jax.vmap(lambda row, blocks: atmosphere_matrix(row, blocks, lat_count))(crossing_bands, atmosphere_regrid)
    to_atmosphere = jnp.transpose(to_atmosphere, (1, 0, 2)).reshape(lat_count, ocean_rows)
    mask_value = land_mask.astype(jnp.float32)
    surface = jnp.dot(ocean_state, surface_read, preferred_element_type=jnp.float32)
    coarse = lax.optimization_barrier(jnp.mean((mask_value * surface).reshape(ocean_rows, lon_count, ratio), axis=2))
    surface_atmosphere = jnp.dot(to_atmosphere, coarse, precision=highest)
    mixed_input = (atmosphere.astype(jnp.float32) + surface_atmosphere[:, :, None] * surface_embed[None, None, :]).astype(jnp.bfloat16)
    table = wave_table(lon_count, legendre_forward.shape[0]).astype(jnp.float32)
    spectrum = jnp.einsum('gk,agc->akc', table, mixed_input.astype(jnp.float32)).astype(jnp.bfloat16)
    returned = spectral_block(spectrum, legendre_forward, legendre_inverse, spectral_mix)
    response = jnp.einsum('gk,akc->agc', table, returned.astype(jnp.float32))
    atmosphere_next = (mixed_input.astype(jnp.float32) + jax.nn.gelu(response)).astype(jnp.bfloat16)
    flux = jnp.einsum('agc,cf->agf', atmosphere.astype(jnp.float32), flux_read.astype(jnp.float32))
    flux_ocean = jnp.dot(to_ocean, flux.reshape(lat_count, lon_count * flux_count), precision=highest)
    forcing_coarse = jnp.einsum('ogf,fc->ogc', flux_ocean.reshape(ocean_rows, lon_count, flux_count), flux_embed.astype(jnp.float32), precision=highest)
    forcing = jnp.broadcast_to(forcing_coarse[:, :, None, :], (ocean_rows, lon_count, ratio, ocean_channels)).reshape(ocean_rows, ocean_lon, ocean_channels)
    state = (ocean_state.astype(jnp.float32) + mask_value[:, :, None] * forcing).astype(jnp.bfloat16)
    states = []
    for layer in range(conv_kernel.shape[0]):
        states.append(state)
        state = ocean_layer(state, mask_value, conv_kernel[layer], norm_gain[layer], expand_weight[layer], project_weight[layer], band)
    ocean_next = state
    cotangent = ocean_cotangent.astype(jnp.float32)
    for layer in range(conv_kernel.shape[0] - 1, -1, -1):
        cotangent = ocean_layer_adjoint(states[layer], mask_value, conv_kernel[layer], norm_gain[layer], expand_weight[layer], project_weight[layer], cotangent, band)
    forcing_adjoint = (mask_value[:, :, None] * cotangent).reshape(ocean_rows, lon_count, ratio, ocean_channels).sum(axis=2)
    flux_ocean_adjoint = jnp.einsum('ogc,fc->ogf', forcing_adjoint, flux_embed.astype(jnp.float32), precision=highest)
    flux_adjoint = jnp.dot(to_ocean.T, flux_ocean_adjoint.reshape(ocean_rows, lon_count * flux_count), precision=highest)
    flux_adjoint = flux_adjoint.reshape(lat_count, lon_count, flux_count)
    from_flux = jnp.einsum('agf,cf->agc', flux_adjoint, flux_read.astype(jnp.float32), precision=highest)
    atmosphere_adjoint = atmosphere_cotangent.astype(jnp.float32)
    _, gelu_back = jax.vjp(jax.nn.gelu, response)
    response_adjoint = gelu_back(atmosphere_adjoint)[0].astype(jnp.bfloat16)
    returned_adjoint = jnp.einsum('gk,agc->akc', table, response_adjoint.astype(jnp.float32)).astype(jnp.bfloat16)
    spectrum_adjoint = spectral_adjoint(returned_adjoint, legendre_forward, legendre_inverse, spectral_mix)
    input_adjoint = atmosphere_adjoint + jnp.einsum('gk,akc->agc', table, spectrum_adjoint.astype(jnp.float32))
    atmosphere_grad = input_adjoint + from_flux
    surface_adjoint = jnp.einsum('agc,c->ag', input_adjoint, surface_embed, precision=highest)
    coarse_adjoint = jnp.dot(to_atmosphere.T, surface_adjoint, precision=highest)
    widened = jnp.broadcast_to(coarse_adjoint[:, :, None], (ocean_rows, lon_count, ratio)).reshape(ocean_rows, ocean_lon)
    surface_grad = mask_value * widened / ratio
    ocean_grad = cotangent + surface_grad[:, :, None] * surface_read.astype(jnp.float32)[None, None, :]
    return (atmosphere_next, ocean_next, atmosphere_grad, ocean_grad)
```

```python
import jax
import jax.numpy as jnp
from jax import lax
from jax.experimental import pallas as pl
from jax.experimental.pallas import tpu as pltpu
from jax.sharding import PartitionSpec as P

SEC_TILE = ("sec", "tile")
TILE = "tile"
LOGICAL = pl.DeviceIdType.LOGICAL
DEVICES = 128
GROUPS = 64
SLOTS = 8
LANES = 256


def remote(src, dst, send_sem, recv_sem, device):
    return pltpu.make_async_remote_copy(
        src_ref=src,
        dst_ref=dst,
        send_sem=send_sem,
        recv_sem=recv_sem,
        device_id=device,
        device_id_type=LOGICAL,
    )


def all_to_all_kernel(x_ref, o_ref, landed, send_sem, recv_sem):
    me = lax.axis_index("sec") * GROUPS + lax.axis_index("tile")
    barrier = pltpu.get_barrier_semaphore()

    def greet(i, carry):
        pl.semaphore_signal(
            barrier, inc=1, device_id=(me + i) % DEVICES, device_id_type=LOGICAL
        )
        return carry

    lax.fori_loop(1, DEVICES, greet, 0)
    pl.semaphore_wait(barrier, DEVICES - 1)

    def send(i, carry):
        peer = (me + i) % DEVICES
        remote(x_ref.at[peer], landed.at[me], send_sem, recv_sem, peer).start()
        return carry

    lax.fori_loop(1, DEVICES, send, 0)
    landed[me] = x_ref[me]
    every = landed.at[pl.ds(0, DEVICES - 1)]
    pltpu.make_async_copy(every, every, recv_sem).wait()
    pltpu.make_async_copy(every, every, send_sem).wait()
    o_ref[...] = landed[...]


def all_to_all(blocks, number):
    return pl.pallas_call(
        all_to_all_kernel,
        out_shape=jax.ShapeDtypeStruct(blocks.shape, blocks.dtype),
        in_specs=[pl.BlockSpec(memory_space=pltpu.VMEM)],
        out_specs=pl.BlockSpec(memory_space=pltpu.VMEM),
        scratch_shapes=[
            pltpu.VMEM(blocks.shape, blocks.dtype),
            pltpu.SemaphoreType.DMA,
            pltpu.SemaphoreType.DMA,
        ],
        compiler_params=pltpu.CompilerParams(collective_id=number, has_side_effects=True),
        name=f"exchange_{number}",
    )(blocks)


def regrid_kernel(
    rows_ref, parts_ref, gathered_ref, summed_ref, rows_in, parts_in, sems
):
    sec = lax.axis_index("sec")
    group = lax.axis_index("tile")
    me = sec * GROUPS + group
    barrier = pltpu.get_barrier_semaphore()

    def group_device(k):
        return (k % 2) * GROUPS + (me // 2 + 1 - k // 2 + GROUPS) % GROUPS

    def band_device(slot):
        return (2 * group - 2 + slot + DEVICES) % DEVICES

    mine = me * 0
    for k in range(SLOTS):
        for peer in (group_device(k), band_device(k)):
            mine = mine + jnp.where(peer == me, 1, 0)

            @pl.when(peer != me)
            def _():
                pl.semaphore_signal(barrier, inc=1, device_id=peer, device_id_type=LOGICAL)

    pl.semaphore_wait(barrier, 2 * SLOTS - mine)

    for k in range(SLOTS):
        target = group_device(k)
        slot = me % 2 + 2 * (k // 2)

        @pl.when(target != me)
        def _():
            remote(
                rows_ref.at[k % 2], rows_in.at[slot], sems.at[0, k], sems.at[1, slot], target
            ).start()

        @pl.when(target == me)
        def _():
            rows_in[slot] = rows_ref[k % 2]

        band = band_device(k)
        place = (k // 2) * 2 + sec

        @pl.when(band != me)
        def _():
            remote(
                parts_ref.at[k], parts_in.at[place], sems.at[2, k], sems.at[3, place], band
            ).start()

        @pl.when(band == me)
        def _():
            parts_in[place] = parts_ref[k]

    for k in range(SLOTS):

        @pl.when(band_device(k) != me)
        def _():
            remote(rows_ref.at[0], rows_in.at[k], sems.at[0, k], sems.at[1, k], me).wait_recv()
            remote(parts_ref.at[k], parts_in.at[k], sems.at[2, k], sems.at[3, k], me).wait_send()

        @pl.when(group_device(k) != me)
        def _():
            remote(rows_ref.at[0], rows_in.at[k], sems.at[0, k], sems.at[1, k], me).wait_send()
            remote(parts_ref.at[k], parts_in.at[k], sems.at[2, k], sems.at[3, k], me).wait_recv()

    gathered_ref[...] = rows_in[...]
    for half in range(2):
        total = parts_in[half]
        for k in range(1, 4):
            total = total + parts_in[2 * k + half]
        summed_ref[half] = total


def regrid(rows, parts, number):
    _, r, lanes = rows.shape
    _, q, _ = parts.shape
    vmem = pl.BlockSpec(memory_space=pltpu.VMEM)
    return pl.pallas_call(
        regrid_kernel,
        out_shape=(
            jax.ShapeDtypeStruct((SLOTS, r, lanes), jnp.float32),
            jax.ShapeDtypeStruct((2, q, lanes), jnp.float32),
        ),
        in_specs=[vmem, vmem],
        out_specs=(vmem, vmem),
        scratch_shapes=[
            pltpu.VMEM((SLOTS, r, lanes), jnp.float32),
            pltpu.VMEM((SLOTS, q, lanes), jnp.float32),
            pltpu.SemaphoreType.DMA((4, SLOTS)),
        ],
        compiler_params=pltpu.CompilerParams(collective_id=number, has_side_effects=True),
        name=f"regrid_{number}",
    )(rows, parts)


def slot_weights(bands_row, blocks, group):
    slot = bands_row[:, None] - (2 * group - 2)
    onehot = (slot == jnp.arange(SLOTS, dtype=jnp.int32)[None, :]).astype(jnp.float32)
    return jnp.sum(onehot[:, :, None] * blocks[:, None, :], axis=0)


def padded_lanes(values):
    return jnp.pad(values, [(0, 0)] * (values.ndim - 1) + [(0, LANES - values.shape[-1])])


def with_halo(x, sides, width, wrap):
    for axis, dim in sides:
        size, length = (lax.axis_size(axis), x.shape[dim])
        up = [(i, (i + 1) % size) for i in range(size if wrap else size - 1)]
        down = [(j, i) for i, j in up]
        last = lax.slice_in_dim(x, length - width, length, axis=dim)
        first = lax.slice_in_dim(x, 0, width, axis=dim)
        before = lax.ppermute(last, axis, up)
        after = lax.ppermute(first, axis, down)
        x = jnp.concatenate([before, x, after], axis=dim)
    return x


def wave_table(lon_count, mode_count):
    longitude = jnp.arange(lon_count, dtype=jnp.int32)
    wavenumber = jnp.arange(mode_count, dtype=jnp.int32)
    phase = (longitude[:, None] * wavenumber[None, :] % lon_count).astype(jnp.float32) * (
        2.0 * jnp.pi / lon_count
    )
    scaled = jnp.stack([jnp.cos(phase), -jnp.sin(phase)], axis=2) * jnp.sqrt(
        jnp.float32(2.0 / lon_count)
    )
    return scaled.reshape(lon_count, 2 * mode_count).astype(jnp.bfloat16)


def depthwise(window, kernel):
    radius = kernel.shape[0] // 2
    height = window.shape[0] - 2 * radius
    extent = window.shape[1] - 2 * radius
    wide = window.astype(jnp.float32)
    weights = kernel.astype(jnp.float32)
    total = jnp.zeros((height, extent, window.shape[2]), jnp.float32)
    for shift_row in range(kernel.shape[0]):
        for shift_col in range(kernel.shape[1]):
            total = (
                total
                + wide[shift_row : shift_row + height, shift_col : shift_col + extent]
                * weights[shift_row, shift_col]
            )
    return total


def cell_forward(hidden, gain, expand, project):
    center = hidden - jnp.mean(hidden, axis=-1, keepdims=True)
    inverse_std = lax.rsqrt(jnp.mean(center * center, axis=-1, keepdims=True) + 1e-06)
    normed = (center * inverse_std * gain).astype(jnp.bfloat16)
    before = jnp.dot(normed, expand, preferred_element_type=jnp.float32)
    active = jax.nn.gelu(before).astype(jnp.bfloat16)
    return jnp.dot(active, project, preferred_element_type=jnp.float32)


def cell_backward(hidden, gain, expand, project, mask_value, cotangent):
    center = hidden - jnp.mean(hidden, axis=-1, keepdims=True)
    inverse_std = lax.rsqrt(jnp.mean(center * center, axis=-1, keepdims=True) + 1e-06)
    unit = center * inverse_std
    normed = (unit * gain).astype(jnp.bfloat16)
    before = jnp.dot(normed, expand, preferred_element_type=jnp.float32)
    masked = (mask_value[:, :, None] * cotangent).astype(jnp.bfloat16)
    active_adjoint = jnp.dot(masked, project.T, preferred_element_type=jnp.float32)
    _, gelu_back = jax.vjp(jax.nn.gelu, before)
    before_adjoint = gelu_back(active_adjoint)[0].astype(jnp.bfloat16)
    normed_adjoint = jnp.dot(before_adjoint, expand.T, preferred_element_type=jnp.float32)
    scaled = normed_adjoint * gain
    result = inverse_std * (
        scaled
        - jnp.mean(scaled, axis=-1, keepdims=True)
        - unit * jnp.mean(scaled * unit, axis=-1, keepdims=True)
    )
    return result.astype(jnp.bfloat16)


def mix_complex(coefficient, mix_real, mix_imag):
    real_part = coefficient[:, :, 0]
    imag_part = coefficient[:, :, 1]
    out_real = jnp.einsum(
        "lmc,cd->lmd", real_part, mix_real, preferred_element_type=jnp.float32
    ) - jnp.einsum("lmc,cd->lmd", imag_part, mix_imag, preferred_element_type=jnp.float32)
    out_imag = jnp.einsum(
        "lmc,cd->lmd", imag_part, mix_real, preferred_element_type=jnp.float32
    ) + jnp.einsum("lmc,cd->lmd", real_part, mix_imag, preferred_element_type=jnp.float32)
    return jnp.stack([out_real, out_imag], axis=2).astype(jnp.bfloat16)


def spectral_block(spectrum, forward, inverse, mixing):
    lat_count, columns, channels = spectrum.shape
    split = spectrum.reshape(lat_count, columns // 2, 2, channels)
    coefficient = jnp.einsum(
        "mla,amrc->lmrc", forward, split, preferred_element_type=jnp.float32
    ).astype(jnp.bfloat16)
    mixed = mix_complex(coefficient, mixing[0], mixing[1])
    returned = jnp.einsum(
        "mal,lmrc->amrc", inverse, mixed, preferred_element_type=jnp.float32
    ).astype(jnp.bfloat16)
    return returned.reshape(lat_count, columns, channels)


def spectral_adjoint(returned_adjoint, forward, inverse, mixing):
    lat_count, columns, channels = returned_adjoint.shape
    split = returned_adjoint.reshape(lat_count, columns // 2, 2, channels)
    mixed_adjoint = jnp.einsum(
        "mal,amrc->lmrc", inverse, split, preferred_element_type=jnp.float32
    ).astype(jnp.bfloat16)
    real_part = mixed_adjoint[:, :, 0]
    imag_part = mixed_adjoint[:, :, 1]
    back_real = jnp.einsum(
        "lmd,cd->lmc", real_part, mixing[0], preferred_element_type=jnp.float32
    ) + jnp.einsum("lmd,cd->lmc", imag_part, mixing[1], preferred_element_type=jnp.float32)
    back_imag = jnp.einsum(
        "lmd,cd->lmc", imag_part, mixing[0], preferred_element_type=jnp.float32
    ) - jnp.einsum("lmd,cd->lmc", real_part, mixing[1], preferred_element_type=jnp.float32)
    coefficient_adjoint = jnp.stack([back_real, back_imag], axis=2).astype(jnp.bfloat16)
    spectrum_adjoint = jnp.einsum(
        "mla,lmrc->amrc", forward, coefficient_adjoint, preferred_element_type=jnp.float32
    ).astype(jnp.bfloat16)
    return spectrum_adjoint.reshape(lat_count, columns, channels)


def rims(values, width):
    with_rows = with_halo(values, ((TILE, 0),), width, False)
    return with_halo(with_rows, (("sec", 1),), width, True)


def per_device(
    atmosphere,
    ocean_state,
    land_mask,
    crossing_bands,
    ocean_regrid,
    atmosphere_regrid,
    surface_read,
    surface_embed,
    flux_read,
    flux_embed,
    legendre_forward,
    legendre_inverse,
    spectral_mix,
    conv_kernel,
    norm_gain,
    expand_weight,
    project_weight,
    atmosphere_cotangent,
    ocean_cotangent,
):
    band_total = lax.axis_size(SEC_TILE)
    lat_rows, lon_count, channels = atmosphere.shape
    ocean_rows, ocean_lon, ocean_channels = ocean_state.shape
    half = lon_count // lax.axis_size("sec")
    offset = lax.axis_index("sec") * half
    ratio = ocean_lon // half
    flux_count = flux_read.shape[1]
    radius = conv_kernel.shape[1] // 2
    layer_count = conv_kernel.shape[0]
    highest = lax.Precision.HIGHEST
    mask_value = land_mask.astype(jnp.float32)
    group = lax.axis_index("tile")
    to_ocean = slot_weights(crossing_bands[0], ocean_regrid[0, :, :, 0], group)
    to_atmosphere = slot_weights(crossing_bands[0], atmosphere_regrid[0, :, 0, :], group)
    surface = jnp.dot(ocean_state, surface_read, preferred_element_type=jnp.float32)
    coarse = jnp.mean((mask_value * surface).reshape(ocean_rows, half, ratio), axis=2)
    flux = jnp.einsum(
        "hgc,cf->hfg",
        atmosphere.reshape(2, half, channels),
        flux_read,
        preferred_element_type=jnp.float32,
    )
    flux_rows, surface_rows = regrid(
        padded_lanes(flux),
        padded_lanes(jnp.dot(to_atmosphere, coarse, precision=highest))[:, None, :],
        0,
    )
    surface_atmosphere = surface_rows[:, 0, :half].reshape(1, lon_count)
    flux_ocean = jnp.einsum("so,sfg->ogf", to_ocean, flux_rows[:, :, :half], precision=highest)
    mixed_input = (
        atmosphere.astype(jnp.float32)
        + surface_atmosphere[:, :, None] * surface_embed[None, None, :]
    ).astype(jnp.bfloat16)
    table = wave_table(lon_count, legendre_forward.shape[0] * band_total)
    spectrum = jnp.einsum(
        "gk,agc->akc", table, mixed_input, preferred_element_type=jnp.float32
    ).astype(jnp.bfloat16)
    modes = legendre_forward.shape[0] * band_total
    at_modes = all_to_all(spectrum.reshape(modes, 2, channels), 1)
    returned = spectral_block(at_modes, legendre_forward, legendre_inverse, spectral_mix)
    returned = all_to_all(returned, 2).reshape(1, 2 * modes, channels)
    response = jnp.einsum("gk,akc->agc", table, returned, preferred_element_type=jnp.float32)
    atmosphere_next = (mixed_input.astype(jnp.float32) + jax.nn.gelu(response)).astype(jnp.bfloat16)
    forcing_coarse = jnp.einsum(
        "ogf,fc->ogc",
        flux_ocean,
        flux_embed.astype(jnp.float32),
        precision=highest,
    )
    forcing = jnp.broadcast_to(
        forcing_coarse[:, :, None, :], (ocean_rows, half, ratio, ocean_channels)
    ).reshape(ocean_rows, ocean_lon, ocean_channels)
    state = (ocean_state.astype(jnp.float32) + mask_value[:, :, None] * forcing).astype(
        jnp.bfloat16
    )
    windows = []
    for layer in range(layer_count):
        window = rims(state, radius)
        windows.append(window)
        update = cell_forward(
            depthwise(window, conv_kernel[layer]),
            norm_gain[layer],
            expand_weight[layer],
            project_weight[layer],
        )
        state = (state.astype(jnp.float32) + mask_value[:, :, None] * update).astype(jnp.bfloat16)
    cotangent = ocean_cotangent.astype(jnp.float32)
    for layer in range(layer_count - 1, -1, -1):
        hidden = depthwise(windows[layer], conv_kernel[layer])
        hidden_adjoint = cell_backward(
            hidden,
            norm_gain[layer],
            expand_weight[layer],
            project_weight[layer],
            mask_value,
            cotangent,
        )
        cotangent = cotangent + depthwise(
            rims(hidden_adjoint, radius), conv_kernel[layer, ::-1, ::-1]
        )
    forcing_adjoint = (
        (mask_value[:, :, None] * cotangent)
        .reshape(ocean_rows, half, ratio, ocean_channels)
        .sum(axis=2)
    )
    flux_ocean_adjoint = jnp.einsum(
        "ogc,fc->ofg", forcing_adjoint, flux_embed.astype(jnp.float32), precision=highest
    )
    atmosphere_adjoint = atmosphere_cotangent.astype(jnp.float32)
    _, gelu_back = jax.vjp(jax.nn.gelu, response)
    response_adjoint = gelu_back(atmosphere_adjoint)[0].astype(jnp.bfloat16)
    returned_adjoint = jnp.einsum(
        "gk,agc->akc", table, response_adjoint, preferred_element_type=jnp.float32
    ).astype(jnp.bfloat16)
    at_modes_adjoint = all_to_all(returned_adjoint.reshape(modes, 2, channels), 3)
    spectrum_adjoint = spectral_adjoint(
        at_modes_adjoint, legendre_forward, legendre_inverse, spectral_mix
    )
    spectrum_adjoint = all_to_all(spectrum_adjoint, 4).reshape(1, 2 * modes, channels)
    input_adjoint = atmosphere_adjoint + jnp.einsum(
        "gk,akc->agc", table, spectrum_adjoint, preferred_element_type=jnp.float32
    )
    surface_adjoint = jnp.einsum("agc,c->ag", input_adjoint, surface_embed, precision=highest)
    parts = jnp.einsum("so,ofg->sfg", to_ocean, flux_ocean_adjoint, precision=highest)
    surface_rows_adjoint, flux_adjoint = regrid(
        padded_lanes(surface_adjoint.reshape(2, 1, half)), padded_lanes(parts), 5
    )
    from_flux = jnp.einsum(
        "hfg,cf->hgc",
        flux_adjoint[:, :, :half],
        flux_read.astype(jnp.float32),
        precision=highest,
    ).reshape(1, lon_count, channels)
    atmosphere_grad = input_adjoint + from_flux
    coarse_adjoint = jnp.einsum(
        "so,sg->og", to_atmosphere, surface_rows_adjoint[:, 0, :half], precision=highest
    )
    widened_adjoint = jnp.broadcast_to(
        coarse_adjoint[:, :, None], (ocean_rows, half, ratio)
    ).reshape(ocean_rows, ocean_lon)
    surface_grad = mask_value * widened_adjoint / ratio
    ocean_grad = (
        cotangent + surface_grad[:, :, None] * surface_read.astype(jnp.float32)[None, None, :]
    )
    return (atmosphere_next, state, atmosphere_grad, ocean_grad)


def solution(mesh):
    placed = (
        P(SEC_TILE, None, None),
        P(TILE, "sec", None),
        P(TILE, "sec"),
        P(TILE, None),
        P(TILE, None, None, None),
        P(TILE, None, None, None),
        P(),
        P(),
        P(),
        P(),
        P(SEC_TILE, None, None),
        P(SEC_TILE, None, None),
        P(),
        P(),
        P(),
        P(),
        P(),
        P(SEC_TILE, None, None),
        P(TILE, "sec", None),
    )
    return jax.shard_map(
        per_device,
        mesh=mesh,
        in_specs=placed,
        out_specs=(
            P(SEC_TILE, None, None),
            P(TILE, "sec", None),
            P(SEC_TILE, None, None),
            P(TILE, "sec", None),
        ),
        check_vma=False,
    )
```

```python
import functools

import jax
import jax.numpy as jnp
from jax import lax
from jax.experimental import pallas as pl
from jax.experimental.pallas import tpu as pltpu
from jax.sharding import PartitionSpec as P

SEC_TILE = ("sec", "tile")
TILE = "tile"
LOGICAL = pl.DeviceIdType.LOGICAL
DEVICES = 128
GROUPS = 64
SLOTS = 8
LANES = 256


def remote(src, dst, send_sem, recv_sem, device):
    return pltpu.make_async_remote_copy(
        src_ref=src,
        dst_ref=dst,
        send_sem=send_sem,
        recv_sem=recv_sem,
        device_id=device,
        device_id_type=LOGICAL,
    )


def all_to_all_kernel(x_ref, o_ref, landed, send_sem, recv_sem):
    me = lax.axis_index("sec") * GROUPS + lax.axis_index("tile")
    barrier = pltpu.get_barrier_semaphore()

    def greet(i, carry):
        pl.semaphore_signal(
            barrier, inc=1, device_id=(me + i) % DEVICES, device_id_type=LOGICAL
        )
        return carry

    lax.fori_loop(1, DEVICES, greet, 0)
    pl.semaphore_wait(barrier, DEVICES - 1)

    def send(i, carry):
        peer = (me + i) % DEVICES
        remote(x_ref.at[peer], landed.at[me], send_sem, recv_sem, peer).start()
        return carry

    lax.fori_loop(1, DEVICES, send, 0)
    landed[me] = x_ref[me]
    every = landed.at[pl.ds(0, DEVICES - 1)]
    pltpu.make_async_copy(every, every, recv_sem).wait()
    pltpu.make_async_copy(every, every, send_sem).wait()
    o_ref[...] = landed[...]


def all_to_all(blocks, number):
    return pl.pallas_call(
        all_to_all_kernel,
        out_shape=jax.ShapeDtypeStruct(blocks.shape, blocks.dtype),
        in_specs=[pl.BlockSpec(memory_space=pltpu.VMEM)],
        out_specs=pl.BlockSpec(memory_space=pltpu.VMEM),
        scratch_shapes=[
            pltpu.VMEM(blocks.shape, blocks.dtype),
            pltpu.SemaphoreType.DMA,
            pltpu.SemaphoreType.DMA,
        ],
        compiler_params=pltpu.CompilerParams(collective_id=number, has_side_effects=True),
        name=f"exchange_{number}",
    )(blocks)


def regrid_kernel(
    rows_ref, parts_ref, gathered_ref, summed_ref, rows_in, parts_in, sems
):
    sec = lax.axis_index("sec")
    group = lax.axis_index("tile")
    me = sec * GROUPS + group
    barrier = pltpu.get_barrier_semaphore()

    def group_device(k):
        return (k % 2) * GROUPS + (me // 2 + 1 - k // 2 + GROUPS) % GROUPS

    def band_device(slot):
        return (2 * group - 2 + slot + DEVICES) % DEVICES

    mine = me * 0
    for k in range(SLOTS):
        for peer in (group_device(k), band_device(k)):
            mine = mine + jnp.where(peer == me, 1, 0)

            @pl.when(peer != me)
            def _():
                pl.semaphore_signal(barrier, inc=1, device_id=peer, device_id_type=LOGICAL)

    pl.semaphore_wait(barrier, 2 * SLOTS - mine)

    for k in range(SLOTS):
        target = group_device(k)
        slot = me % 2 + 2 * (k // 2)

        @pl.when(target != me)
        def _():
            remote(
                rows_ref.at[k % 2], rows_in.at[slot], sems.at[0, k], sems.at[1, slot], target
            ).start()

        @pl.when(target == me)
        def _():
            rows_in[slot] = rows_ref[k % 2]

        band = band_device(k)
        place = (k // 2) * 2 + sec

        @pl.when(band != me)
        def _():
            remote(
                parts_ref.at[k], parts_in.at[place], sems.at[2, k], sems.at[3, place], band
            ).start()

        @pl.when(band == me)
        def _():
            parts_in[place] = parts_ref[k]

    for k in range(SLOTS):

        @pl.when(band_device(k) != me)
        def _():
            remote(rows_ref.at[0], rows_in.at[k], sems.at[0, k], sems.at[1, k], me).wait_recv()
            remote(parts_ref.at[k], parts_in.at[k], sems.at[2, k], sems.at[3, k], me).wait_send()

        @pl.when(group_device(k) != me)
        def _():
            remote(rows_ref.at[0], rows_in.at[k], sems.at[0, k], sems.at[1, k], me).wait_send()
            remote(parts_ref.at[k], parts_in.at[k], sems.at[2, k], sems.at[3, k], me).wait_recv()

    gathered_ref[...] = rows_in[...]
    for half in range(2):
        total = parts_in[half]
        for k in range(1, 4):
            total = total + parts_in[2 * k + half]
        summed_ref[half] = total


def regrid(rows, parts, number):
    _, r, lanes = rows.shape
    _, q, _ = parts.shape
    vmem = pl.BlockSpec(memory_space=pltpu.VMEM)
    return pl.pallas_call(
        regrid_kernel,
        out_shape=(
            jax.ShapeDtypeStruct((SLOTS, r, lanes), jnp.float32),
            jax.ShapeDtypeStruct((2, q, lanes), jnp.float32),
        ),
        in_specs=[vmem, vmem],
        out_specs=(vmem, vmem),
        scratch_shapes=[
            pltpu.VMEM((SLOTS, r, lanes), jnp.float32),
            pltpu.VMEM((SLOTS, q, lanes), jnp.float32),
            pltpu.SemaphoreType.DMA((4, SLOTS)),
        ],
        compiler_params=pltpu.CompilerParams(collective_id=number, has_side_effects=True),
        name=f"regrid_{number}",
    )(rows, parts)


X = 144
CHUNKS = 5
ROWS = 8
WIDE = 736
EDGE = 8
CELL = 128
TAPS = 7
REACH = 3


def spread_taps(bands, taps_ref, layer, flipped):
    eye = lax.broadcasted_iota(jnp.int32, (CELL, CELL), 0) == lax.broadcasted_iota(
        jnp.int32, (CELL, CELL), 1
    )

    def one(v, carry):
        for u in range(TAPS):
            if flipped:
                row = taps_ref[layer, pl.ds((TAPS - 1 - u) * TAPS + (TAPS - 1) - v, 1), :]
            else:
                row = taps_ref[layer, pl.ds(u * TAPS + v, 1), :]
            block = jnp.where(eye, row, 0.0).astype(jnp.bfloat16)
            for q in range(2):
                bands[v, pl.ds((u + q) * CELL, CELL), pl.ds(q * CELL, CELL)] = block
        return carry

    lax.fori_loop(0, TAPS, one, 0)


def convolve(window, bands, hidden, x0):
    total = None
    for v in range(TAPS):
        rows = [
            window[r, pl.ds(x0 + EDGE - REACH + v, X), :].astype(jnp.bfloat16)
            for r in range(ROWS + 2 * REACH)
        ]
        left = jnp.concatenate(
            [jnp.concatenate(rows[2 * p : 2 * p + 8], axis=1) for p in range(ROWS // 2)], axis=0
        )
        part = jnp.dot(left, bands[v], preferred_element_type=jnp.float32)
        total = part if total is None else total + part
    for p in range(ROWS // 2):
        for q in range(2):
            hidden[2 * p + q] = total[p * X : (p + 1) * X, q * CELL : (q + 1) * CELL]


def normalized(hidden):
    center = hidden - jnp.mean(hidden, axis=-1, keepdims=True)
    rstd = lax.rsqrt(jnp.mean(center * center, axis=-1, keepdims=True) + 1e-06)
    return center * rstd, rstd


GELU_A = 0.7978845608028654
GELU_B = GELU_A * 0.044715


def gelu_pair(v):
    square = v * v
    t = jnp.tanh(v * (GELU_A + GELU_B * square))
    half = 0.5 * v
    value = half + half * t
    slope = (0.5 + 0.5 * t) + (half * (1.0 - t * t)) * (GELU_A + (3.0 * GELU_B) * square)
    return value, slope


def dot32(a, b):
    return jnp.dot(a, b, preferred_element_type=jnp.float32)


def dot_t(a, b):
    return lax.dot_general(a, b, (((1,), (1,)), ((), ())), preferred_element_type=jnp.float32)


def adjoint_cell(masked, slope, unit, rstd, gain, expand, project):
    before_adj = (slope * dot_t(masked, project)).astype(jnp.bfloat16)
    scaled = dot_t(before_adj, expand) * gain
    inner = jnp.mean(scaled * unit, axis=-1, keepdims=True)
    return (rstd * (scaled - jnp.mean(scaled, axis=-1, keepdims=True) - unit * inner)).astype(
        jnp.bfloat16
    )


def ocean_kernel(
    linked,
    state_ref,
    mask_ref,
    cot_ref,
    taps_ref,
    gain_ref,
    expand_ref,
    project_ref,
    next_ref,
    grad_ref,
    win_a,
    win_b,
    bands,
    hidden,
    unit_0,
    rstd_0,
    slope_0,
    out_rows,
    in_rows,
    in_cols,
    row_sems,
    col_sems,
):
    sec = lax.axis_index("sec") if linked else 0
    tile = lax.axis_index("tile") if linked else 0
    last_tile = GROUPS - 1 if linked else 0
    me = sec * GROUPS + tile
    side = (1 - sec) * GROUPS + tile
    windows = (win_a, win_b)

    if linked:
        barrier = pltpu.get_barrier_semaphore()
        pl.semaphore_signal(barrier, inc=1, device_id=side, device_id_type=LOGICAL)

        @pl.when(tile > 0)
        def _():
            for peer in (me - 1, side - 1):
                pl.semaphore_signal(barrier, inc=1, device_id=peer, device_id_type=LOGICAL)

        @pl.when(tile < last_tile)
        def _():
            for peer in (me + 1, side + 1):
                pl.semaphore_signal(barrier, inc=1, device_id=peer, device_id_type=LOGICAL)

    zero_rows = jnp.zeros((REACH, WIDE, CELL), jnp.float32)

    @pl.when(tile == 0)
    def _():
        for w in windows:
            w[0:REACH] = zero_rows

    @pl.when(tile == last_tile)
    def _():
        for w in windows:
            w[REACH + ROWS :] = zero_rows

    if not linked:
        for w in windows:
            w[:, 0:EDGE] = jnp.zeros((14, EDGE, CELL), jnp.float32)
            w[:, WIDE - EDGE :] = jnp.zeros((14, EDGE, CELL), jnp.float32)
    for v in range(TAPS):
        bands[v, 0:CELL, CELL:] = jnp.zeros((CELL, CELL), jnp.bfloat16)
        bands[v, 7 * CELL :, :CELL] = jnp.zeros((CELL, CELL), jnp.bfloat16)

    if linked:
        count = 1 + jnp.where(tile > 0, 2, 0) + jnp.where(tile < last_tile, 2, 0)
        pl.semaphore_wait(barrier, count)

    def row_copy(e, way, c, peer):
        x0 = pl.multiple_of(c * X, 16)
        return remote(
            out_rows.at[e, pl.ds(0 if way == 0 else ROWS - REACH, REACH), pl.ds(x0, X)],
            in_rows.at[e, way, :, pl.ds(x0, X)],
            row_sems.at[0, e, way, c],
            row_sems.at[1, e, way, c],
            peer,
        )

    def col_copy(e, edge, part, peer):
        source = windows[e % 2]
        first, size, place = ((0, ROWS, REACH), (0, REACH, REACH + ROWS), (ROWS - REACH, REACH, 0))[
            part
        ]
        return remote(
            source.at[
                pl.ds(REACH + first, size), pl.ds(EDGE if edge == 0 else WIDE - 2 * EDGE, EDGE)
            ],
            in_cols.at[e, edge, pl.ds(place, size)],
            col_sems.at[0, e, edge, part],
            col_sems.at[1, e, edge, part],
            peer,
        )

    def send_chunk(e, k, c):
        if not linked:
            return

        @pl.when(tile > 0)
        def _():
            row_copy(e, 0, c, me - 1).start()

        @pl.when(tile < last_tile)
        def _():
            row_copy(e, 1, c, me + 1).start()

        for edge in range(2):

            @pl.when(k == edge)
            def _():
                col_copy(e, edge, 0, side).start()

                @pl.when(tile > 0)
                def _():
                    col_copy(e, edge, 1, side - 1).start()

                @pl.when(tile < last_tile)
                def _():
                    col_copy(e, edge, 2, side + 1).start()

    def take_rows(e, c):
        x0 = pl.multiple_of(c * X, 16)
        window = windows[e % 2]

        @pl.when(tile > 0)
        def _():
            row_copy(e, 1, c, me - 1).wait_recv()
            window[0:REACH, pl.ds(EDGE + x0, X), :] = in_rows[e, 1, :, pl.ds(x0, X), :].astype(
                jnp.float32
            )

        @pl.when(tile < last_tile)
        def _():
            row_copy(e, 0, c, me + 1).wait_recv()
            window[REACH + ROWS :, pl.ds(EDGE + x0, X), :] = in_rows[
                e, 0, :, pl.ds(x0, X), :
            ].astype(jnp.float32)

    def take_cols(e, edge):
        window = windows[e % 2]
        at = pl.ds(0 if edge == 1 else WIDE - EDGE, EDGE)
        col_copy(e, edge, 0, side).wait_recv()
        window[pl.ds(REACH, ROWS), at, :] = in_cols[e, edge, pl.ds(REACH, ROWS)]

        @pl.when(tile > 0)
        def _():
            col_copy(e, edge, 2, side - 1).wait_recv()
            window[pl.ds(0, REACH), at, :] = in_cols[e, edge, pl.ds(0, REACH)]

        @pl.when(tile < last_tile)
        def _():
            col_copy(e, edge, 1, side + 1).wait_recv()
            window[pl.ds(REACH + ROWS, REACH), at, :] = in_cols[
                e, edge, pl.ds(REACH + ROWS, REACH)
            ]

    def take_halo(e, k):
        if not linked:
            return

        @pl.when(k == 0)
        def _():
            take_rows(e, 0)
            take_rows(e, 1)
            take_cols(e, 1)

        @pl.when(k == 1)
        def _():
            take_rows(e, CHUNKS - 1)
            take_rows(e, CHUNKS - 2)
            take_cols(e, 0)

        @pl.when(k == 2)
        def _():
            take_rows(e, CHUNKS // 2)

    def sent(e):
        if not linked:
            return

        def one(c, carry):
            @pl.when(tile > 0)
            def _():
                row_copy(e, 0, c, me - 1).wait_send()

            @pl.when(tile < last_tile)
            def _():
                row_copy(e, 1, c, me + 1).wait_send()

            return carry

        lax.fori_loop(0, CHUNKS, one, 0)
        for edge in range(2):
            col_copy(e, edge, 0, side).wait_send()

            @pl.when(tile > 0)
            def _():
                col_copy(e, edge, 1, side - 1).wait_send()

            @pl.when(tile < last_tile)
            def _():
                col_copy(e, edge, 2, side + 1).wait_send()

    def chunk_of(k):
        return jnp.where(k % 2 == 0, k // 2, CHUNKS - 1 - k // 2)

    def keep(e, y, x0, value):
        windows[e % 2][y + REACH, pl.ds(EDGE + x0, X), :] = value.astype(jnp.float32)
        if linked:
            out_rows[e, y, pl.ds(x0, X), :] = value

    def stage(e, body):
        def chunk(k, carry):
            c = chunk_of(k)
            x0 = pl.multiple_of(c * X, 16)
            take_halo(e, k)
            convolve(windows[e % 2], bands, hidden, x0)

            def row(y, inner):
                body(y, x0, hidden[y])
                return inner

            lax.fori_loop(0, ROWS, row, 0)
            if e < 3:
                send_chunk(e + 1, k, c)
            return carry

        lax.fori_loop(0, CHUNKS, chunk, 0)
        sent(e)

    def first(k, carry):
        c = chunk_of(k)
        x0 = pl.multiple_of(c * X, 16)

        def row(y, inner):
            keep(0, y, x0, state_ref[y, pl.ds(x0, X), :])
            return inner

        lax.fori_loop(0, ROWS, row, 0)
        send_chunk(0, k, c)
        return carry

    lax.fori_loop(0, CHUNKS, first, 0)

    def mask_of(y, x0):
        return mask_ref[y, pl.ds(x0, X), :].astype(jnp.float32)

    def own(e, y, x0):
        return windows[e % 2][y + REACH, pl.ds(EDGE + x0, X), :]

    spread_taps(bands, taps_ref, 0, False)

    def forward_0(y, x0, hid):
        unit, rstd = normalized(hid)
        normed = (unit * gain_ref[0:1, :]).astype(jnp.bfloat16)
        value, slope = gelu_pair(dot32(normed, expand_ref[0]))
        update = dot32(value.astype(jnp.bfloat16), project_ref[0])
        unit_0[y, pl.ds(x0, X), :] = unit
        rstd_0[y, pl.ds(x0, X), :] = jnp.broadcast_to(rstd, (X, CELL))
        slope_0[y, pl.ds(x0, X), :] = slope
        keep(1, y, x0, (own(0, y, x0) + mask_of(y, x0) * update).astype(jnp.bfloat16))

    stage(0, forward_0)
    spread_taps(bands, taps_ref, 1, False)

    def forward_1(y, x0, hid):
        unit, rstd = normalized(hid)
        gain = gain_ref[1:2, :]
        normed = (unit * gain).astype(jnp.bfloat16)
        value, slope = gelu_pair(dot32(normed, expand_ref[1]))
        update = dot32(value.astype(jnp.bfloat16), project_ref[1])
        mask = mask_of(y, x0)
        next_ref[y, pl.ds(x0, X), :] = (own(1, y, x0) + mask * update).astype(jnp.bfloat16)
        masked = (mask * cot_ref[y, pl.ds(x0, X), :].astype(jnp.float32)).astype(jnp.bfloat16)
        keep(
            2, y, x0, adjoint_cell(masked, slope, unit, rstd, gain, expand_ref[1], project_ref[1])
        )

    stage(1, forward_1)
    spread_taps(bands, taps_ref, 1, True)

    def backward_0(y, x0, hid):
        cot = cot_ref[y, pl.ds(x0, X), :].astype(jnp.float32) + hid
        grad_ref[y, pl.ds(x0, X), :] = cot
        masked = (mask_of(y, x0) * cot).astype(jnp.bfloat16)
        keep(
            3,
            y,
            x0,
            adjoint_cell(
                masked,
                slope_0[y, pl.ds(x0, X), :],
                unit_0[y, pl.ds(x0, X), :],
                rstd_0[y, pl.ds(x0, X), :],
                gain_ref[0:1, :],
                expand_ref[0],
                project_ref[0],
            ),
        )

    stage(2, backward_0)
    spread_taps(bands, taps_ref, 0, True)

    def last(y, x0, hid):
        grad_ref[y, pl.ds(x0, X), :] = grad_ref[y, pl.ds(x0, X), :] + hid

    stage(3, last)


def ocean(state, mask, cotangent, taps, gain, expand, project, linked=True):
    vmem = pl.BlockSpec(memory_space=pltpu.VMEM)
    whole = (ROWS, CHUNKS * X, CELL)
    f32, bf16 = (jnp.float32, jnp.bfloat16)
    return pl.pallas_call(
        functools.partial(ocean_kernel, linked),
        out_shape=(jax.ShapeDtypeStruct(whole, bf16), jax.ShapeDtypeStruct(whole, f32)),
        in_specs=[vmem] * 7,
        out_specs=(vmem, vmem),
        scratch_shapes=[
            pltpu.VMEM((ROWS + 2 * REACH, WIDE, CELL), f32),
            pltpu.VMEM((ROWS + 2 * REACH, WIDE, CELL), f32),
            pltpu.VMEM((TAPS, 8 * CELL, 2 * CELL), bf16),
            pltpu.VMEM((ROWS, X, CELL), f32),
            pltpu.VMEM(whole, f32),
            pltpu.VMEM(whole, f32),
            pltpu.VMEM((ROWS, CHUNKS * X, 4 * CELL), f32),
            pltpu.VMEM((4, ROWS, CHUNKS * X, CELL), bf16),
            pltpu.VMEM((4, 2, REACH, CHUNKS * X, CELL), bf16),
            pltpu.VMEM((4, 2, ROWS + 2 * REACH, EDGE, CELL), f32),
            pltpu.SemaphoreType.DMA((2, 4, 2, CHUNKS)),
            pltpu.SemaphoreType.DMA((2, 4, 2, 3)),
        ],
        compiler_params=pltpu.CompilerParams(
            collective_id=6 if linked else None, has_side_effects=linked, vmem_limit_bytes=67000000
        ),
        name="ocean",
    )(state, mask, cotangent, taps, gain, expand, project)


def slot_weights(bands_row, blocks, group):
    slot = bands_row[:, None] - (2 * group - 2)
    onehot = (slot == jnp.arange(SLOTS, dtype=jnp.int32)[None, :]).astype(jnp.float32)
    return jnp.sum(onehot[:, :, None] * blocks[:, None, :], axis=0)


def padded_lanes(values):
    return jnp.pad(values, [(0, 0)] * (values.ndim - 1) + [(0, LANES - values.shape[-1])])


def wave_table(lon_count, mode_count):
    longitude = jnp.arange(lon_count, dtype=jnp.int32)
    wavenumber = jnp.arange(mode_count, dtype=jnp.int32)
    phase = (longitude[:, None] * wavenumber[None, :] % lon_count).astype(jnp.float32) * (
        2.0 * jnp.pi / lon_count
    )
    scaled = jnp.stack([jnp.cos(phase), -jnp.sin(phase)], axis=2) * jnp.sqrt(
        jnp.float32(2.0 / lon_count)
    )
    return scaled.reshape(lon_count, 2 * mode_count).astype(jnp.bfloat16)


def mix_complex(coefficient, mix_real, mix_imag):
    real_part = coefficient[:, :, 0]
    imag_part = coefficient[:, :, 1]
    out_real = jnp.einsum(
        "lmc,cd->lmd", real_part, mix_real, preferred_element_type=jnp.float32
    ) - jnp.einsum("lmc,cd->lmd", imag_part, mix_imag, preferred_element_type=jnp.float32)
    out_imag = jnp.einsum(
        "lmc,cd->lmd", imag_part, mix_real, preferred_element_type=jnp.float32
    ) + jnp.einsum("lmc,cd->lmd", real_part, mix_imag, preferred_element_type=jnp.float32)
    return jnp.stack([out_real, out_imag], axis=2).astype(jnp.bfloat16)


def spectral_block(spectrum, forward, inverse, mixing):
    lat_count, columns, channels = spectrum.shape
    split = spectrum.reshape(lat_count, columns // 2, 2, channels)
    coefficient = jnp.einsum(
        "mla,amrc->lmrc", forward, split, preferred_element_type=jnp.float32
    ).astype(jnp.bfloat16)
    mixed = mix_complex(coefficient, mixing[0], mixing[1])
    returned = jnp.einsum(
        "mal,lmrc->amrc", inverse, mixed, preferred_element_type=jnp.float32
    ).astype(jnp.bfloat16)
    return returned.reshape(lat_count, columns, channels)


def spectral_adjoint(returned_adjoint, forward, inverse, mixing):
    lat_count, columns, channels = returned_adjoint.shape
    split = returned_adjoint.reshape(lat_count, columns // 2, 2, channels)
    mixed_adjoint = jnp.einsum(
        "mal,amrc->lmrc", inverse, split, preferred_element_type=jnp.float32
    ).astype(jnp.bfloat16)
    real_part = mixed_adjoint[:, :, 0]
    imag_part = mixed_adjoint[:, :, 1]
    back_real = jnp.einsum(
        "lmd,cd->lmc", real_part, mixing[0], preferred_element_type=jnp.float32
    ) + jnp.einsum("lmd,cd->lmc", imag_part, mixing[1], preferred_element_type=jnp.float32)
    back_imag = jnp.einsum(
        "lmd,cd->lmc", imag_part, mixing[0], preferred_element_type=jnp.float32
    ) - jnp.einsum("lmd,cd->lmc", real_part, mixing[1], preferred_element_type=jnp.float32)
    coefficient_adjoint = jnp.stack([back_real, back_imag], axis=2).astype(jnp.bfloat16)
    spectrum_adjoint = jnp.einsum(
        "mla,lmrc->amrc", forward, coefficient_adjoint, preferred_element_type=jnp.float32
    ).astype(jnp.bfloat16)
    return spectrum_adjoint.reshape(lat_count, columns, channels)


def per_device(
    atmosphere,
    ocean_state,
    land_mask,
    crossing_bands,
    ocean_regrid,
    atmosphere_regrid,
    surface_read,
    surface_embed,
    flux_read,
    flux_embed,
    legendre_forward,
    legendre_inverse,
    spectral_mix,
    conv_kernel,
    norm_gain,
    expand_weight,
    project_weight,
    atmosphere_cotangent,
    ocean_cotangent,
):
    band_total = lax.axis_size(SEC_TILE)
    lat_rows, lon_count, channels = atmosphere.shape
    ocean_rows, ocean_lon, ocean_channels = ocean_state.shape
    half = lon_count // lax.axis_size("sec")
    offset = lax.axis_index("sec") * half
    ratio = ocean_lon // half
    flux_count = flux_read.shape[1]
    highest = lax.Precision.HIGHEST
    mask_value = land_mask.astype(jnp.float32)
    group = lax.axis_index("tile")
    to_ocean = slot_weights(crossing_bands[0], ocean_regrid[0, :, :, 0], group)
    to_atmosphere = slot_weights(crossing_bands[0], atmosphere_regrid[0, :, 0, :], group)
    surface = jnp.dot(ocean_state, surface_read, preferred_element_type=jnp.float32)
    coarse = jnp.mean((mask_value * surface).reshape(ocean_rows, half, ratio), axis=2)
    flux = jnp.einsum(
        "hgc,cf->hfg",
        atmosphere.reshape(2, half, channels),
        flux_read,
        preferred_element_type=jnp.float32,
    )
    flux_rows, surface_rows = regrid(
        padded_lanes(flux),
        padded_lanes(jnp.dot(to_atmosphere, coarse, precision=highest))[:, None, :],
        0,
    )
    surface_atmosphere = surface_rows[:, 0, :half].reshape(1, lon_count)
    flux_ocean = jnp.einsum("so,sfg->ogf", to_ocean, flux_rows[:, :, :half], precision=highest)
    mixed_input = (
        atmosphere.astype(jnp.float32)
        + surface_atmosphere[:, :, None] * surface_embed[None, None, :]
    ).astype(jnp.bfloat16)
    table = wave_table(lon_count, legendre_forward.shape[0] * band_total)
    spectrum = jnp.einsum(
        "gk,agc->akc", table, mixed_input, preferred_element_type=jnp.float32
    ).astype(jnp.bfloat16)
    modes = legendre_forward.shape[0] * band_total
    at_modes = all_to_all(spectrum.reshape(modes, 2, channels), 1)
    returned = spectral_block(at_modes, legendre_forward, legendre_inverse, spectral_mix)
    returned = all_to_all(returned, 2).reshape(1, 2 * modes, channels)
    response = jnp.einsum("gk,akc->agc", table, returned, preferred_element_type=jnp.float32)
    atmosphere_next = (mixed_input.astype(jnp.float32) + jax.nn.gelu(response)).astype(jnp.bfloat16)
    forcing_coarse = jnp.einsum(
        "ogf,fc->ogc",
        flux_ocean,
        flux_embed.astype(jnp.float32),
        precision=highest,
    )
    forcing = jnp.broadcast_to(
        forcing_coarse[:, :, None, :], (ocean_rows, half, ratio, ocean_channels)
    ).reshape(ocean_rows, ocean_lon, ocean_channels)
    state = (ocean_state.astype(jnp.float32) + mask_value[:, :, None] * forcing).astype(
        jnp.bfloat16
    )
    layer_count = conv_kernel.shape[0]
    state, cotangent = ocean(
        state,
        jnp.broadcast_to(mask_value[:, :, None], state.shape).astype(jnp.bfloat16),
        ocean_cotangent,
        conv_kernel.reshape(layer_count, TAPS * TAPS, CELL).astype(jnp.float32),
        norm_gain,
        expand_weight,
        project_weight,
    )
    forcing_adjoint = (
        (mask_value[:, :, None] * cotangent)
        .reshape(ocean_rows, half, ratio, ocean_channels)
        .sum(axis=2)
    )
    flux_ocean_adjoint = jnp.einsum(
        "ogc,fc->ofg", forcing_adjoint, flux_embed.astype(jnp.float32), precision=highest
    )
    atmosphere_adjoint = atmosphere_cotangent.astype(jnp.float32)
    _, gelu_back = jax.vjp(jax.nn.gelu, response)
    response_adjoint = gelu_back(atmosphere_adjoint)[0].astype(jnp.bfloat16)
    returned_adjoint = jnp.einsum(
        "gk,agc->akc", table, response_adjoint, preferred_element_type=jnp.float32
    ).astype(jnp.bfloat16)
    at_modes_adjoint = all_to_all(returned_adjoint.reshape(modes, 2, channels), 3)
    spectrum_adjoint = spectral_adjoint(
        at_modes_adjoint, legendre_forward, legendre_inverse, spectral_mix
    )
    spectrum_adjoint = all_to_all(spectrum_adjoint, 4).reshape(1, 2 * modes, channels)
    input_adjoint = atmosphere_adjoint + jnp.einsum(
        "gk,akc->agc", table, spectrum_adjoint, preferred_element_type=jnp.float32
    )
    surface_adjoint = jnp.einsum("agc,c->ag", input_adjoint, surface_embed, precision=highest)
    parts = jnp.einsum("so,ofg->sfg", to_ocean, flux_ocean_adjoint, precision=highest)
    surface_rows_adjoint, flux_adjoint = regrid(
        padded_lanes(surface_adjoint.reshape(2, 1, half)), padded_lanes(parts), 5
    )
    from_flux = jnp.einsum(
        "hfg,cf->hgc",
        flux_adjoint[:, :, :half],
        flux_read.astype(jnp.float32),
        precision=highest,
    ).reshape(1, lon_count, channels)
    atmosphere_grad = input_adjoint + from_flux
    coarse_adjoint = jnp.einsum(
        "so,sg->og", to_atmosphere, surface_rows_adjoint[:, 0, :half], precision=highest
    )
    widened_adjoint = jnp.broadcast_to(
        coarse_adjoint[:, :, None], (ocean_rows, half, ratio)
    ).reshape(ocean_rows, ocean_lon)
    surface_grad = mask_value * widened_adjoint / ratio
    ocean_grad = (
        cotangent + surface_grad[:, :, None] * surface_read.astype(jnp.float32)[None, None, :]
    )
    return (atmosphere_next, state, atmosphere_grad, ocean_grad)


def solution(mesh):
    placed = (
        P(SEC_TILE, None, None),
        P(TILE, "sec", None),
        P(TILE, "sec"),
        P(TILE, None),
        P(TILE, None, None, None),
        P(TILE, None, None, None),
        P(),
        P(),
        P(),
        P(),
        P(SEC_TILE, None, None),
        P(SEC_TILE, None, None),
        P(),
        P(),
        P(),
        P(),
        P(),
        P(SEC_TILE, None, None),
        P(TILE, "sec", None),
    )
    return jax.shard_map(
        per_device,
        mesh=mesh,
        in_specs=placed,
        out_specs=(
            P(SEC_TILE, None, None),
            P(TILE, "sec", None),
            P(SEC_TILE, None, None),
            P(TILE, "sec", None),
        ),
        check_vma=False,
    )
```

```python
import functools

import jax
import jax.numpy as jnp
import numpy as np
from jax import lax
from jax.experimental import pallas as pl
from jax.experimental.pallas import tpu as pltpu
from jax.sharding import PartitionSpec as P

SEC_TILE = ("sec", "tile")
TILE = "tile"
LOGICAL = pl.DeviceIdType.LOGICAL
DEVICES = 128
GROUPS = 64
SLOTS = 8
LANES = 256


def remote(src, dst, send_sem, recv_sem, device):
    return pltpu.make_async_remote_copy(
        src_ref=src,
        dst_ref=dst,
        send_sem=send_sem,
        recv_sem=recv_sem,
        device_id=device,
        device_id_type=LOGICAL,
    )


def regrid_kernel(
    rows_ref, parts_ref, gathered_ref, summed_ref, rows_in, parts_in, sems
):
    sec = lax.axis_index("sec")
    group = lax.axis_index("tile")
    me = sec * GROUPS + group
    barrier = pltpu.get_barrier_semaphore()

    def group_device(k):
        return (k % 2) * GROUPS + (me // 2 + 1 - k // 2 + GROUPS) % GROUPS

    def band_device(slot):
        return (2 * group - 2 + slot + DEVICES) % DEVICES

    mine = me * 0
    for k in range(SLOTS):
        for peer in (group_device(k), band_device(k)):
            mine = mine + jnp.where(peer == me, 1, 0)

            @pl.when(peer != me)
            def _():
                pl.semaphore_signal(barrier, inc=1, device_id=peer, device_id_type=LOGICAL)

    pl.semaphore_wait(barrier, 2 * SLOTS - mine)

    for k in range(SLOTS):
        target = group_device(k)
        slot = me % 2 + 2 * (k // 2)

        @pl.when(target != me)
        def _():
            remote(
                rows_ref.at[k % 2], rows_in.at[slot], sems.at[0, k], sems.at[1, slot], target
            ).start()

        @pl.when(target == me)
        def _():
            rows_in[slot] = rows_ref[k % 2]

        band = band_device(k)
        place = (k // 2) * 2 + sec

        @pl.when(band != me)
        def _():
            remote(
                parts_ref.at[k], parts_in.at[place], sems.at[2, k], sems.at[3, place], band
            ).start()

        @pl.when(band == me)
        def _():
            parts_in[place] = parts_ref[k]

    for k in range(SLOTS):

        @pl.when(band_device(k) != me)
        def _():
            remote(rows_ref.at[0], rows_in.at[k], sems.at[0, k], sems.at[1, k], me).wait_recv()
            remote(parts_ref.at[k], parts_in.at[k], sems.at[2, k], sems.at[3, k], me).wait_send()

        @pl.when(group_device(k) != me)
        def _():
            remote(rows_ref.at[0], rows_in.at[k], sems.at[0, k], sems.at[1, k], me).wait_send()
            remote(parts_ref.at[k], parts_in.at[k], sems.at[2, k], sems.at[3, k], me).wait_recv()

    gathered_ref[...] = rows_in[...]
    for half in range(2):
        total = parts_in[half]
        for k in range(1, 4):
            total = total + parts_in[2 * k + half]
        summed_ref[half] = total


def regrid(rows, parts, number):
    _, r, lanes = rows.shape
    _, q, _ = parts.shape
    vmem = pl.BlockSpec(memory_space=pltpu.VMEM)
    return pl.pallas_call(
        regrid_kernel,
        out_shape=(
            jax.ShapeDtypeStruct((SLOTS, r, lanes), jnp.float32),
            jax.ShapeDtypeStruct((2, q, lanes), jnp.float32),
        ),
        in_specs=[vmem, vmem],
        out_specs=(vmem, vmem),
        scratch_shapes=[
            pltpu.VMEM((SLOTS, r, lanes), jnp.float32),
            pltpu.VMEM((SLOTS, q, lanes), jnp.float32),
            pltpu.SemaphoreType.DMA((4, SLOTS)),
        ],
        compiler_params=pltpu.CompilerParams(collective_id=number, has_side_effects=True),
        name=f"regrid_{number}",
    )(rows, parts)


X = 144
CHUNKS = 5
ROWS = 8
WIDE = 736
EDGE = 8
CELL = 128
TAPS = 7
REACH = 3
ALON = 360


def spread_taps(bands, taps_ref, layer, flipped):
    eye = lax.broadcasted_iota(jnp.int32, (CELL, CELL), 0) == lax.broadcasted_iota(
        jnp.int32, (CELL, CELL), 1
    )

    def one(v, carry):
        for u in range(TAPS):
            if flipped:
                row = taps_ref[layer, pl.ds((TAPS - 1 - u) * TAPS + (TAPS - 1) - v, 1), :]
            else:
                row = taps_ref[layer, pl.ds(u * TAPS + v, 1), :]
            block = jnp.where(eye, row, 0.0).astype(jnp.bfloat16)
            for q in range(2):
                bands[v, pl.ds((u + q) * CELL, CELL), pl.ds(q * CELL, CELL)] = block
        return carry

    lax.fori_loop(0, TAPS, one, 0)


def convolve(window, bands, hidden, x0):
    total = None
    for v in range(TAPS):
        rows = [
            window[r, pl.ds(x0 + EDGE - REACH + v, X), :].astype(jnp.bfloat16)
            for r in range(ROWS + 2 * REACH)
        ]
        left = jnp.concatenate(
            [jnp.concatenate(rows[2 * p : 2 * p + 8], axis=1) for p in range(ROWS // 2)], axis=0
        )
        part = jnp.dot(left, bands[v], preferred_element_type=jnp.float32)
        total = part if total is None else total + part
    for p in range(ROWS // 2):
        for q in range(2):
            hidden[2 * p + q] = total[p * X : (p + 1) * X, q * CELL : (q + 1) * CELL]


def normalized(hidden):
    center = hidden - jnp.mean(hidden, axis=-1, keepdims=True)
    rstd = lax.rsqrt(jnp.mean(center * center, axis=-1, keepdims=True) + 1e-06)
    return center * rstd, rstd


GELU_A = 0.7978845608028654
GELU_B = GELU_A * 0.044715


def gelu_pair(v):
    square = v * v
    t = jnp.tanh(v * (GELU_A + GELU_B * square))
    half = 0.5 * v
    value = half + half * t
    slope = (0.5 + 0.5 * t) + (half * (1.0 - t * t)) * (GELU_A + (3.0 * GELU_B) * square)
    return value, slope


def dot32(a, b):
    return jnp.dot(a, b, preferred_element_type=jnp.float32)


def dot_t(a, b):
    return lax.dot_general(a, b, (((1,), (1,)), ((), ())), preferred_element_type=jnp.float32)


def adjoint_cell(masked, slope, unit, rstd, gain, expand, project):
    before_adj = (slope * dot_t(masked, project)).astype(jnp.bfloat16)
    scaled = dot_t(before_adj, expand) * gain
    inner = jnp.mean(scaled * unit, axis=-1, keepdims=True)
    return (rstd * (scaled - jnp.mean(scaled, axis=-1, keepdims=True) - unit * inner)).astype(
        jnp.bfloat16
    )


def ocean_kernel(
    linked,
    state_ref,
    mask_ref,
    cot_ref,
    taps_ref,
    gain_ref,
    expand_ref,
    project_ref,
    atmosphere_ref,
    atmosphere_cot_ref,
    spectrum_ref,
    wave_ref,
    wave_t_ref,
    forward_ref,
    inverse_ref,
    mix_ref,
    next_ref,
    grad_ref,
    atmosphere_next_ref,
    input_adj_ref,
    win_a,
    win_b,
    bands,
    hidden,
    unit_0,
    rstd_0,
    slope_0,
    out_rows,
    in_rows,
    in_cols,
    row_sems,
    col_sems,
    leaving,
    landed,
    swap_sems,
):
    sec = lax.axis_index("sec") if linked else 0
    tile = lax.axis_index("tile") if linked else 0
    last_tile = GROUPS - 1 if linked else 0
    me = sec * GROUPS + tile
    side = (1 - sec) * GROUPS + tile
    windows = (win_a, win_b)

    if linked:
        barrier = pltpu.get_barrier_semaphore()

        def greet(i, carry):
            pl.semaphore_signal(
                barrier, inc=1, device_id=(me + i) % DEVICES, device_id_type=LOGICAL
            )
            return carry

        lax.fori_loop(1, DEVICES, greet, 0)

    zero_rows = jnp.zeros((REACH, WIDE, CELL), jnp.float32)

    @pl.when(tile == 0)
    def _():
        for w in windows:
            w[0:REACH] = zero_rows

    @pl.when(tile == last_tile)
    def _():
        for w in windows:
            w[REACH + ROWS :] = zero_rows

    if not linked:
        for w in windows:
            w[:, 0:EDGE] = jnp.zeros((14, EDGE, CELL), jnp.float32)
            w[:, WIDE - EDGE :] = jnp.zeros((14, EDGE, CELL), jnp.float32)
    for v in range(TAPS):
        bands[v, 0:CELL, CELL:] = jnp.zeros((CELL, CELL), jnp.bfloat16)
        bands[v, 7 * CELL :, :CELL] = jnp.zeros((CELL, CELL), jnp.bfloat16)

    if linked:
        pl.semaphore_wait(barrier, DEVICES - 1)

    def put_blocks(x, values):
        for j in range(6):
            leaving[x, pl.ds(j, DEVICES, stride=8), :] = values[:, j * CELL : (j + 1) * CELL]
        if not linked:
            return

        def send(i, carry):
            peer = (me + i) % DEVICES
            remote(
                leaving.at[x, pl.ds(pl.multiple_of(peer * 8, 8), 8)],
                landed.at[x, pl.ds(pl.multiple_of(me * 8, 8), 8)],
                swap_sems.at[0, x],
                swap_sems.at[1, x],
                peer,
            ).start()
            return carry

        lax.fori_loop(1, DEVICES, send, 0)
        mine = pl.ds(pl.multiple_of(me * 8, 8), 8)
        landed[x, mine, :] = leaving[x, mine, :]

    def take_blocks(x):
        source = landed
        if linked:
            every = landed.at[x, pl.ds(0, (DEVICES - 1) * 8)]
            pltpu.make_async_copy(every, every, swap_sems.at[1, x]).wait()
            pltpu.make_async_copy(every, every, swap_sems.at[0, x]).wait()
        else:
            source = leaving
        return jnp.concatenate(
            [source[x, pl.ds(j, DEVICES, stride=8), :] for j in range(6)], axis=1
        ).astype(jnp.bfloat16)

    def rounded(values):
        return values.astype(jnp.bfloat16).astype(jnp.float32)

    half_c = 3 * CELL

    def spectral():
        coefficient = dot32(forward_ref[...], take_blocks(0)).astype(jnp.bfloat16)
        real, imag = (coefficient[:, :half_c], coefficient[:, half_c:])
        mixed = jnp.concatenate(
            [
                dot32(real, mix_ref[0]) - dot32(imag, mix_ref[1]),
                dot32(imag, mix_ref[0]) + dot32(real, mix_ref[1]),
            ],
            axis=1,
        ).astype(jnp.bfloat16)
        put_blocks(1, rounded(dot32(inverse_ref[...], mixed)))

    def respond():
        returned = take_blocks(1)
        returned = jnp.concatenate([returned[:, :half_c], returned[:, half_c:]], axis=0)
        parts = []
        for j in range(3):
            cols = pl.ds(j * CELL, CELL)
            response = dot32(wave_ref[...], returned[:, j * CELL : (j + 1) * CELL])
            value, slope = gelu_pair(response)
            atmosphere_next_ref[:, cols] = (
                atmosphere_ref[:, cols].astype(jnp.float32) + value
            ).astype(jnp.bfloat16)
            response_adj = (slope * atmosphere_cot_ref[:, cols].astype(jnp.float32)).astype(
                jnp.bfloat16
            )
            parts.append(dot32(wave_t_ref[...], response_adj))
        put_blocks(
            2,
            rounded(
                jnp.concatenate([p[:DEVICES] for p in parts] + [p[DEVICES:] for p in parts], axis=1)
            ),
        )

    def dot_first(a, b):
        return lax.dot_general(
            a, b, (((0,), (0,)), ((), ())), preferred_element_type=jnp.float32
        )

    def spectral_back():
        mixed_adj = dot_first(inverse_ref[...], take_blocks(2)).astype(jnp.bfloat16)
        real, imag = (mixed_adj[:, :half_c], mixed_adj[:, half_c:])
        coefficient_adj = jnp.concatenate(
            [
                dot_t(real, mix_ref[0]) + dot_t(imag, mix_ref[1]),
                dot_t(imag, mix_ref[0]) - dot_t(real, mix_ref[1]),
            ],
            axis=1,
        ).astype(jnp.bfloat16)
        put_blocks(3, rounded(dot_first(forward_ref[...], coefficient_adj)))

    def absorb():
        spectrum_adj = take_blocks(3)
        spectrum_adj = jnp.concatenate([spectrum_adj[:, :half_c], spectrum_adj[:, half_c:]], axis=0)
        for j in range(3):
            cols = pl.ds(j * CELL, CELL)
            input_adj_ref[:, cols] = atmosphere_cot_ref[:, cols].astype(jnp.float32) + dot32(
                wave_ref[...], spectrum_adj[:, j * CELL : (j + 1) * CELL]
            )

    def row_copy(e, way, c, peer):
        x0 = pl.multiple_of(c * X, 16)
        return remote(
            out_rows.at[e, pl.ds(0 if way == 0 else ROWS - REACH, REACH), pl.ds(x0, X)],
            in_rows.at[e, way, :, pl.ds(x0, X)],
            row_sems.at[0, e, way, c],
            row_sems.at[1, e, way, c],
            peer,
        )

    def col_copy(e, edge, part, peer):
        source = windows[e % 2]
        first, size, place = ((0, ROWS, REACH), (0, REACH, REACH + ROWS), (ROWS - REACH, REACH, 0))[
            part
        ]
        return remote(
            source.at[
                pl.ds(REACH + first, size), pl.ds(EDGE if edge == 0 else WIDE - 2 * EDGE, EDGE)
            ],
            in_cols.at[e, edge, pl.ds(place, size)],
            col_sems.at[0, e, edge, part],
            col_sems.at[1, e, edge, part],
            peer,
        )

    def send_chunk(e, k, c):
        if not linked:
            return

        @pl.when(tile > 0)
        def _():
            row_copy(e, 0, c, me - 1).start()

        @pl.when(tile < last_tile)
        def _():
            row_copy(e, 1, c, me + 1).start()

        for edge in range(2):

            @pl.when(k == edge)
            def _():
                col_copy(e, edge, 0, side).start()

                @pl.when(tile > 0)
                def _():
                    col_copy(e, edge, 1, side - 1).start()

                @pl.when(tile < last_tile)
                def _():
                    col_copy(e, edge, 2, side + 1).start()

    def take_rows(e, c):
        x0 = pl.multiple_of(c * X, 16)
        window = windows[e % 2]

        @pl.when(tile > 0)
        def _():
            row_copy(e, 1, c, me - 1).wait_recv()
            window[0:REACH, pl.ds(EDGE + x0, X), :] = in_rows[e, 1, :, pl.ds(x0, X), :].astype(
                jnp.float32
            )

        @pl.when(tile < last_tile)
        def _():
            row_copy(e, 0, c, me + 1).wait_recv()
            window[REACH + ROWS :, pl.ds(EDGE + x0, X), :] = in_rows[
                e, 0, :, pl.ds(x0, X), :
            ].astype(jnp.float32)

    def take_cols(e, edge):
        window = windows[e % 2]
        at = pl.ds(0 if edge == 1 else WIDE - EDGE, EDGE)
        col_copy(e, edge, 0, side).wait_recv()
        window[pl.ds(REACH, ROWS), at, :] = in_cols[e, edge, pl.ds(REACH, ROWS)]

        @pl.when(tile > 0)
        def _():
            col_copy(e, edge, 2, side - 1).wait_recv()
            window[pl.ds(0, REACH), at, :] = in_cols[e, edge, pl.ds(0, REACH)]

        @pl.when(tile < last_tile)
        def _():
            col_copy(e, edge, 1, side + 1).wait_recv()
            window[pl.ds(REACH + ROWS, REACH), at, :] = in_cols[
                e, edge, pl.ds(REACH + ROWS, REACH)
            ]

    def take_halo(e, k):
        if not linked:
            return

        @pl.when(k == 0)
        def _():
            take_rows(e, 0)
            take_rows(e, 1)
            take_cols(e, 1)

        @pl.when(k == 1)
        def _():
            take_rows(e, CHUNKS - 1)
            take_rows(e, CHUNKS - 2)
            take_cols(e, 0)

        @pl.when(k == 2)
        def _():
            take_rows(e, CHUNKS // 2)

    def sent(e):
        if not linked:
            return

        def one(c, carry):
            @pl.when(tile > 0)
            def _():
                row_copy(e, 0, c, me - 1).wait_send()

            @pl.when(tile < last_tile)
            def _():
                row_copy(e, 1, c, me + 1).wait_send()

            return carry

        lax.fori_loop(0, CHUNKS, one, 0)
        for edge in range(2):
            col_copy(e, edge, 0, side).wait_send()

            @pl.when(tile > 0)
            def _():
                col_copy(e, edge, 1, side - 1).wait_send()

            @pl.when(tile < last_tile)
            def _():
                col_copy(e, edge, 2, side + 1).wait_send()

    def chunk_of(k):
        return jnp.where(k % 2 == 0, k // 2, CHUNKS - 1 - k // 2)

    def keep(e, y, x0, value):
        windows[e % 2][y + REACH, pl.ds(EDGE + x0, X), :] = value.astype(jnp.float32)
        if linked:
            out_rows[e, y, pl.ds(x0, X), :] = value

    def stage(e, body):
        def chunk(k, carry):
            c = chunk_of(k)
            x0 = pl.multiple_of(c * X, 16)
            take_halo(e, k)
            convolve(windows[e % 2], bands, hidden, x0)

            def row(y, inner):
                body(y, x0, hidden[y])
                return inner

            lax.fori_loop(0, ROWS, row, 0)
            if e < 3:
                send_chunk(e + 1, k, c)
            return carry

        lax.fori_loop(0, CHUNKS, chunk, 0)
        sent(e)

    def first(k, carry):
        c = chunk_of(k)
        x0 = pl.multiple_of(c * X, 16)

        def row(y, inner):
            keep(0, y, x0, state_ref[y, pl.ds(x0, X), :])
            return inner

        lax.fori_loop(0, ROWS, row, 0)
        send_chunk(0, k, c)
        return carry

    lax.fori_loop(0, CHUNKS, first, 0)
    put_blocks(0, spectrum_ref[...])

    def mask_of(y, x0):
        return mask_ref[y, pl.ds(x0, X), :].astype(jnp.float32)

    def own(e, y, x0):
        return windows[e % 2][y + REACH, pl.ds(EDGE + x0, X), :]

    spread_taps(bands, taps_ref, 0, False)

    def forward_0(y, x0, hid):
        unit, rstd = normalized(hid)
        normed = (unit * gain_ref[0:1, :]).astype(jnp.bfloat16)
        value, slope = gelu_pair(dot32(normed, expand_ref[0]))
        update = dot32(value.astype(jnp.bfloat16), project_ref[0])
        unit_0[y, pl.ds(x0, X), :] = unit
        rstd_0[y, pl.ds(x0, X), :] = jnp.broadcast_to(rstd, (X, CELL))
        slope_0[y, pl.ds(x0, X), :] = slope
        keep(1, y, x0, (own(0, y, x0) + mask_of(y, x0) * update).astype(jnp.bfloat16))

    stage(0, forward_0)
    spectral()
    spread_taps(bands, taps_ref, 1, False)

    def forward_1(y, x0, hid):
        unit, rstd = normalized(hid)
        gain = gain_ref[1:2, :]
        normed = (unit * gain).astype(jnp.bfloat16)
        value, slope = gelu_pair(dot32(normed, expand_ref[1]))
        update = dot32(value.astype(jnp.bfloat16), project_ref[1])
        mask = mask_of(y, x0)
        next_ref[y, pl.ds(x0, X), :] = (own(1, y, x0) + mask * update).astype(jnp.bfloat16)
        masked = (mask * cot_ref[y, pl.ds(x0, X), :].astype(jnp.float32)).astype(jnp.bfloat16)
        keep(
            2, y, x0, adjoint_cell(masked, slope, unit, rstd, gain, expand_ref[1], project_ref[1])
        )

    stage(1, forward_1)
    respond()
    spread_taps(bands, taps_ref, 1, True)

    def backward_0(y, x0, hid):
        cot = cot_ref[y, pl.ds(x0, X), :].astype(jnp.float32) + hid
        grad_ref[y, pl.ds(x0, X), :] = cot
        masked = (mask_of(y, x0) * cot).astype(jnp.bfloat16)
        keep(
            3,
            y,
            x0,
            adjoint_cell(
                masked,
                slope_0[y, pl.ds(x0, X), :],
                unit_0[y, pl.ds(x0, X), :],
                rstd_0[y, pl.ds(x0, X), :],
                gain_ref[0:1, :],
                expand_ref[0],
                project_ref[0],
            ),
        )

    stage(2, backward_0)
    spectral_back()
    spread_taps(bands, taps_ref, 0, True)

    def last(y, x0, hid):
        grad_ref[y, pl.ds(x0, X), :] = grad_ref[y, pl.ds(x0, X), :] + hid

    stage(3, last)
    absorb()


def ocean(*operands, linked=True):
    vmem = pl.BlockSpec(memory_space=pltpu.VMEM)
    whole = (ROWS, CHUNKS * X, CELL)
    f32, bf16 = (jnp.float32, jnp.bfloat16)
    return pl.pallas_call(
        functools.partial(ocean_kernel, linked),
        out_shape=(
            jax.ShapeDtypeStruct(whole, bf16),
            jax.ShapeDtypeStruct(whole, f32),
            jax.ShapeDtypeStruct((ALON, 3 * CELL), bf16),
            jax.ShapeDtypeStruct((ALON, 3 * CELL), f32),
        ),
        in_specs=[vmem] * 15,
        out_specs=(vmem,) * 4,
        scratch_shapes=[
            pltpu.VMEM((ROWS + 2 * REACH, WIDE, CELL), f32),
            pltpu.VMEM((ROWS + 2 * REACH, WIDE, CELL), f32),
            pltpu.VMEM((TAPS, 8 * CELL, 2 * CELL), bf16),
            pltpu.VMEM((ROWS, X, CELL), f32),
            pltpu.VMEM(whole, f32),
            pltpu.VMEM(whole, f32),
            pltpu.VMEM((ROWS, CHUNKS * X, 4 * CELL), f32),
            pltpu.VMEM((4, ROWS, CHUNKS * X, CELL), bf16),
            pltpu.VMEM((4, 2, REACH, CHUNKS * X, CELL), bf16),
            pltpu.VMEM((4, 2, ROWS + 2 * REACH, EDGE, CELL), f32),
            pltpu.SemaphoreType.DMA((2, 4, 2, CHUNKS)),
            pltpu.SemaphoreType.DMA((2, 4, 2, 3)),
            pltpu.VMEM((4, DEVICES * 8, CELL), f32),
            pltpu.VMEM((4, DEVICES * 8, CELL), f32),
            pltpu.SemaphoreType.DMA((2, 4)),
        ],
        compiler_params=pltpu.CompilerParams(
            collective_id=6 if linked else None, has_side_effects=linked, vmem_limit_bytes=67000000
        ),
        name="ocean",
    )(*operands)


def wave_table():
    place = np.arange(ALON, dtype=np.int32)[:, None] * np.arange(DEVICES, dtype=np.int32)[None, :]
    phase = (place % ALON).astype(np.float32) * np.float32(2.0 * np.pi / ALON)
    both = np.concatenate([np.cos(phase), -np.sin(phase)], axis=1)
    return (both * np.sqrt(np.float32(2.0 / ALON))).astype(jnp.bfloat16)


def slot_weights(bands_row, blocks, group):
    slot = bands_row[:, None] - (2 * group - 2)
    onehot = (slot == jnp.arange(SLOTS, dtype=jnp.int32)[None, :]).astype(jnp.float32)
    return jnp.sum(onehot[:, :, None] * blocks[:, None, :], axis=0)


def padded_lanes(values):
    return jnp.pad(values, [(0, 0)] * (values.ndim - 1) + [(0, LANES - values.shape[-1])])


def per_device(
    atmosphere,
    ocean_state,
    land_mask,
    crossing_bands,
    ocean_regrid,
    atmosphere_regrid,
    surface_read,
    surface_embed,
    flux_read,
    flux_embed,
    legendre_forward,
    legendre_inverse,
    spectral_mix,
    conv_kernel,
    norm_gain,
    expand_weight,
    project_weight,
    atmosphere_cotangent,
    ocean_cotangent,
):
    lat_rows, lon_count, channels = atmosphere.shape
    ocean_rows, ocean_lon, ocean_channels = ocean_state.shape
    half = lon_count // lax.axis_size("sec")
    offset = lax.axis_index("sec") * half
    ratio = ocean_lon // half
    flux_count = flux_read.shape[1]
    highest = lax.Precision.HIGHEST
    mask_value = land_mask.astype(jnp.float32)
    group = lax.axis_index("tile")
    to_ocean = slot_weights(crossing_bands[0], ocean_regrid[0, :, :, 0], group)
    to_atmosphere = slot_weights(crossing_bands[0], atmosphere_regrid[0, :, 0, :], group)
    surface = jnp.dot(ocean_state, surface_read, preferred_element_type=jnp.float32)
    coarse = jnp.mean((mask_value * surface).reshape(ocean_rows, half, ratio), axis=2)
    flux = jnp.einsum(
        "hgc,cf->hfg",
        atmosphere.reshape(2, half, channels),
        flux_read,
        preferred_element_type=jnp.float32,
    )
    flux_rows, surface_rows = regrid(
        padded_lanes(flux),
        padded_lanes(jnp.dot(to_atmosphere, coarse, precision=highest))[:, None, :],
        0,
    )
    surface_atmosphere = surface_rows[:, 0, :half].reshape(1, lon_count)
    flux_ocean = jnp.einsum("so,sfg->ogf", to_ocean, flux_rows[:, :, :half], precision=highest)
    mixed_input = (
        atmosphere.astype(jnp.float32)
        + surface_atmosphere[:, :, None] * surface_embed[None, None, :]
    ).astype(jnp.bfloat16)
    table = wave_table()
    spectrum = jnp.einsum(
        "gk,gc->kc", jnp.asarray(table), mixed_input[0], preferred_element_type=jnp.float32
    )
    spectrum = spectrum.astype(jnp.bfloat16).astype(jnp.float32)
    spectrum = jnp.concatenate([spectrum[:DEVICES], spectrum[DEVICES:]], axis=1)
    forcing_coarse = jnp.einsum(
        "ogf,fc->ogc",
        flux_ocean,
        flux_embed.astype(jnp.float32),
        precision=highest,
    )
    forcing = jnp.broadcast_to(
        forcing_coarse[:, :, None, :], (ocean_rows, half, ratio, ocean_channels)
    ).reshape(ocean_rows, ocean_lon, ocean_channels)
    state = (ocean_state.astype(jnp.float32) + mask_value[:, :, None] * forcing).astype(
        jnp.bfloat16
    )
    layer_count = conv_kernel.shape[0]
    state, cotangent, atmosphere_next, input_adjoint = ocean(
        state,
        jnp.broadcast_to(mask_value[:, :, None], state.shape).astype(jnp.bfloat16),
        ocean_cotangent,
        conv_kernel.reshape(layer_count, TAPS * TAPS, CELL).astype(jnp.float32),
        norm_gain,
        expand_weight,
        project_weight,
        mixed_input[0],
        atmosphere_cotangent[0],
        spectrum,
        jnp.asarray(table),
        jnp.asarray(np.ascontiguousarray(table.T)),
        legendre_forward[0],
        legendre_inverse[0],
        spectral_mix,
    )
    forcing_adjoint = (
        (mask_value[:, :, None] * cotangent)
        .reshape(ocean_rows, half, ratio, ocean_channels)
        .sum(axis=2)
    )
    flux_ocean_adjoint = jnp.einsum(
        "ogc,fc->ofg", forcing_adjoint, flux_embed.astype(jnp.float32), precision=highest
    )
    surface_adjoint = jnp.einsum("gc,c->g", input_adjoint, surface_embed, precision=highest)
    parts = jnp.einsum("so,ofg->sfg", to_ocean, flux_ocean_adjoint, precision=highest)
    surface_rows_adjoint, flux_adjoint = regrid(
        padded_lanes(surface_adjoint.reshape(2, 1, half)), padded_lanes(parts), 5
    )
    from_flux = jnp.einsum(
        "hfg,cf->hgc",
        flux_adjoint[:, :, :half],
        flux_read.astype(jnp.float32),
        precision=highest,
    ).reshape(lon_count, channels)
    atmosphere_grad = input_adjoint + from_flux
    coarse_adjoint = jnp.einsum(
        "so,sg->og", to_atmosphere, surface_rows_adjoint[:, 0, :half], precision=highest
    )
    widened_adjoint = jnp.broadcast_to(
        coarse_adjoint[:, :, None], (ocean_rows, half, ratio)
    ).reshape(ocean_rows, ocean_lon)
    surface_grad = mask_value * widened_adjoint / ratio
    ocean_grad = (
        cotangent + surface_grad[:, :, None] * surface_read.astype(jnp.float32)[None, None, :]
    )
    return (atmosphere_next[None], state, atmosphere_grad[None], ocean_grad)


def solution(mesh):
    placed = (
        P(SEC_TILE, None, None),
        P(TILE, "sec", None),
        P(TILE, "sec"),
        P(TILE, None),
        P(TILE, None, None, None),
        P(TILE, None, None, None),
        P(),
        P(),
        P(),
        P(),
        P(SEC_TILE, None, None),
        P(SEC_TILE, None, None),
        P(),
        P(),
        P(),
        P(),
        P(),
        P(SEC_TILE, None, None),
        P(TILE, "sec", None),
    )
    return jax.shard_map(
        per_device,
        mesh=mesh,
        in_specs=placed,
        out_specs=(
            P(SEC_TILE, None, None),
            P(TILE, "sec", None),
            P(SEC_TILE, None, None),
            P(TILE, "sec", None),
        ),
        check_vma=False,
    )
```

```python
import functools

import jax
import jax.numpy as jnp
import numpy as np
from jax import lax
from jax.experimental import pallas as pl
from jax.experimental.pallas import tpu as pltpu
from jax.sharding import PartitionSpec as P

SEC_TILE = ("sec", "tile")
TILE = "tile"
LOGICAL = pl.DeviceIdType.LOGICAL
DEVICES = 128
GROUPS = 64
SLOTS = 8
LANES = 256


def remote(src, dst, send_sem, recv_sem, device):
    return pltpu.make_async_remote_copy(
        src_ref=src,
        dst_ref=dst,
        send_sem=send_sem,
        recv_sem=recv_sem,
        device_id=device,
        device_id_type=LOGICAL,
    )


def regrid_peers():
    sec = lax.axis_index("sec")
    group = lax.axis_index("tile")
    me = sec * GROUPS + group

    def group_device(k):
        return (k % 2) * GROUPS + (me // 2 + 1 - k // 2 + GROUPS) % GROUPS

    def band_device(slot):
        return (2 * group - 2 + slot + DEVICES) % DEVICES

    return sec, me, group_device, band_device


def swap_rows(rows_ref, parts_ref, rows_in, parts_in, sems):
    sec, me, group_device, band_device = regrid_peers()

    for k in range(SLOTS):
        target = group_device(k)
        slot = me % 2 + 2 * (k // 2)

        @pl.when(target != me)
        def _():
            remote(
                rows_ref.at[k % 2], rows_in.at[slot], sems.at[0, k], sems.at[1, slot], target
            ).start()

        @pl.when(target == me)
        def _():
            rows_in[slot] = rows_ref[k % 2]

        band = band_device(k)
        place = (k // 2) * 2 + sec

        @pl.when(band != me)
        def _():
            remote(
                parts_ref.at[k], parts_in.at[place], sems.at[2, k], sems.at[3, place], band
            ).start()

        @pl.when(band == me)
        def _():
            parts_in[place] = parts_ref[k]

    for k in range(SLOTS):

        @pl.when(band_device(k) != me)
        def _():
            remote(rows_ref.at[0], rows_in.at[k], sems.at[0, k], sems.at[1, k], me).wait_recv()
            remote(parts_ref.at[k], parts_in.at[k], sems.at[2, k], sems.at[3, k], me).wait_send()

        @pl.when(group_device(k) != me)
        def _():
            remote(rows_ref.at[0], rows_in.at[k], sems.at[0, k], sems.at[1, k], me).wait_send()
            remote(parts_ref.at[k], parts_in.at[k], sems.at[2, k], sems.at[3, k], me).wait_recv()


def regrid_kernel(
    rows_ref, parts_ref, gathered_ref, summed_ref, rows_in, parts_in, sems
):
    _, me, group_device, band_device = regrid_peers()
    barrier = pltpu.get_barrier_semaphore()

    mine = me * 0
    for k in range(SLOTS):
        for peer in (group_device(k), band_device(k)):
            mine = mine + jnp.where(peer == me, 1, 0)

            @pl.when(peer != me)
            def _():
                pl.semaphore_signal(barrier, inc=1, device_id=peer, device_id_type=LOGICAL)

    pl.semaphore_wait(barrier, 2 * SLOTS - mine)

    swap_rows(rows_ref, parts_ref, rows_in, parts_in, sems)
    gathered_ref[...] = rows_in[...]
    for half in range(2):
        total = parts_in[half]
        for k in range(1, 4):
            total = total + parts_in[2 * k + half]
        summed_ref[half] = total


def regrid(rows, parts, number):
    _, r, lanes = rows.shape
    _, q, _ = parts.shape
    vmem = pl.BlockSpec(memory_space=pltpu.VMEM)
    return pl.pallas_call(
        regrid_kernel,
        out_shape=(
            jax.ShapeDtypeStruct((SLOTS, r, lanes), jnp.float32),
            jax.ShapeDtypeStruct((2, q, lanes), jnp.float32),
        ),
        in_specs=[vmem, vmem],
        out_specs=(vmem, vmem),
        scratch_shapes=[
            pltpu.VMEM((SLOTS, r, lanes), jnp.float32),
            pltpu.VMEM((SLOTS, q, lanes), jnp.float32),
            pltpu.SemaphoreType.DMA((4, SLOTS)),
        ],
        compiler_params=pltpu.CompilerParams(collective_id=number, has_side_effects=True),
        name=f"regrid_{number}",
    )(rows, parts)


X = 144
CHUNKS = 5
ROWS = 8
WIDE = 736
EDGE = 8
CELL = 128
TAPS = 7
REACH = 3
ALON = 360


def spread_taps(bands, taps_ref, layer, flipped):
    eye = lax.broadcasted_iota(jnp.int32, (CELL, CELL), 0) == lax.broadcasted_iota(
        jnp.int32, (CELL, CELL), 1
    )

    def one(v, carry):
        for u in range(TAPS):
            if flipped:
                row = taps_ref[layer, pl.ds((TAPS - 1 - u) * TAPS + (TAPS - 1) - v, 1), :]
            else:
                row = taps_ref[layer, pl.ds(u * TAPS + v, 1), :]
            block = jnp.where(eye, row, 0.0).astype(jnp.bfloat16)
            for q in range(2):
                bands[v, pl.ds((u + q) * CELL, CELL), pl.ds(q * CELL, CELL)] = block
        return carry

    lax.fori_loop(0, TAPS, one, 0)


def convolve(window, bands, sums, x0):
    total = None
    for v in range(TAPS):
        rows = [
            window[r, pl.ds(x0 + EDGE - REACH + v, X), :].astype(jnp.bfloat16)
            for r in range(ROWS + 2 * REACH)
        ]
        left = jnp.concatenate(
            [jnp.concatenate(rows[2 * p : 2 * p + 8], axis=1) for p in range(ROWS // 2)], axis=0
        )
        part = jnp.dot(left, bands[v], preferred_element_type=jnp.float32)
        total = part if total is None else total + part
    sums[...] = total


def normalized(hidden):
    center = hidden - jnp.mean(hidden, axis=-1, keepdims=True)
    rstd = lax.rsqrt(jnp.mean(center * center, axis=-1, keepdims=True) + 1e-06)
    return center * rstd, rstd


GELU_A = 0.7978845608028654
GELU_B = GELU_A * 0.044715


def gelu_pair(v):
    square = v * v
    w = 0.5 + 0.5 * jnp.tanh(v * (GELU_A + GELU_B * square))
    value = v * w
    slope = w + value * (1.0 - w) * (2.0 * GELU_A + (6.0 * GELU_B) * square)
    return value, slope


def split(values):
    high = values.astype(jnp.bfloat16)
    return high, (values - high.astype(jnp.float32)).astype(jnp.bfloat16)


def dot32(a, b):
    return jnp.dot(a, b, preferred_element_type=jnp.float32)


def dot_t(a, b):
    return lax.dot_general(a, b, (((1,), (1,)), ((), ())), preferred_element_type=jnp.float32)


def ocean_kernel(
    linked,
    state_ref,
    mask_ref,
    cot_ref,
    taps_ref,
    gain_ref,
    expand_ref,
    project_ref,
    atmosphere_ref,
    atmosphere_cot_ref,
    spectrum_ref,
    wave_ref,
    wave_t_ref,
    forward_ref,
    inverse_ref,
    mix_ref,
    embed_rows_ref,
    group_ref,
    to_ocean_ref,
    to_atmosphere_ref,
    surface_embed_ref,
    surface_read_ref,
    flux_read_ref,
    next_ref,
    grad_ref,
    atmosphere_next_ref,
    input_adj_ref,
    win_a,
    win_b,
    bands,
    sums,
    unit_0,
    rstd_0,
    slope_0,
    unit_1,
    rstd_1,
    before,
    active,
    out_rows,
    in_rows,
    in_cols,
    row_sems,
    col_sems,
    leaving,
    landed,
    swap_sems,
    flux_rows,
    coarse_rows,
    rows_out,
    parts_out,
    rows_in,
    parts_in,
    regrid_sems,
):
    sec = lax.axis_index("sec") if linked else 0
    tile = lax.axis_index("tile") if linked else 0
    last_tile = GROUPS - 1 if linked else 0
    me = sec * GROUPS + tile
    side = (1 - sec) * GROUPS + tile
    windows = (win_a, win_b)

    if linked:
        barrier = pltpu.get_barrier_semaphore()

        def greet(i, carry):
            pl.semaphore_signal(
                barrier, inc=1, device_id=(me + i) % DEVICES, device_id_type=LOGICAL
            )
            return carry

        lax.fori_loop(1, DEVICES, greet, 0)

    zero_rows = jnp.zeros((REACH, WIDE, CELL), jnp.float32)

    @pl.when(tile == 0)
    def _():
        for w in windows:
            w[0:REACH] = zero_rows

    @pl.when(tile == last_tile)
    def _():
        for w in windows:
            w[REACH + ROWS :] = zero_rows

    if not linked:
        for w in windows:
            w[:, 0:EDGE] = jnp.zeros((14, EDGE, CELL), jnp.float32)
            w[:, WIDE - EDGE :] = jnp.zeros((14, EDGE, CELL), jnp.float32)
    for v in range(TAPS):
        bands[v, 0:CELL, CELL:] = jnp.zeros((CELL, CELL), jnp.bfloat16)
        bands[v, 7 * CELL :, :CELL] = jnp.zeros((CELL, CELL), jnp.bfloat16)

    if linked:
        pl.semaphore_wait(barrier, DEVICES - 1)

    def put_blocks(x, values):
        for j in range(6):
            leaving[x, pl.ds(j, DEVICES, stride=8), :] = values[:, j * CELL : (j + 1) * CELL]
        if not linked:
            return

        def send(i, carry):
            peer = (me + i) % DEVICES
            remote(
                leaving.at[x, pl.ds(pl.multiple_of(peer * 8, 8), 8)],
                landed.at[x, pl.ds(pl.multiple_of(me * 8, 8), 8)],
                swap_sems.at[0, x],
                swap_sems.at[1, x],
                peer,
            ).start()
            return carry

        lax.fori_loop(1, DEVICES, send, 0)
        mine = pl.ds(pl.multiple_of(me * 8, 8), 8)
        landed[x, mine, :] = leaving[x, mine, :]

    def take_blocks(x):
        source = landed
        if linked:
            every = landed.at[x, pl.ds(0, (DEVICES - 1) * 8)]
            pltpu.make_async_copy(every, every, swap_sems.at[1, x]).wait()
            pltpu.make_async_copy(every, every, swap_sems.at[0, x]).wait()
        else:
            source = leaving
        return jnp.concatenate(
            [source[x, pl.ds(j, DEVICES, stride=8), :] for j in range(6)], axis=1
        ).astype(jnp.bfloat16)

    def rounded(values):
        return values.astype(jnp.bfloat16).astype(jnp.float32)

    half_c = 3 * CELL

    def spectral():
        coefficient = dot32(forward_ref[...], take_blocks(0)).astype(jnp.bfloat16)
        real, imag = (coefficient[:, :half_c], coefficient[:, half_c:])
        mixed = jnp.concatenate(
            [
                dot32(real, mix_ref[0]) - dot32(imag, mix_ref[1]),
                dot32(imag, mix_ref[0]) + dot32(real, mix_ref[1]),
            ],
            axis=1,
        ).astype(jnp.bfloat16)
        put_blocks(1, rounded(dot32(inverse_ref[...], mixed)))

    def respond():
        returned = take_blocks(1)
        returned = jnp.concatenate([returned[:, :half_c], returned[:, half_c:]], axis=0)
        parts = []
        for j in range(3):
            cols = pl.ds(j * CELL, CELL)
            response = dot32(wave_ref[...], returned[:, j * CELL : (j + 1) * CELL])
            value, slope = gelu_pair(response)
            atmosphere_next_ref[:, cols] = (
                atmosphere_ref[:, cols].astype(jnp.float32) + value
            ).astype(jnp.bfloat16)
            response_adj = (slope * atmosphere_cot_ref[:, cols].astype(jnp.float32)).astype(
                jnp.bfloat16
            )
            parts.append(dot32(wave_t_ref[...], response_adj))
        put_blocks(
            2,
            rounded(
                jnp.concatenate([p[:DEVICES] for p in parts] + [p[DEVICES:] for p in parts], axis=1)
            ),
        )

    def dot_first(a, b):
        return lax.dot_general(
            a, b, (((0,), (0,)), ((), ())), preferred_element_type=jnp.float32
        )

    def spectral_back():
        mixed_adj = dot_first(inverse_ref[...], take_blocks(2)).astype(jnp.bfloat16)
        real, imag = (mixed_adj[:, :half_c], mixed_adj[:, half_c:])
        coefficient_adj = jnp.concatenate(
            [
                dot_t(real, mix_ref[0]) + dot_t(imag, mix_ref[1]),
                dot_t(imag, mix_ref[0]) - dot_t(real, mix_ref[1]),
            ],
            axis=1,
        ).astype(jnp.bfloat16)
        put_blocks(3, rounded(dot_first(forward_ref[...], coefficient_adj)))

    def absorb():
        spectrum_adj = take_blocks(3)
        spectrum_adj = jnp.concatenate([spectrum_adj[:, :half_c], spectrum_adj[:, half_c:]], axis=0)
        for j in range(3):
            cols = pl.ds(j * CELL, CELL)
            input_adj_ref[:, cols] = atmosphere_cot_ref[:, cols].astype(jnp.float32) + dot32(
                wave_ref[...], spectrum_adj[:, j * CELL : (j + 1) * CELL]
            )

    def row_copy(e, way, c, peer):
        x0 = pl.multiple_of(c * X, 16)
        return remote(
            out_rows.at[e, pl.ds(0 if way == 0 else ROWS - REACH, REACH), pl.ds(x0, X)],
            in_rows.at[e, way, :, pl.ds(x0, X)],
            row_sems.at[0, e, way, c],
            row_sems.at[1, e, way, c],
            peer,
        )

    def col_copy(e, edge, part, peer):
        source = windows[e % 2]
        first, size, place = ((0, ROWS, REACH), (0, REACH, REACH + ROWS), (ROWS - REACH, REACH, 0))[
            part
        ]
        return remote(
            source.at[
                pl.ds(REACH + first, size), pl.ds(EDGE if edge == 0 else WIDE - 2 * EDGE, EDGE)
            ],
            in_cols.at[e, edge, pl.ds(place, size)],
            col_sems.at[0, e, edge, part],
            col_sems.at[1, e, edge, part],
            peer,
        )

    def send_chunk(e, k, c):
        if not linked:
            return

        @pl.when(tile > 0)
        def _():
            row_copy(e, 0, c, me - 1).start()

        @pl.when(tile < last_tile)
        def _():
            row_copy(e, 1, c, me + 1).start()

        for edge in range(2):

            @pl.when(k == edge)
            def _():
                col_copy(e, edge, 0, side).start()

                @pl.when(tile > 0)
                def _():
                    col_copy(e, edge, 1, side - 1).start()

                @pl.when(tile < last_tile)
                def _():
                    col_copy(e, edge, 2, side + 1).start()

    def take_rows(e, c):
        x0 = pl.multiple_of(c * X, 16)
        window = windows[e % 2]

        @pl.when(tile > 0)
        def _():
            row_copy(e, 1, c, me - 1).wait_recv()
            window[0:REACH, pl.ds(EDGE + x0, X), :] = in_rows[e, 1, :, pl.ds(x0, X), :].astype(
                jnp.float32
            )

        @pl.when(tile < last_tile)
        def _():
            row_copy(e, 0, c, me + 1).wait_recv()
            window[REACH + ROWS :, pl.ds(EDGE + x0, X), :] = in_rows[
                e, 0, :, pl.ds(x0, X), :
            ].astype(jnp.float32)

    def take_cols(e, edge):
        window = windows[e % 2]
        at = pl.ds(0 if edge == 1 else WIDE - EDGE, EDGE)
        col_copy(e, edge, 0, side).wait_recv()
        window[pl.ds(REACH, ROWS), at, :] = in_cols[e, edge, pl.ds(REACH, ROWS)]

        @pl.when(tile > 0)
        def _():
            col_copy(e, edge, 2, side - 1).wait_recv()
            window[pl.ds(0, REACH), at, :] = in_cols[e, edge, pl.ds(0, REACH)]

        @pl.when(tile < last_tile)
        def _():
            col_copy(e, edge, 1, side + 1).wait_recv()
            window[pl.ds(REACH + ROWS, REACH), at, :] = in_cols[
                e, edge, pl.ds(REACH + ROWS, REACH)
            ]

    def take_halo(e, k):
        if not linked:
            return

        @pl.when(k == 0)
        def _():
            take_rows(e, 0)
            take_rows(e, 1)
            take_cols(e, 1)

        @pl.when(k == 1)
        def _():
            take_rows(e, CHUNKS - 1)
            take_rows(e, CHUNKS - 2)
            take_cols(e, 0)

        @pl.when(k == 2)
        def _():
            take_rows(e, CHUNKS // 2)

    def sent(e):
        if not linked:
            return

        def one(c, carry):
            @pl.when(tile > 0)
            def _():
                row_copy(e, 0, c, me - 1).wait_send()

            @pl.when(tile < last_tile)
            def _():
                row_copy(e, 1, c, me + 1).wait_send()

            return carry

        lax.fori_loop(0, CHUNKS, one, 0)
        for edge in range(2):
            col_copy(e, edge, 0, side).wait_send()

            @pl.when(tile > 0)
            def _():
                col_copy(e, edge, 1, side - 1).wait_send()

            @pl.when(tile < last_tile)
            def _():
                col_copy(e, edge, 2, side + 1).wait_send()

    def chunk_of(k):
        return jnp.where(k % 2 == 0, k // 2, CHUNKS - 1 - k // 2)

    def keep(e, y, x0, value):
        windows[e % 2][y + REACH, pl.ds(EDGE + x0, X), :] = value.astype(jnp.float32)
        if linked:
            out_rows[e, y, pl.ds(x0, X), :] = value

    half_cells = ROWS // 2 * X

    def origin(k):
        return pl.multiple_of(chunk_of(k) * X, 16)

    def conv(e, k):
        convolve(windows[e % 2], bands, sums, origin(k))

    def halves(one):
        def half(q, inner):
            one(q, pl.ds(pl.multiple_of(q * half_cells, 16), half_cells))
            return inner

        lax.fori_loop(0, 2, half, 0)

    def half_of(q):
        return sums[:, pl.ds(pl.multiple_of(q * CELL, CELL), CELL)]

    def row_part(values, p):
        return values[p * X : (p + 1) * X]

    def stacked(read):
        return jnp.concatenate([read(p) for p in range(ROWS // 2)], axis=0)

    def forward_stage(e, layer, keep_norm, keep_slope, finish):
        def normalize(k):
            def one(q, at):
                unit, rstd = normalized(half_of(q))
                keep_norm(k, at, unit, rstd)
                dense = (unit * gain_ref[layer : layer + 1, :]).astype(jnp.bfloat16)
                before[at, :] = dot32(dense, expand_ref[layer])

            halves(one)

        def activate(k, y):
            at = pl.ds(pl.multiple_of(y * X, 16), X)
            value, slope = gelu_pair(before[at, :])
            active[at, :] = value.astype(jnp.bfloat16)
            keep_slope(k, at, slope)

        def close(k):
            def one(q, at):
                finish(k, q, at, dot32(active[at, :], project_ref[layer]))

            halves(one)
            send_chunk(e + 1, k, chunk_of(k))

        def chunk(k, carry):
            take_halo(e, k)
            conv(e, k)
            normalize(k)

            def piece(y, inner):
                activate(k, y)
                return inner

            lax.fori_loop(0, ROWS, piece, 0)
            close(k)
            return carry

        lax.fori_loop(0, CHUNKS, chunk, 0)
        sent(e)

    def backward_stage(e, one, after=None):
        def chunk(k, carry):
            take_halo(e, k)
            conv(e, k)
            halves(lambda q, at: one(k, q, at))
            if after is not None:
                after(k)
            if e < 3:
                send_chunk(e + 1, k, chunk_of(k))
            return carry

        lax.fori_loop(0, CHUNKS, chunk, 0)
        sent(e)

    def first(k, carry):
        c = chunk_of(k)
        x0 = pl.multiple_of(c * X, 16)

        def row(y, inner):
            keep(0, y, x0, state_ref[y, pl.ds(x0, X), :])
            return inner

        lax.fori_loop(0, ROWS, row, 0)
        send_chunk(0, k, c)
        return carry

    lax.fori_loop(0, CHUNKS, first, 0)
    put_blocks(0, spectrum_ref[...])

    def mask_of(y, x0):
        return mask_ref[y, pl.ds(x0, X), :].astype(jnp.float32)

    def own(e, y, x0):
        return windows[e % 2][y + REACH, pl.ds(EDGE + x0, X), :]

    spread_taps(bands, taps_ref, 0, False)

    def keep_norm_0(k, at, unit, rstd):
        c = chunk_of(k)
        unit_0[c, at, :] = unit
        rstd_0[c, at, :] = jnp.broadcast_to(rstd, unit.shape)

    def keep_slope_0(k, at, slope):
        slope_0[chunk_of(k), at, :] = slope.astype(jnp.bfloat16)

    def finish_0(k, q, at, update):
        x0 = origin(k)
        for p in range(ROWS // 2):
            y = 2 * p + q
            new = own(0, y, x0) + mask_of(y, x0) * row_part(update, p)
            keep(1, y, x0, new.astype(jnp.bfloat16))

    forward_stage(0, 0, keep_norm_0, keep_slope_0, finish_0)
    spectral()
    spread_taps(bands, taps_ref, 1, False)

    def adjoint(e, k, q, at, masked, slope, unit, rstd, layer):
        x0 = origin(k)
        active[at, :] = (slope * dot_t(masked, project_ref[layer])).astype(jnp.bfloat16)
        scaled = dot_t(active[at, :], expand_ref[layer]) * gain_ref[layer : layer + 1, :]
        inner = jnp.mean(scaled * unit, axis=-1, keepdims=True)
        result = rstd * (scaled - jnp.mean(scaled, axis=-1, keepdims=True) - unit * inner)
        for p in range(ROWS // 2):
            keep(e, 2 * p + q, x0, row_part(result, p).astype(jnp.bfloat16))

    def cot_of(y, x0):
        return cot_ref[y, pl.ds(x0, X), :].astype(jnp.float32)

    def keep_norm_1(k, at, unit, rstd):
        unit_1[at, :] = unit
        rstd_1[at, :] = jnp.broadcast_to(rstd, unit.shape)

    def keep_slope_1(k, at, slope):
        before[at, :] = slope

    def finish_1(k, q, at, update):
        x0 = origin(k)
        for p in range(ROWS // 2):
            y = 2 * p + q
            new = own(1, y, x0) + mask_of(y, x0) * row_part(update, p)
            next_ref[y, pl.ds(x0, X), :] = new.astype(jnp.bfloat16)
        masked = stacked(lambda p: mask_of(2 * p + q, x0) * cot_of(2 * p + q, x0))
        adjoint(
            2, k, q, at, masked.astype(jnp.bfloat16), before[at, :], unit_1[at, :], rstd_1[at, :], 1
        )

    forward_stage(1, 1, keep_norm_1, keep_slope_1, finish_1)
    respond()
    spread_taps(bands, taps_ref, 1, True)

    def backward_0(k, q, at):
        c, x0 = (chunk_of(k), origin(k))
        hid = half_of(q)
        parts = []
        for p in range(ROWS // 2):
            y = 2 * p + q
            cot = cot_of(y, x0) + row_part(hid, p)
            grad_ref[y, pl.ds(x0, X), :] = cot
            parts.append(mask_of(y, x0) * cot)
        masked = jnp.concatenate(parts, axis=0).astype(jnp.bfloat16)
        slope = slope_0[c, at, :].astype(jnp.float32)
        adjoint(3, k, q, at, masked, slope, unit_0[c, at, :], rstd_0[c, at, :], 0)

    backward_stage(2, backward_0)
    spectral_back()
    spread_taps(bands, taps_ref, 0, True)

    def last(k, q, at):
        x0 = origin(k)
        hid = half_of(q)
        for p in range(ROWS // 2):
            y = 2 * p + q
            grad_ref[y, pl.ds(x0, X), :] = grad_ref[y, pl.ds(x0, X), :] + row_part(hid, p)

    def gather_flux(k):
        x0 = origin(k)
        lanes = jnp.concatenate(
            [mask_of(y, x0) * grad_ref[y, pl.ds(x0, X), :] for y in range(ROWS)], axis=1
        )
        high, rest = split(lanes)
        flux_rows[pl.ds(x0, X), :] = dot32(high, embed_rows_ref[...]) + dot32(
            rest, embed_rows_ref[...]
        )

    backward_stage(3, last, gather_flux)
    absorb()
    half = ALON // 2
    high, rest = split(flux_rows[...])
    flux_by_row = dot_first(high, group_ref[...]) + dot_first(rest, group_ref[...])
    for slot in range(SLOTS):
        total = to_ocean_ref[slot, 0] * flux_by_row[0:8]
        for o in range(1, ROWS):
            total = total + to_ocean_ref[slot, o] * flux_by_row[8 * o : 8 * o + 8]
        parts_out[slot] = total
    embed_high, embed_rest = split(jnp.broadcast_to(surface_embed_ref[...], (8, half_c)))
    rows_out[...] = jnp.zeros((2, 1, LANES), jnp.float32)
    for h in range(2):
        high, rest = split(input_adj_ref[pl.ds(h * half, half), :])
        row = dot_t(embed_high, high) + dot_t(embed_rest, high) + dot_t(embed_high, rest)
        rows_out[h, :, 0:half] = row[0:1]
    swap_rows(rows_out, parts_out, rows_in, parts_in, regrid_sems)
    for o in range(ROWS):
        total = to_atmosphere_ref[0, o] * rows_in[0]
        for slot in range(1, SLOTS):
            total = total + to_atmosphere_ref[slot, o] * rows_in[slot]
        coarse_rows[o : o + 1, :] = total
    coarse_high, coarse_rest = split(coarse_rows[...])
    read = surface_read_ref[...] * 0.25
    row_number = lax.broadcasted_iota(jnp.int32, (ROWS, CELL), 0)

    def widen(o, carry):
        pick = jnp.where(row_number == o, 1.0, 0.0).astype(jnp.bfloat16)
        spread = dot32(group_ref[...], dot_first(coarse_high, pick).astype(jnp.bfloat16)) + dot32(
            group_ref[...], dot_first(coarse_rest, pick).astype(jnp.bfloat16)
        )
        grad_ref[o] = grad_ref[o] + mask_ref[o].astype(jnp.float32) * spread * read
        return carry

    lax.fori_loop(0, ROWS, widen, 0)
    flux_read_twice = jnp.concatenate([flux_read_ref[...], flux_read_ref[...]], axis=0)
    for h in range(2):
        total = parts_in[h]
        for k in range(1, 4):
            total = total + parts_in[2 * k + h]
        high, rest = split(total)
        from_flux = dot_first(
            jnp.concatenate([high.astype(jnp.float32), rest.astype(jnp.float32)], axis=0).astype(
                jnp.bfloat16
            ),
            flux_read_twice,
        )
        at = pl.ds(h * half, half)
        input_adj_ref[at, :] = input_adj_ref[at, :] + from_flux[:half]


def ocean(*operands, linked=True):
    vmem = pl.BlockSpec(memory_space=pltpu.VMEM)
    smem = pl.BlockSpec(memory_space=pltpu.SMEM)
    whole = (ROWS, CHUNKS * X, CELL)
    f32, bf16 = (jnp.float32, jnp.bfloat16)
    return pl.pallas_call(
        functools.partial(ocean_kernel, linked),
        out_shape=(
            jax.ShapeDtypeStruct(whole, bf16),
            jax.ShapeDtypeStruct(whole, f32),
            jax.ShapeDtypeStruct((ALON, 3 * CELL), bf16),
            jax.ShapeDtypeStruct((ALON, 3 * CELL), f32),
        ),
        in_specs=[vmem] * 17 + [smem] * 2 + [vmem] * 3,
        out_specs=(vmem,) * 4,
        scratch_shapes=[
            pltpu.VMEM((ROWS + 2 * REACH, WIDE, CELL), f32),
            pltpu.VMEM((ROWS + 2 * REACH, WIDE, CELL), f32),
            pltpu.VMEM((TAPS, 8 * CELL, 2 * CELL), bf16),
            pltpu.VMEM((ROWS // 2 * X, 2 * CELL), f32),
            pltpu.VMEM((CHUNKS, ROWS * X, CELL), f32),
            pltpu.VMEM((CHUNKS, ROWS * X, CELL), f32),
            pltpu.VMEM((CHUNKS, ROWS * X, 4 * CELL), bf16),
            pltpu.VMEM((ROWS * X, CELL), f32),
            pltpu.VMEM((ROWS * X, CELL), f32),
            pltpu.VMEM((ROWS * X, 4 * CELL), f32),
            pltpu.VMEM((ROWS * X, 4 * CELL), bf16),
            pltpu.VMEM((4, ROWS, CHUNKS * X, CELL), bf16),
            pltpu.VMEM((4, 2, REACH, CHUNKS * X, CELL), bf16),
            pltpu.VMEM((4, 2, ROWS + 2 * REACH, EDGE, CELL), f32),
            pltpu.SemaphoreType.DMA((2, 4, 2, CHUNKS)),
            pltpu.SemaphoreType.DMA((2, 4, 2, 3)),
            pltpu.VMEM((4, DEVICES * 8, CELL), f32),
            pltpu.VMEM((4, DEVICES * 8, CELL), f32),
            pltpu.SemaphoreType.DMA((2, 4)),
            pltpu.VMEM((CHUNKS * X, ROWS * SLOTS), f32),
            pltpu.VMEM((ROWS, LANES), f32),
            pltpu.VMEM((2, 1, LANES), f32),
            pltpu.VMEM((SLOTS, 8, LANES), f32),
            pltpu.VMEM((SLOTS, 1, LANES), f32),
            pltpu.VMEM((SLOTS, 8, LANES), f32),
            pltpu.SemaphoreType.DMA((4, SLOTS)),
        ],
        compiler_params=pltpu.CompilerParams(
            collective_id=6 if linked else None, has_side_effects=linked, vmem_limit_bytes=67000000
        ),
        name="ocean",
    )(*operands)


def wave_table():
    place = np.arange(ALON, dtype=np.int32)[:, None] * np.arange(DEVICES, dtype=np.int32)[None, :]
    phase = (place % ALON).astype(np.float32) * np.float32(2.0 * np.pi / ALON)
    both = np.concatenate([np.cos(phase), -np.sin(phase)], axis=1)
    return (both * np.sqrt(np.float32(2.0 / ALON))).astype(jnp.bfloat16)


def slot_weights(bands_row, blocks, group):
    slot = bands_row[:, None] - (2 * group - 2)
    onehot = (slot == jnp.arange(SLOTS, dtype=jnp.int32)[None, :]).astype(jnp.float32)
    return jnp.sum(onehot[:, :, None] * blocks[:, None, :], axis=0)


def padded_lanes(values):
    return jnp.pad(values, [(0, 0)] * (values.ndim - 1) + [(0, LANES - values.shape[-1])])


def per_device(
    atmosphere,
    ocean_state,
    land_mask,
    crossing_bands,
    ocean_regrid,
    atmosphere_regrid,
    surface_read,
    surface_embed,
    flux_read,
    flux_embed,
    legendre_forward,
    legendre_inverse,
    spectral_mix,
    conv_kernel,
    norm_gain,
    expand_weight,
    project_weight,
    atmosphere_cotangent,
    ocean_cotangent,
):
    lat_rows, lon_count, channels = atmosphere.shape
    ocean_rows, ocean_lon, ocean_channels = ocean_state.shape
    half = lon_count // lax.axis_size("sec")
    offset = lax.axis_index("sec") * half
    ratio = ocean_lon // half
    flux_count = flux_read.shape[1]
    highest = lax.Precision.HIGHEST
    mask_value = land_mask.astype(jnp.float32)
    group = lax.axis_index("tile")
    to_ocean = slot_weights(crossing_bands[0], ocean_regrid[0, :, :, 0], group)
    to_atmosphere = slot_weights(crossing_bands[0], atmosphere_regrid[0, :, 0, :], group)
    surface = jnp.dot(ocean_state, surface_read, preferred_element_type=jnp.float32)
    coarse = jnp.mean((mask_value * surface).reshape(ocean_rows, half, ratio), axis=2)
    flux = jnp.einsum(
        "hgc,cf->hfg",
        atmosphere.reshape(2, half, channels),
        flux_read,
        preferred_element_type=jnp.float32,
    )
    flux_rows, surface_rows = regrid(
        padded_lanes(flux),
        padded_lanes(jnp.dot(to_atmosphere, coarse, precision=highest))[:, None, :],
        0,
    )
    surface_atmosphere = surface_rows[:, 0, :half].reshape(1, lon_count)
    flux_ocean = jnp.einsum("so,sfg->ogf", to_ocean, flux_rows[:, :, :half], precision=highest)
    mixed_input = (
        atmosphere.astype(jnp.float32)
        + surface_atmosphere[:, :, None] * surface_embed[None, None, :]
    ).astype(jnp.bfloat16)
    table = wave_table()
    spectrum = jnp.einsum(
        "gk,gc->kc", jnp.asarray(table), mixed_input[0], preferred_element_type=jnp.float32
    )
    spectrum = spectrum.astype(jnp.bfloat16).astype(jnp.float32)
    spectrum = jnp.concatenate([spectrum[:DEVICES], spectrum[DEVICES:]], axis=1)
    forcing_coarse = jnp.einsum(
        "ogf,fc->ogc",
        flux_ocean,
        flux_embed.astype(jnp.float32),
        precision=highest,
    )
    forcing = jnp.broadcast_to(
        forcing_coarse[:, :, None, :], (ocean_rows, half, ratio, ocean_channels)
    ).reshape(ocean_rows, ocean_lon, ocean_channels)
    state = (ocean_state.astype(jnp.float32) + mask_value[:, :, None] * forcing).astype(
        jnp.bfloat16
    )
    layer_count = conv_kernel.shape[0]
    embed_rows = (
        jnp.eye(ocean_rows, dtype=flux_embed.dtype)[:, None, :, None]
        * flux_embed.T[None, :, None, :]
    ).reshape(ocean_rows * ocean_channels, ocean_rows * flux_count)
    grouping = np.arange(ocean_lon)[:, None] // ratio == np.arange(LANES)[None, :]
    grouping = grouping.astype(jnp.bfloat16)
    state, ocean_grad, atmosphere_next, atmosphere_grad = ocean(
        state,
        jnp.broadcast_to(mask_value[:, :, None], state.shape).astype(jnp.bfloat16),
        ocean_cotangent,
        conv_kernel.reshape(layer_count, TAPS * TAPS, CELL).astype(jnp.float32),
        norm_gain,
        expand_weight,
        project_weight,
        mixed_input[0],
        atmosphere_cotangent[0],
        spectrum,
        jnp.asarray(table),
        jnp.asarray(np.ascontiguousarray(table.T)),
        legendre_forward[0],
        legendre_inverse[0],
        spectral_mix,
        embed_rows,
        jnp.asarray(grouping),
        to_ocean,
        to_atmosphere,
        surface_embed[None, :],
        surface_read.astype(jnp.float32)[None, :],
        flux_read.T,
    )
    return (atmosphere_next[None], state, atmosphere_grad[None], ocean_grad)


def solution(mesh):
    placed = (
        P(SEC_TILE, None, None),
        P(TILE, "sec", None),
        P(TILE, "sec"),
        P(TILE, None),
        P(TILE, None, None, None),
        P(TILE, None, None, None),
        P(),
        P(),
        P(),
        P(),
        P(SEC_TILE, None, None),
        P(SEC_TILE, None, None),
        P(),
        P(),
        P(),
        P(),
        P(),
        P(SEC_TILE, None, None),
        P(TILE, "sec", None),
    )
    return jax.shard_map(
        per_device,
        mesh=mesh,
        in_specs=placed,
        out_specs=(
            P(SEC_TILE, None, None),
            P(TILE, "sec", None),
            P(SEC_TILE, None, None),
            P(TILE, "sec", None),
        ),
        check_vma=False,
    )
```

```python
import functools

import jax
import jax.numpy as jnp
import numpy as np
from jax import lax
from jax.experimental import pallas as pl
from jax.experimental.pallas import tpu as pltpu
from jax.sharding import PartitionSpec as P

SEC_TILE = ("sec", "tile")
TILE = "tile"
LOGICAL = pl.DeviceIdType.LOGICAL
DEVICES = 128
GROUPS = 64
SLOTS = 8
LANES = 256
X = 144
CHUNKS = 5
ROWS = 8
WIDE = 736
EDGE = 8
CELL = 128
TAPS = 7
REACH = 3
ALON = 360


def remote(src, dst, send_sem, recv_sem, device):
    return pltpu.make_async_remote_copy(
        src_ref=src,
        dst_ref=dst,
        send_sem=send_sem,
        recv_sem=recv_sem,
        device_id=device,
        device_id_type=LOGICAL,
    )


def regrid_peers():
    sec = lax.axis_index("sec")
    group = lax.axis_index("tile")
    me = sec * GROUPS + group

    def group_device(k):
        return (k % 2) * GROUPS + (me // 2 + 1 - k // 2 + GROUPS) % GROUPS

    def band_device(slot):
        return (2 * group - 2 + slot + DEVICES) % DEVICES

    return sec, me, group_device, band_device


def send_rows(rows_ref, parts_ref, rows_in, parts_in, sems):
    sec, me, group_device, band_device = regrid_peers()

    for k in range(SLOTS):
        target = group_device(k)
        slot = me % 2 + 2 * (k // 2)

        @pl.when(target != me)
        def _():
            remote(
                rows_ref.at[k % 2], rows_in.at[slot], sems.at[0, k], sems.at[1, slot], target
            ).start()

        @pl.when(target == me)
        def _():
            rows_in[slot] = rows_ref[k % 2]

        band = band_device(k)
        place = (k // 2) * 2 + sec

        @pl.when(band != me)
        def _():
            remote(
                parts_ref.at[k], parts_in.at[place], sems.at[2, k], sems.at[3, place], band
            ).start()

        @pl.when(band == me)
        def _():
            parts_in[place] = parts_ref[k]


def wait_rows(rows_ref, parts_ref, rows_in, parts_in, sems):
    _, me, group_device, band_device = regrid_peers()

    for k in range(SLOTS):

        @pl.when(band_device(k) != me)
        def _():
            remote(rows_ref.at[0], rows_in.at[k], sems.at[0, k], sems.at[1, k], me).wait_recv()
            remote(parts_ref.at[k], parts_in.at[k], sems.at[2, k], sems.at[3, k], me).wait_send()

        @pl.when(group_device(k) != me)
        def _():
            remote(rows_ref.at[0], rows_in.at[k], sems.at[0, k], sems.at[1, k], me).wait_send()
            remote(parts_ref.at[k], parts_in.at[k], sems.at[2, k], sems.at[3, k], me).wait_recv()


def spread_taps(bands, taps_ref, layer, flipped):
    eye = lax.broadcasted_iota(jnp.int32, (CELL, CELL), 0) == lax.broadcasted_iota(
        jnp.int32, (CELL, CELL), 1
    )

    def one(v, carry):
        for u in range(TAPS):
            if flipped:
                row = taps_ref[layer, pl.ds((TAPS - 1 - u) * TAPS + (TAPS - 1) - v, 1), :]
            else:
                row = taps_ref[layer, pl.ds(u * TAPS + v, 1), :]
            block = jnp.where(eye, row, 0.0).astype(jnp.bfloat16)
            for q in range(2):
                bands[v, pl.ds((u + q) * CELL, CELL), pl.ds(q * CELL, CELL)] = block
        return carry

    lax.fori_loop(0, TAPS, one, 0)


VECTOR_TAPS = 2
STRIP = 16


def tap_row(taps_ref, layer, flipped, u, v):
    at = (TAPS - 1 - u) * TAPS + TAPS - 1 - v if flipped else u * TAPS + v
    return taps_ref[layer, at : at + 1, :]


def convolve(window, bands, sums, x0, taps_ref, layer, flipped):
    count = TAPS - VECTOR_TAPS
    strips = X // STRIP
    total = None
    done = 0
    for v in range(count):
        rows = [
            window[r, pl.ds(x0 + EDGE - REACH + v, X), :].astype(jnp.bfloat16)
            for r in range(ROWS + 2 * REACH)
        ]
        left = jnp.concatenate(
            [jnp.concatenate(rows[2 * p : 2 * p + 8], axis=1) for p in range(ROWS // 2)], axis=0
        )
        part = jnp.dot(left, bands[v], preferred_element_type=jnp.float32)
        total = part if total is None else total + part
        upto = strips * (v + 1) // count
        for strip in range(done, upto):
            parts = [None] * ROWS
            for w in range(count, TAPS):
                for r in range(ROWS + 2 * REACH):
                    cells = window[r, pl.ds(x0 + EDGE - REACH + w + strip * STRIP, STRIP), :]
                    for y in range(max(0, r - TAPS + 1), min(ROWS, r + 1)):
                        term = cells * tap_row(taps_ref, layer, flipped, r - y, w)
                        parts[y] = term if parts[y] is None else parts[y] + term
            for y in range(ROWS):
                sums[
                    pl.ds(y // 2 * X + strip * STRIP, STRIP), y % 2 * CELL : (y % 2 + 1) * CELL
                ] = parts[y]
        done = upto
    sums[...] = sums[...] + total


def normalized(hidden):
    center = hidden - jnp.mean(hidden, axis=-1, keepdims=True)
    rstd = lax.rsqrt(jnp.mean(center * center, axis=-1, keepdims=True) + 1e-06)
    return center * rstd, rstd


GELU_A = 0.7978845608028654
GELU_B = GELU_A * 0.044715


def gelu_pair(v):
    square = v * v
    w = 0.5 + 0.5 * jnp.tanh(v * (GELU_A + GELU_B * square))
    value = v * w
    slope = w + value * (1.0 - w) * (2.0 * GELU_A + (6.0 * GELU_B) * square)
    return value, slope


def split(values):
    high = values.astype(jnp.bfloat16)
    return high, (values - high.astype(jnp.float32)).astype(jnp.bfloat16)


def dot32(a, b):
    return jnp.dot(a, b, preferred_element_type=jnp.float32)


def dot_t(a, b):
    return lax.dot_general(a, b, (((1,), (1,)), ((), ())), preferred_element_type=jnp.float32)


def ocean_kernel(
    linked,
    state_ref,
    land_ref,
    cot_ref,
    taps_ref,
    gain_ref,
    expand_ref,
    project_ref,
    raw_ref,
    atmosphere_cot_ref,
    wave_ref,
    wave_t_ref,
    forward_ref,
    inverse_ref,
    mix_ref,
    embed_rows_ref,
    read_rows_ref,
    flux_embed_ref,
    group_ref,
    to_ocean_ref,
    to_atmosphere_ref,
    surface_embed_ref,
    surface_read_ref,
    flux_read_ref,
    next_ref,
    grad_ref,
    atmosphere_next_ref,
    input_adj_ref,
    win_a,
    win_b,
    bands,
    sums,
    unit_0,
    rstd_0,
    slope_0,
    unit_1,
    rstd_1,
    before,
    active,
    out_rows,
    in_rows,
    in_cols,
    row_sems,
    col_sems,
    leaving,
    landed,
    swap_sems,
    flux_rows,
    coarse_rows,
    rows_out,
    parts_out,
    rows_in,
    parts_in,
    regrid_sems,
    mask_ref,
    atmosphere_ref,
    first_rows_out,
    first_parts_out,
    first_rows_in,
    first_parts_in,
    first_sems,
    flux_cells,
):
    sec = lax.axis_index("sec") if linked else 0
    tile = lax.axis_index("tile") if linked else 0
    last_tile = GROUPS - 1 if linked else 0
    me = sec * GROUPS + tile
    side = (1 - sec) * GROUPS + tile
    windows = (win_a, win_b)

    if linked:
        barrier = pltpu.get_barrier_semaphore()

        def greet(i, carry):
            pl.semaphore_signal(
                barrier, inc=1, device_id=(me + i) % DEVICES, device_id_type=LOGICAL
            )
            return carry

        lax.fori_loop(1, DEVICES, greet, 0)

    zero_rows = jnp.zeros((REACH, WIDE, CELL), jnp.float32)

    @pl.when(tile == 0)
    def _():
        for w in windows:
            w[0:REACH] = zero_rows

    @pl.when(tile == last_tile)
    def _():
        for w in windows:
            w[REACH + ROWS :] = zero_rows

    if not linked:
        for w in windows:
            w[:, 0:EDGE] = jnp.zeros((14, EDGE, CELL), jnp.float32)
            w[:, WIDE - EDGE :] = jnp.zeros((14, EDGE, CELL), jnp.float32)
    for v in range(TAPS):
        bands[v, 0:CELL, CELL:] = jnp.zeros((CELL, CELL), jnp.bfloat16)
        bands[v, 7 * CELL :, :CELL] = jnp.zeros((CELL, CELL), jnp.bfloat16)


    def put_blocks(x, values):
        for j in range(6):
            leaving[x, pl.ds(j, DEVICES, stride=8), :] = values[:, j * CELL : (j + 1) * CELL]
        if not linked:
            return

        def send(i, carry):
            peer = (me + i) % DEVICES
            remote(
                leaving.at[x, pl.ds(pl.multiple_of(peer * 8, 8), 8)],
                landed.at[x, pl.ds(pl.multiple_of(me * 8, 8), 8)],
                swap_sems.at[0, x],
                swap_sems.at[1, x],
                peer,
            ).start()
            return carry

        lax.fori_loop(1, DEVICES, send, 0)
        mine = pl.ds(pl.multiple_of(me * 8, 8), 8)
        landed[x, mine, :] = leaving[x, mine, :]

    def take_blocks(x):
        source = landed
        if linked:
            every = landed.at[x, pl.ds(0, (DEVICES - 1) * 8)]
            pltpu.make_async_copy(every, every, swap_sems.at[1, x]).wait()
            pltpu.make_async_copy(every, every, swap_sems.at[0, x]).wait()
        else:
            source = leaving
        return jnp.concatenate(
            [source[x, pl.ds(j, DEVICES, stride=8), :] for j in range(6)], axis=1
        ).astype(jnp.bfloat16)

    def rounded(values):
        return values.astype(jnp.bfloat16).astype(jnp.float32)

    half_c = 3 * CELL

    def spectral():
        coefficient = dot32(forward_ref[...], take_blocks(0)).astype(jnp.bfloat16)
        real, imag = (coefficient[:, :half_c], coefficient[:, half_c:])
        mixed = jnp.concatenate(
            [
                dot32(real, mix_ref[0]) - dot32(imag, mix_ref[1]),
                dot32(imag, mix_ref[0]) + dot32(real, mix_ref[1]),
            ],
            axis=1,
        ).astype(jnp.bfloat16)
        put_blocks(1, rounded(dot32(inverse_ref[...], mixed)))

    def respond():
        returned = take_blocks(1)
        returned = jnp.concatenate([returned[:, :half_c], returned[:, half_c:]], axis=0)
        parts = []
        for j in range(3):
            cols = pl.ds(j * CELL, CELL)
            response = dot32(wave_ref[...], returned[:, j * CELL : (j + 1) * CELL])
            value, slope = gelu_pair(response)
            atmosphere_next_ref[:, cols] = (
                atmosphere_ref[:, cols].astype(jnp.float32) + value
            ).astype(jnp.bfloat16)
            response_adj = (slope * atmosphere_cot_ref[:, cols].astype(jnp.float32)).astype(
                jnp.bfloat16
            )
            parts.append(dot32(wave_t_ref[...], response_adj))
        put_blocks(
            2,
            rounded(
                jnp.concatenate([p[:DEVICES] for p in parts] + [p[DEVICES:] for p in parts], axis=1)
            ),
        )

    def dot_first(a, b):
        return lax.dot_general(
            a, b, (((0,), (0,)), ((), ())), preferred_element_type=jnp.float32
        )

    def spectral_back():
        mixed_adj = dot_first(inverse_ref[...], take_blocks(2)).astype(jnp.bfloat16)
        real, imag = (mixed_adj[:, :half_c], mixed_adj[:, half_c:])
        coefficient_adj = jnp.concatenate(
            [
                dot_t(real, mix_ref[0]) + dot_t(imag, mix_ref[1]),
                dot_t(imag, mix_ref[0]) - dot_t(real, mix_ref[1]),
            ],
            axis=1,
        ).astype(jnp.bfloat16)
        put_blocks(3, rounded(dot_first(forward_ref[...], coefficient_adj)))

    def absorb():
        spectrum_adj = take_blocks(3)
        spectrum_adj = jnp.concatenate([spectrum_adj[:, :half_c], spectrum_adj[:, half_c:]], axis=0)
        for j in range(3):
            cols = pl.ds(j * CELL, CELL)
            input_adj_ref[:, cols] = atmosphere_cot_ref[:, cols].astype(jnp.float32) + dot32(
                wave_ref[...], spectrum_adj[:, j * CELL : (j + 1) * CELL]
            )

    def row_copy(e, way, c, peer):
        x0 = pl.multiple_of(c * X, 16)
        return remote(
            out_rows.at[e, pl.ds(0 if way == 0 else ROWS - REACH, REACH), pl.ds(x0, X)],
            in_rows.at[e, way, :, pl.ds(x0, X)],
            row_sems.at[0, e, way, c],
            row_sems.at[1, e, way, c],
            peer,
        )

    def col_copy(e, edge, part, peer):
        source = windows[e % 2]
        first, size, place = ((0, ROWS, REACH), (0, REACH, REACH + ROWS), (ROWS - REACH, REACH, 0))[
            part
        ]
        return remote(
            source.at[
                pl.ds(REACH + first, size), pl.ds(EDGE if edge == 0 else WIDE - 2 * EDGE, EDGE)
            ],
            in_cols.at[e, edge, pl.ds(place, size)],
            col_sems.at[0, e, edge, part],
            col_sems.at[1, e, edge, part],
            peer,
        )

    def send_chunk(e, k, c):
        if not linked:
            return

        @pl.when(tile > 0)
        def _():
            row_copy(e, 0, c, me - 1).start()

        @pl.when(tile < last_tile)
        def _():
            row_copy(e, 1, c, me + 1).start()

        for edge in range(2):

            @pl.when(k == edge)
            def _():
                col_copy(e, edge, 0, side).start()

                @pl.when(tile > 0)
                def _():
                    col_copy(e, edge, 1, side - 1).start()

                @pl.when(tile < last_tile)
                def _():
                    col_copy(e, edge, 2, side + 1).start()

    def take_rows(e, c):
        x0 = pl.multiple_of(c * X, 16)
        window = windows[e % 2]

        @pl.when(tile > 0)
        def _():
            row_copy(e, 1, c, me - 1).wait_recv()
            window[0:REACH, pl.ds(EDGE + x0, X), :] = in_rows[e, 1, :, pl.ds(x0, X), :].astype(
                jnp.float32
            )

        @pl.when(tile < last_tile)
        def _():
            row_copy(e, 0, c, me + 1).wait_recv()
            window[REACH + ROWS :, pl.ds(EDGE + x0, X), :] = in_rows[
                e, 0, :, pl.ds(x0, X), :
            ].astype(jnp.float32)

    def take_cols(e, edge):
        window = windows[e % 2]
        at = pl.ds(0 if edge == 1 else WIDE - EDGE, EDGE)
        col_copy(e, edge, 0, side).wait_recv()
        window[pl.ds(REACH, ROWS), at, :] = in_cols[e, edge, pl.ds(REACH, ROWS)]

        @pl.when(tile > 0)
        def _():
            col_copy(e, edge, 2, side - 1).wait_recv()
            window[pl.ds(0, REACH), at, :] = in_cols[e, edge, pl.ds(0, REACH)]

        @pl.when(tile < last_tile)
        def _():
            col_copy(e, edge, 1, side + 1).wait_recv()
            window[pl.ds(REACH + ROWS, REACH), at, :] = in_cols[
                e, edge, pl.ds(REACH + ROWS, REACH)
            ]

    def take_halo(e, k):
        if not linked:
            return

        @pl.when(k == 0)
        def _():
            take_rows(e, 0)
            take_rows(e, 1)
            take_cols(e, 1)

        @pl.when(k == 1)
        def _():
            take_rows(e, CHUNKS - 1)
            take_rows(e, CHUNKS - 2)
            take_cols(e, 0)

        @pl.when(k == 2)
        def _():
            take_rows(e, CHUNKS // 2)

    def sent(e):
        if not linked:
            return

        def one(c, carry):
            @pl.when(tile > 0)
            def _():
                row_copy(e, 0, c, me - 1).wait_send()

            @pl.when(tile < last_tile)
            def _():
                row_copy(e, 1, c, me + 1).wait_send()

            return carry

        lax.fori_loop(0, CHUNKS, one, 0)
        for edge in range(2):
            col_copy(e, edge, 0, side).wait_send()

            @pl.when(tile > 0)
            def _():
                col_copy(e, edge, 1, side - 1).wait_send()

            @pl.when(tile < last_tile)
            def _():
                col_copy(e, edge, 2, side + 1).wait_send()

    def chunk_of(k):
        return jnp.where(k % 2 == 0, k // 2, CHUNKS - 1 - k // 2)

    def keep(e, y, x0, value):
        windows[e % 2][y + REACH, pl.ds(EDGE + x0, X), :] = value.astype(jnp.float32)
        if linked:
            out_rows[e, y, pl.ds(x0, X), :] = value

    half_cells = ROWS // 2 * X

    def origin(k):
        return pl.multiple_of(chunk_of(k) * X, 16)

    def conv(e, k):
        layer, flipped = ((0, False), (1, False), (1, True), (0, True))[e]
        convolve(windows[e % 2], bands, sums, origin(k), taps_ref, layer, flipped)

    def halves(one):
        def half(q, inner):
            one(q, pl.ds(pl.multiple_of(q * half_cells, 16), half_cells))
            return inner

        lax.fori_loop(0, 2, half, 0)

    def half_of(q):
        return sums[:, pl.ds(pl.multiple_of(q * CELL, CELL), CELL)]

    def row_part(values, p):
        return values[p * X : (p + 1) * X]

    def stacked(read):
        return jnp.concatenate([read(p) for p in range(ROWS // 2)], axis=0)

    def forward_stage(e, layer, keep_norm, keep_slope, finish):
        def normalize(k):
            def one(q, at):
                unit, rstd = normalized(half_of(q))
                keep_norm(k, at, unit, rstd)
                dense = (unit * gain_ref[layer : layer + 1, :]).astype(jnp.bfloat16)
                before[at, :] = dot32(dense, expand_ref[layer])

            halves(one)

        def activate(k, y):
            at = pl.ds(pl.multiple_of(y * X, 16), X)
            value, slope = gelu_pair(before[at, :])
            active[at, :] = value.astype(jnp.bfloat16)
            keep_slope(k, at, slope)

        def close(k):
            def one(q, at):
                finish(k, q, at, dot32(active[at, :], project_ref[layer]))

            halves(one)
            send_chunk(e + 1, k, chunk_of(k))

        def chunk(k, carry):
            take_halo(e, k)
            conv(e, k)
            normalize(k)

            def piece(y, inner):
                activate(k, y)
                return inner

            lax.fori_loop(0, ROWS, piece, 0)
            close(k)
            return carry

        lax.fori_loop(0, CHUNKS, chunk, 0)
        sent(e)

    def backward_stage(e, one, after=None):
        def chunk(k, carry):
            take_halo(e, k)
            conv(e, k)
            halves(lambda q, at: one(k, q, at))
            if after is not None:
                after(k)
            if e < 3:
                send_chunk(e + 1, k, chunk_of(k))
            return carry

        lax.fori_loop(0, CHUNKS, chunk, 0)
        sent(e)

    half = ALON // 2
    row_number = lax.broadcasted_iota(jnp.int32, (ROWS, CELL), 0)
    land = land_ref[...].astype(jnp.float32).astype(jnp.bfloat16)

    def picked(o):
        return jnp.where(row_number == o, 1.0, 0.0).astype(jnp.bfloat16)

    def spread_mask(o, carry):
        mask_ref[o] = dot_first(land, picked(o)).astype(jnp.bfloat16)
        return carry

    lax.fori_loop(0, ROWS, spread_mask, 0)

    lanes = jnp.concatenate([mask_ref[y] * state_ref[y] for y in range(ROWS)], axis=1)
    high, rest = split(dot32(lanes, read_rows_ref[...]))
    coarse = 0.25 * (dot_first(high, group_ref[...]) + dot_first(rest, group_ref[...]))
    for slot in range(SLOTS):
        total = to_atmosphere_ref[slot, 0] * coarse[0:1]
        for o in range(1, ROWS):
            total = total + to_atmosphere_ref[slot, o] * coarse[o : o + 1]
        first_parts_out[slot] = total
    flux = dot_t(flux_read_ref[...], raw_ref[...])
    first_rows_out[...] = jnp.zeros((2, 8, LANES), jnp.float32)
    first_rows_out[0, :, 0:half] = flux[:, 0:half]
    first_rows_out[1, :, 0:half] = flux[:, half:]
    pl.semaphore_wait(pltpu.get_barrier_semaphore(), DEVICES - 1)
    send_rows(first_rows_out, first_parts_out, first_rows_in, first_parts_in, first_sems)
    spread_taps(bands, taps_ref, 0, False)
    wait_rows(first_rows_out, first_parts_out, first_rows_in, first_parts_in, first_sems)

    for o in range(ROWS):
        total = to_ocean_ref[0, o] * first_rows_in[0]
        for slot in range(1, SLOTS):
            total = total + to_ocean_ref[slot, o] * first_rows_in[slot]
        parts_out[o] = total
    high, rest = split(jnp.concatenate([parts_out[o] for o in range(ROWS)], axis=0))
    flux_cells[0 : ROWS * 8, :] = dot_t(high, group_ref[...])
    flux_cells[ROWS * 8 :, :] = dot_t(rest, group_ref[...])
    flux_embed_twice = jnp.concatenate([flux_embed_ref[...]] * 2, axis=0).astype(jnp.bfloat16)

    def force(o, carry):
        at = pl.multiple_of(o * 8, 8)
        cells = jnp.concatenate(
            [flux_cells[pl.ds(at, 8), :], flux_cells[pl.ds(at + ROWS * 8, 8), :]], axis=0
        ).astype(jnp.bfloat16)
        forcing = dot_first(cells, flux_embed_twice)
        start = (
            state_ref[o].astype(jnp.float32) + mask_ref[o].astype(jnp.float32) * forcing
        ).astype(jnp.bfloat16)
        win_a[o + REACH, EDGE : EDGE + CHUNKS * X, :] = start.astype(jnp.float32)
        out_rows[0, o] = start
        return carry

    lax.fori_loop(0, ROWS, force, 0)

    def first(k, carry):
        send_chunk(0, k, chunk_of(k))
        return carry

    lax.fori_loop(0, CHUNKS, first, 0)

    embed_high, embed_rest = split(surface_embed_ref[...])
    for h in range(2):
        total = first_parts_in[h]
        for k in range(1, 4):
            total = total + first_parts_in[2 * k + h]
        high, rest = split(total)
        blank = jnp.zeros((5, LANES), jnp.float32)
        left = jnp.concatenate(
            [high.astype(jnp.float32), high.astype(jnp.float32), rest.astype(jnp.float32), blank],
            axis=0,
        ).astype(jnp.bfloat16)
        blank = jnp.zeros((5, half_c), jnp.float32)
        right = jnp.concatenate(
            [
                embed_high.astype(jnp.float32),
                embed_rest.astype(jnp.float32),
                embed_high.astype(jnp.float32),
                blank,
            ],
            axis=0,
        ).astype(jnp.bfloat16)
        input_adj_ref[pl.ds(h * half, half), :] = dot_first(left, right)[:half]
    atmosphere_ref[...] = (raw_ref[...].astype(jnp.float32) + input_adj_ref[...]).astype(
        jnp.bfloat16
    )
    spectrum = dot32(wave_t_ref[...], atmosphere_ref[...])
    put_blocks(0, rounded(jnp.concatenate([spectrum[:DEVICES], spectrum[DEVICES:]], axis=1)))

    def mask_of(y, x0):
        return mask_ref[y, pl.ds(x0, X), :].astype(jnp.float32)

    def own(e, y, x0):
        return windows[e % 2][y + REACH, pl.ds(EDGE + x0, X), :]

    def keep_norm_0(k, at, unit, rstd):
        c = chunk_of(k)
        unit_0[c, at, :] = unit
        rstd_0[c, at, :] = jnp.broadcast_to(rstd, unit.shape)

    def keep_slope_0(k, at, slope):
        slope_0[chunk_of(k), at, :] = slope.astype(jnp.bfloat16)

    def finish_0(k, q, at, update):
        x0 = origin(k)
        for p in range(ROWS // 2):
            y = 2 * p + q
            new = own(0, y, x0) + mask_of(y, x0) * row_part(update, p)
            keep(1, y, x0, new.astype(jnp.bfloat16))

    forward_stage(0, 0, keep_norm_0, keep_slope_0, finish_0)
    spectral()
    spread_taps(bands, taps_ref, 1, False)

    def adjoint(e, k, q, at, masked, slope, unit, rstd, layer):
        x0 = origin(k)
        active[at, :] = (slope * dot_t(masked, project_ref[layer])).astype(jnp.bfloat16)
        scaled = dot_t(active[at, :], expand_ref[layer]) * gain_ref[layer : layer + 1, :]
        inner = jnp.mean(scaled * unit, axis=-1, keepdims=True)
        result = rstd * (scaled - jnp.mean(scaled, axis=-1, keepdims=True) - unit * inner)
        for p in range(ROWS // 2):
            keep(e, 2 * p + q, x0, row_part(result, p).astype(jnp.bfloat16))

    def cot_of(y, x0):
        return cot_ref[y, pl.ds(x0, X), :].astype(jnp.float32)

    def keep_norm_1(k, at, unit, rstd):
        unit_1[at, :] = unit
        rstd_1[at, :] = jnp.broadcast_to(rstd, unit.shape)

    def keep_slope_1(k, at, slope):
        before[at, :] = slope

    def finish_1(k, q, at, update):
        x0 = origin(k)
        for p in range(ROWS // 2):
            y = 2 * p + q
            new = own(1, y, x0) + mask_of(y, x0) * row_part(update, p)
            next_ref[y, pl.ds(x0, X), :] = new.astype(jnp.bfloat16)
        masked = stacked(lambda p: mask_of(2 * p + q, x0) * cot_of(2 * p + q, x0))
        adjoint(
            2, k, q, at, masked.astype(jnp.bfloat16), before[at, :], unit_1[at, :], rstd_1[at, :], 1
        )

    forward_stage(1, 1, keep_norm_1, keep_slope_1, finish_1)
    respond()
    spread_taps(bands, taps_ref, 1, True)

    def backward_0(k, q, at):
        c, x0 = (chunk_of(k), origin(k))
        hid = half_of(q)
        parts = []
        for p in range(ROWS // 2):
            y = 2 * p + q
            cot = cot_of(y, x0) + row_part(hid, p)
            grad_ref[y, pl.ds(x0, X), :] = cot
            parts.append(mask_of(y, x0) * cot)
        masked = jnp.concatenate(parts, axis=0).astype(jnp.bfloat16)
        slope = slope_0[c, at, :].astype(jnp.float32)
        adjoint(3, k, q, at, masked, slope, unit_0[c, at, :], rstd_0[c, at, :], 0)

    backward_stage(2, backward_0)
    spectral_back()
    spread_taps(bands, taps_ref, 0, True)

    def last(k, q, at):
        x0 = origin(k)
        hid = half_of(q)
        for p in range(ROWS // 2):
            y = 2 * p + q
            grad_ref[y, pl.ds(x0, X), :] = grad_ref[y, pl.ds(x0, X), :] + row_part(hid, p)

    def gather_flux(k):
        x0 = origin(k)
        lanes = jnp.concatenate(
            [mask_of(y, x0) * grad_ref[y, pl.ds(x0, X), :] for y in range(ROWS)], axis=1
        )
        high, rest = split(lanes)
        flux_rows[pl.ds(x0, X), :] = dot32(high, embed_rows_ref[...]) + dot32(
            rest, embed_rows_ref[...]
        )

    backward_stage(3, last, gather_flux)
    absorb()
    high, rest = split(flux_rows[...])
    flux_by_row = dot_first(high, group_ref[...]) + dot_first(rest, group_ref[...])
    for slot in range(SLOTS):
        total = to_ocean_ref[slot, 0] * flux_by_row[0:8]
        for o in range(1, ROWS):
            total = total + to_ocean_ref[slot, o] * flux_by_row[8 * o : 8 * o + 8]
        parts_out[slot] = total
    embed_high, embed_rest = split(jnp.broadcast_to(surface_embed_ref[...], (8, half_c)))
    rows_out[...] = jnp.zeros((2, 1, LANES), jnp.float32)
    for h in range(2):
        high, rest = split(input_adj_ref[pl.ds(h * half, half), :])
        row = dot_t(embed_high, high) + dot_t(embed_rest, high) + dot_t(embed_high, rest)
        rows_out[h, :, 0:half] = row[0:1]
    send_rows(rows_out, parts_out, rows_in, parts_in, regrid_sems)
    wait_rows(rows_out, parts_out, rows_in, parts_in, regrid_sems)
    for o in range(ROWS):
        total = to_atmosphere_ref[0, o] * rows_in[0]
        for slot in range(1, SLOTS):
            total = total + to_atmosphere_ref[slot, o] * rows_in[slot]
        coarse_rows[o : o + 1, :] = total
    coarse_high, coarse_rest = split(coarse_rows[...])
    read = surface_read_ref[...] * 0.25
    def widen(o, carry):
        pick = picked(o)
        spread = dot32(group_ref[...], dot_first(coarse_high, pick).astype(jnp.bfloat16)) + dot32(
            group_ref[...], dot_first(coarse_rest, pick).astype(jnp.bfloat16)
        )
        grad_ref[o] = grad_ref[o] + mask_ref[o].astype(jnp.float32) * spread * read
        return carry

    lax.fori_loop(0, ROWS, widen, 0)
    flux_read_twice = jnp.concatenate([flux_read_ref[...], flux_read_ref[...]], axis=0)
    for h in range(2):
        total = parts_in[h]
        for k in range(1, 4):
            total = total + parts_in[2 * k + h]
        high, rest = split(total)
        from_flux = dot_first(
            jnp.concatenate([high.astype(jnp.float32), rest.astype(jnp.float32)], axis=0).astype(
                jnp.bfloat16
            ),
            flux_read_twice,
        )
        at = pl.ds(h * half, half)
        input_adj_ref[at, :] = input_adj_ref[at, :] + from_flux[:half]


def ocean(*operands, linked=True):
    vmem = pl.BlockSpec(memory_space=pltpu.VMEM)
    smem = pl.BlockSpec(memory_space=pltpu.SMEM)
    whole = (ROWS, CHUNKS * X, CELL)
    f32, bf16 = (jnp.float32, jnp.bfloat16)
    return pl.pallas_call(
        functools.partial(ocean_kernel, linked),
        out_shape=(
            jax.ShapeDtypeStruct(whole, bf16),
            jax.ShapeDtypeStruct(whole, f32),
            jax.ShapeDtypeStruct((ALON, 3 * CELL), bf16),
            jax.ShapeDtypeStruct((ALON, 3 * CELL), f32),
        ),
        in_specs=[vmem] * 18 + [smem] * 2 + [vmem] * 3,
        out_specs=(vmem,) * 4,
        scratch_shapes=[
            pltpu.VMEM((ROWS + 2 * REACH, WIDE, CELL), f32),
            pltpu.VMEM((ROWS + 2 * REACH, WIDE, CELL), f32),
            pltpu.VMEM((TAPS, 8 * CELL, 2 * CELL), bf16),
            pltpu.VMEM((ROWS // 2 * X, 2 * CELL), f32),
            pltpu.VMEM((CHUNKS, ROWS * X, CELL), f32),
            pltpu.VMEM((CHUNKS, ROWS * X, CELL), f32),
            pltpu.VMEM((CHUNKS, ROWS * X, 4 * CELL), bf16),
            pltpu.VMEM((ROWS * X, CELL), f32),
            pltpu.VMEM((ROWS * X, CELL), f32),
            pltpu.VMEM((ROWS * X, 4 * CELL), f32),
            pltpu.VMEM((ROWS * X, 4 * CELL), bf16),
            pltpu.VMEM((4, ROWS, CHUNKS * X, CELL), bf16),
            pltpu.VMEM((4, 2, REACH, CHUNKS * X, CELL), bf16),
            pltpu.VMEM((4, 2, ROWS + 2 * REACH, EDGE, CELL), f32),
            pltpu.SemaphoreType.DMA((2, 4, 2, CHUNKS)),
            pltpu.SemaphoreType.DMA((2, 4, 2, 3)),
            pltpu.VMEM((4, DEVICES * 8, CELL), f32),
            pltpu.VMEM((4, DEVICES * 8, CELL), f32),
            pltpu.SemaphoreType.DMA((2, 4)),
            pltpu.VMEM((CHUNKS * X, ROWS * SLOTS), f32),
            pltpu.VMEM((ROWS, LANES), f32),
            pltpu.VMEM((2, 1, LANES), f32),
            pltpu.VMEM((SLOTS, 8, LANES), f32),
            pltpu.VMEM((SLOTS, 1, LANES), f32),
            pltpu.VMEM((SLOTS, 8, LANES), f32),
            pltpu.SemaphoreType.DMA((4, SLOTS)),
            pltpu.VMEM(whole, bf16),
            pltpu.VMEM((ALON, 3 * CELL), bf16),
            pltpu.VMEM((2, 8, LANES), f32),
            pltpu.VMEM((SLOTS, 1, LANES), f32),
            pltpu.VMEM((SLOTS, 8, LANES), f32),
            pltpu.VMEM((SLOTS, 1, LANES), f32),
            pltpu.SemaphoreType.DMA((4, SLOTS)),
            pltpu.VMEM((2 * ROWS * 8, CHUNKS * X), f32),
        ],
        compiler_params=pltpu.CompilerParams(
            collective_id=6 if linked else None, has_side_effects=linked, vmem_limit_bytes=67000000
        ),
        name="ocean",
    )(*operands)


def wave_table():
    place = np.arange(ALON, dtype=np.int32)[:, None] * np.arange(DEVICES, dtype=np.int32)[None, :]
    phase = (place % ALON).astype(np.float32) * np.float32(2.0 * np.pi / ALON)
    both = np.concatenate([np.cos(phase), -np.sin(phase)], axis=1)
    return (both * np.sqrt(np.float32(2.0 / ALON))).astype(jnp.bfloat16)


def slot_weights(bands_row, blocks, group):
    slot = bands_row[:, None] - (2 * group - 2)
    onehot = (slot == jnp.arange(SLOTS, dtype=jnp.int32)[None, :]).astype(jnp.float32)
    return jnp.sum(onehot[:, :, None] * blocks[:, None, :], axis=0)


def per_device(
    atmosphere,
    ocean_state,
    land_mask,
    crossing_bands,
    ocean_regrid,
    atmosphere_regrid,
    surface_read,
    surface_embed,
    flux_read,
    flux_embed,
    legendre_forward,
    legendre_inverse,
    spectral_mix,
    conv_kernel,
    norm_gain,
    expand_weight,
    project_weight,
    atmosphere_cotangent,
    ocean_cotangent,
):
    lat_rows, lon_count, channels = atmosphere.shape
    ocean_rows, ocean_lon, ocean_channels = ocean_state.shape
    half = lon_count // lax.axis_size("sec")
    ratio = ocean_lon // half
    flux_count = flux_read.shape[1]
    group = lax.axis_index("tile")
    to_ocean = slot_weights(crossing_bands[0], ocean_regrid[0, :, :, 0], group)
    to_atmosphere = slot_weights(crossing_bands[0], atmosphere_regrid[0, :, 0, :], group)
    table = wave_table()
    layer_count = conv_kernel.shape[0]
    embed_rows = (
        jnp.eye(ocean_rows, dtype=flux_embed.dtype)[:, None, :, None]
        * flux_embed.T[None, :, None, :]
    ).reshape(ocean_rows * ocean_channels, ocean_rows * flux_count)
    read_rows = (
        jnp.eye(ocean_rows, dtype=surface_read.dtype)[:, None, :] * surface_read[None, :, None]
    ).reshape(ocean_rows * ocean_channels, ocean_rows)
    grouping = np.arange(ocean_lon)[:, None] // ratio == np.arange(LANES)[None, :]
    grouping = grouping.astype(jnp.bfloat16)
    state, ocean_grad, atmosphere_next, atmosphere_grad = ocean(
        ocean_state,
        land_mask,
        ocean_cotangent,
        conv_kernel.reshape(layer_count, TAPS * TAPS, CELL).astype(jnp.float32),
        norm_gain,
        expand_weight,
        project_weight,
        atmosphere[0],
        atmosphere_cotangent[0],
        jnp.asarray(table),
        jnp.asarray(np.ascontiguousarray(table.T)),
        legendre_forward[0],
        legendre_inverse[0],
        spectral_mix,
        embed_rows,
        read_rows,
        flux_embed.astype(jnp.float32),
        jnp.asarray(grouping),
        to_ocean,
        to_atmosphere,
        surface_embed[None, :],
        surface_read.astype(jnp.float32)[None, :],
        flux_read.T,
    )
    return (atmosphere_next[None], state, atmosphere_grad[None], ocean_grad)


def solution(mesh):
    placed = (
        P(SEC_TILE, None, None),
        P(TILE, "sec", None),
        P(TILE, "sec"),
        P(TILE, None),
        P(TILE, None, None, None),
        P(TILE, None, None, None),
        P(),
        P(),
        P(),
        P(),
        P(SEC_TILE, None, None),
        P(SEC_TILE, None, None),
        P(),
        P(),
        P(),
        P(),
        P(),
        P(SEC_TILE, None, None),
        P(TILE, "sec", None),
    )
    return jax.shard_map(
        per_device,
        mesh=mesh,
        in_specs=placed,
        out_specs=(
            P(SEC_TILE, None, None),
            P(TILE, "sec", None),
            P(SEC_TILE, None, None),
            P(TILE, "sec", None),
        ),
        check_vma=False,
    )
```

```python
import functools

import jax
import jax.numpy as jnp
import numpy as np
from jax import lax
from jax.experimental import pallas as pl
from jax.experimental.pallas import tpu as pltpu
from jax.sharding import PartitionSpec as P

SEC_TILE = ("sec", "tile")
TILE = "tile"
LOGICAL = pl.DeviceIdType.LOGICAL
DEVICES = 128
GROUPS = 64
SLOTS = 8
LANES = 256
X = 144
CHUNKS = 5
ROWS = 8
WIDE = 736
EDGE = 8
CELL = 128
TAPS = 7
REACH = 3
ALON = 360
EARLY = 7


def remote(src, dst, send_sem, recv_sem, device):
    return pltpu.make_async_remote_copy(
        src_ref=src,
        dst_ref=dst,
        send_sem=send_sem,
        recv_sem=recv_sem,
        device_id=device,
        device_id_type=LOGICAL,
    )


def regrid_peers():
    sec = lax.axis_index("sec")
    group = lax.axis_index("tile")
    me = sec * GROUPS + group

    def group_device(k):
        return (k % 2) * GROUPS + (me // 2 + 1 - k // 2 + GROUPS) % GROUPS

    def band_device(slot):
        return (2 * group - 2 + slot + DEVICES) % DEVICES

    return sec, me, group_device, band_device


def send_rows(rows_ref, parts_ref, rows_in, parts_in, sems):
    sec, me, group_device, band_device = regrid_peers()

    for k in range(SLOTS):
        target = group_device(k)
        slot = me % 2 + 2 * (k // 2)

        @pl.when(target != me)
        def _():
            remote(
                rows_ref.at[k % 2], rows_in.at[slot], sems.at[0, k], sems.at[1, slot], target
            ).start()

        @pl.when(target == me)
        def _():
            rows_in[slot] = rows_ref[k % 2]

        band = band_device(k)
        place = (k // 2) * 2 + sec

        @pl.when(band != me)
        def _():
            remote(
                parts_ref.at[k], parts_in.at[place], sems.at[2, k], sems.at[3, place], band
            ).start()

        @pl.when(band == me)
        def _():
            parts_in[place] = parts_ref[k]


def wait_rows(rows_ref, parts_ref, rows_in, parts_in, sems):
    _, me, group_device, band_device = regrid_peers()

    for k in range(SLOTS):

        @pl.when(band_device(k) != me)
        def _():
            remote(rows_ref.at[0], rows_in.at[k], sems.at[0, k], sems.at[1, k], me).wait_recv()
            remote(parts_ref.at[k], parts_in.at[k], sems.at[2, k], sems.at[3, k], me).wait_send()

        @pl.when(group_device(k) != me)
        def _():
            remote(rows_ref.at[0], rows_in.at[k], sems.at[0, k], sems.at[1, k], me).wait_send()
            remote(parts_ref.at[k], parts_in.at[k], sems.at[2, k], sems.at[3, k], me).wait_recv()


def spread_taps(bands, taps_ref, layer, flipped):
    eye = lax.broadcasted_iota(jnp.int32, (CELL, CELL), 0) == lax.broadcasted_iota(
        jnp.int32, (CELL, CELL), 1
    )

    def one(v, carry):
        for u in range(TAPS):
            if flipped:
                row = taps_ref[layer, pl.ds((TAPS - 1 - u) * TAPS + (TAPS - 1) - v, 1), :]
            else:
                row = taps_ref[layer, pl.ds(u * TAPS + v, 1), :]
            block = jnp.where(eye, row, 0.0).astype(jnp.bfloat16)
            for q in range(2):
                bands[v, pl.ds((u + q) * CELL, CELL), pl.ds(q * CELL, CELL)] = block
        return carry

    lax.fori_loop(0, TAPS, one, 0)


VECTOR_TAPS = 2
STRIP = 16


def tap_row(taps_ref, layer, flipped, u, v):
    at = (TAPS - 1 - u) * TAPS + TAPS - 1 - v if flipped else u * TAPS + v
    return taps_ref[layer, at : at + 1, :]


def convolve(window, bands, sums, x0, taps_ref, layer, flipped):
    count = TAPS - VECTOR_TAPS
    strips = X // STRIP
    total = None
    done = 0
    for v in range(count):
        rows = [
            window[r, pl.ds(x0 + EDGE - REACH + v, X), :].astype(jnp.bfloat16)
            for r in range(ROWS + 2 * REACH)
        ]
        left = jnp.concatenate(
            [jnp.concatenate(rows[2 * p : 2 * p + 8], axis=1) for p in range(ROWS // 2)], axis=0
        )
        part = jnp.dot(left, bands[v], preferred_element_type=jnp.float32)
        total = part if total is None else total + part
        upto = strips * (v + 1) // count
        for strip in range(done, upto):
            parts = [None] * ROWS
            for w in range(count, TAPS):
                for r in range(ROWS + 2 * REACH):
                    cells = window[r, pl.ds(x0 + EDGE - REACH + w + strip * STRIP, STRIP), :]
                    for y in range(max(0, r - TAPS + 1), min(ROWS, r + 1)):
                        term = cells * tap_row(taps_ref, layer, flipped, r - y, w)
                        parts[y] = term if parts[y] is None else parts[y] + term
            for y in range(ROWS):
                sums[
                    pl.ds(y // 2 * X + strip * STRIP, STRIP), y % 2 * CELL : (y % 2 + 1) * CELL
                ] = parts[y]
        done = upto
    sums[...] = sums[...] + total


def normalized(hidden):
    center = hidden - jnp.mean(hidden, axis=-1, keepdims=True)
    rstd = lax.rsqrt(jnp.mean(center * center, axis=-1, keepdims=True) + 1e-06)
    return center * rstd, rstd


GELU_A = 0.7978845608028654
GELU_B = GELU_A * 0.044715


def gelu_pair(v):
    square = v * v
    w = 0.5 + 0.5 * jnp.tanh(v * (GELU_A + GELU_B * square))
    value = v * w
    slope = w + value * (1.0 - w) * (2.0 * GELU_A + (6.0 * GELU_B) * square)
    return value, slope


def split(values):
    high = values.astype(jnp.bfloat16)
    return high, (values - high.astype(jnp.float32)).astype(jnp.bfloat16)


def dot32(a, b):
    return jnp.dot(a, b, preferred_element_type=jnp.float32)


def dot_t(a, b):
    return lax.dot_general(a, b, (((1,), (1,)), ((), ())), preferred_element_type=jnp.float32)


def ocean_kernel(
    linked,
    state_ref,
    land_ref,
    cot_ref,
    kernel_ref,
    gain_ref,
    expand_ref,
    project_ref,
    raw_ref,
    atmosphere_cot_ref,
    wave_ref,
    wave_t_ref,
    forward_ref,
    inverse_ref,
    mix_ref,
    flux_embed_ref,
    group_ref,
    to_ocean_ref,
    to_atmosphere_ref,
    surface_embed_ref,
    surface_read_ref,
    flux_read_ref,
    next_ref,
    grad_ref,
    atmosphere_next_ref,
    input_adj_ref,
    win_a,
    win_b,
    bands,
    sums,
    unit_0,
    rstd_0,
    slope_0,
    unit_1,
    rstd_1,
    before,
    active,
    out_rows,
    in_rows,
    in_cols,
    row_sems,
    col_sems,
    leaving,
    landed,
    swap_sems,
    flux_rows,
    coarse_rows,
    rows_out,
    parts_out,
    rows_in,
    parts_in,
    regrid_sems,
    mask_ref,
    atmosphere_ref,
    first_rows_out,
    first_parts_out,
    first_rows_in,
    first_parts_in,
    first_sems,
    flux_cells,
    taps_ref,
    embed_rows_ref,
    read_rows_ref,
):
    sec = lax.axis_index("sec") if linked else 0
    tile = lax.axis_index("tile") if linked else 0
    last_tile = GROUPS - 1 if linked else 0
    me = sec * GROUPS + tile
    side = (1 - sec) * GROUPS + tile
    windows = (win_a, win_b)

    if linked:
        barrier = pltpu.get_barrier_semaphore()

        def greet(i, carry):
            pl.semaphore_signal(
                barrier, inc=1, device_id=(me + i) % DEVICES, device_id_type=LOGICAL
            )
            return carry

        lax.fori_loop(1, DEVICES, greet, 0)

    zero_rows = jnp.zeros((REACH, WIDE, CELL), jnp.float32)

    @pl.when(tile == 0)
    def _():
        for w in windows:
            w[0:REACH] = zero_rows

    @pl.when(tile == last_tile)
    def _():
        for w in windows:
            w[REACH + ROWS :] = zero_rows

    if not linked:
        for w in windows:
            w[:, 0:EDGE] = jnp.zeros((14, EDGE, CELL), jnp.float32)
            w[:, WIDE - EDGE :] = jnp.zeros((14, EDGE, CELL), jnp.float32)
    for v in range(TAPS):
        bands[v, 0:CELL, CELL:] = jnp.zeros((CELL, CELL), jnp.bfloat16)
        bands[v, 7 * CELL :, :CELL] = jnp.zeros((CELL, CELL), jnp.bfloat16)


    def send_block(x, i):
        peer = lax.rem(me + i, DEVICES)
        remote(
            leaving.at[x, pl.ds(pl.multiple_of(peer * 8, 8), 8)],
            landed.at[x, pl.ds(pl.multiple_of(me * 8, 8), 8)],
            swap_sems.at[0, x],
            swap_sems.at[1, x],
            peer,
        ).start()

    def send_share(x, turn, turns):
        share = (DEVICES - 1 - EARLY) // turns
        for j in range(share):
            send_block(x, EARLY + 1 + turn * share + j)

    def put_blocks(x, values):
        for j in range(6):
            leaving[x, pl.ds(j, DEVICES, stride=8), :] = values[:, j * CELL : (j + 1) * CELL]

        def send(i, carry):
            send_block(x, i)
            return carry

        lax.fori_loop(1, DEVICES if x == 3 else EARLY + 1, send, 0)
        mine = pl.ds(pl.multiple_of(me * 8, 8), 8)
        landed[x, mine, :] = leaving[x, mine, :]

    def take_blocks(x):
        source = landed
        if linked:
            every = landed.at[x, pl.ds(0, (DEVICES - 1) * 8)]
            pltpu.make_async_copy(every, every, swap_sems.at[1, x]).wait()
            pltpu.make_async_copy(every, every, swap_sems.at[0, x]).wait()
        else:
            source = leaving
        return jnp.concatenate(
            [source[x, pl.ds(j, DEVICES, stride=8), :] for j in range(6)], axis=1
        ).astype(jnp.bfloat16)

    def rounded(values):
        return values.astype(jnp.bfloat16).astype(jnp.float32)

    half_c = 3 * CELL

    def spectral():
        coefficient = dot32(forward_ref[...], take_blocks(0)).astype(jnp.bfloat16)
        real, imag = (coefficient[:, :half_c], coefficient[:, half_c:])
        mixed = jnp.concatenate(
            [
                dot32(real, mix_ref[0]) - dot32(imag, mix_ref[1]),
                dot32(imag, mix_ref[0]) + dot32(real, mix_ref[1]),
            ],
            axis=1,
        ).astype(jnp.bfloat16)
        put_blocks(1, rounded(dot32(inverse_ref[...], mixed)))

    def respond():
        returned = take_blocks(1)
        returned = jnp.concatenate([returned[:, :half_c], returned[:, half_c:]], axis=0)
        parts = []
        for j in range(3):
            cols = pl.ds(j * CELL, CELL)
            response = dot32(wave_ref[...], returned[:, j * CELL : (j + 1) * CELL])
            value, slope = gelu_pair(response)
            atmosphere_next_ref[:, cols] = (
                atmosphere_ref[:, cols].astype(jnp.float32) + value
            ).astype(jnp.bfloat16)
            response_adj = (slope * atmosphere_cot_ref[:, cols].astype(jnp.float32)).astype(
                jnp.bfloat16
            )
            parts.append(dot32(wave_t_ref[...], response_adj))
        put_blocks(
            2,
            rounded(
                jnp.concatenate([p[:DEVICES] for p in parts] + [p[DEVICES:] for p in parts], axis=1)
            ),
        )

    def dot_first(a, b):
        return lax.dot_general(
            a, b, (((0,), (0,)), ((), ())), preferred_element_type=jnp.float32
        )

    def spectral_back():
        mixed_adj = dot_first(inverse_ref[...], take_blocks(2)).astype(jnp.bfloat16)
        real, imag = (mixed_adj[:, :half_c], mixed_adj[:, half_c:])
        coefficient_adj = jnp.concatenate(
            [
                dot_t(real, mix_ref[0]) + dot_t(imag, mix_ref[1]),
                dot_t(imag, mix_ref[0]) - dot_t(real, mix_ref[1]),
            ],
            axis=1,
        ).astype(jnp.bfloat16)
        put_blocks(3, rounded(dot_first(forward_ref[...], coefficient_adj)))

    def absorb():
        spectrum_adj = take_blocks(3)
        spectrum_adj = jnp.concatenate([spectrum_adj[:, :half_c], spectrum_adj[:, half_c:]], axis=0)
        for j in range(3):
            cols = pl.ds(j * CELL, CELL)
            input_adj_ref[:, cols] = atmosphere_cot_ref[:, cols].astype(jnp.float32) + dot32(
                wave_ref[...], spectrum_adj[:, j * CELL : (j + 1) * CELL]
            )

    def row_copy(e, way, c, peer):
        x0 = pl.multiple_of(c * X, 16)
        return remote(
            out_rows.at[e, pl.ds(0 if way == 0 else ROWS - REACH, REACH), pl.ds(x0, X)],
            in_rows.at[e, way, :, pl.ds(x0, X)],
            row_sems.at[0, e, way, c],
            row_sems.at[1, e, way, c],
            peer,
        )

    def col_copy(e, edge, part, peer):
        source = windows[e % 2]
        first, size, place = ((0, ROWS, REACH), (0, REACH, REACH + ROWS), (ROWS - REACH, REACH, 0))[
            part
        ]
        return remote(
            source.at[
                pl.ds(REACH + first, size), pl.ds(EDGE if edge == 0 else WIDE - 2 * EDGE, EDGE)
            ],
            in_cols.at[e, edge, pl.ds(place, size)],
            col_sems.at[0, e, edge, part],
            col_sems.at[1, e, edge, part],
            peer,
        )

    def send_chunk(e, k, c):
        if not linked:
            return

        @pl.when(tile > 0)
        def _():
            row_copy(e, 0, c, me - 1).start()

        @pl.when(tile < last_tile)
        def _():
            row_copy(e, 1, c, me + 1).start()

        for edge in range(2):

            @pl.when(k == edge)
            def _():
                col_copy(e, edge, 0, side).start()

                @pl.when(tile > 0)
                def _():
                    col_copy(e, edge, 1, side - 1).start()

                @pl.when(tile < last_tile)
                def _():
                    col_copy(e, edge, 2, side + 1).start()

    def take_rows(e, c):
        x0 = pl.multiple_of(c * X, 16)
        window = windows[e % 2]

        @pl.when(tile > 0)
        def _():
            row_copy(e, 1, c, me - 1).wait_recv()
            window[0:REACH, pl.ds(EDGE + x0, X), :] = in_rows[e, 1, :, pl.ds(x0, X), :].astype(
                jnp.float32
            )

        @pl.when(tile < last_tile)
        def _():
            row_copy(e, 0, c, me + 1).wait_recv()
            window[REACH + ROWS :, pl.ds(EDGE + x0, X), :] = in_rows[
                e, 0, :, pl.ds(x0, X), :
            ].astype(jnp.float32)

    def take_cols(e, edge):
        window = windows[e % 2]
        at = pl.ds(0 if edge == 1 else WIDE - EDGE, EDGE)
        col_copy(e, edge, 0, side).wait_recv()
        window[pl.ds(REACH, ROWS), at, :] = in_cols[e, edge, pl.ds(REACH, ROWS)]

        @pl.when(tile > 0)
        def _():
            col_copy(e, edge, 2, side - 1).wait_recv()
            window[pl.ds(0, REACH), at, :] = in_cols[e, edge, pl.ds(0, REACH)]

        @pl.when(tile < last_tile)
        def _():
            col_copy(e, edge, 1, side + 1).wait_recv()
            window[pl.ds(REACH + ROWS, REACH), at, :] = in_cols[
                e, edge, pl.ds(REACH + ROWS, REACH)
            ]

    def take_halo(e, k):
        if not linked:
            return

        @pl.when(k == 0)
        def _():
            take_rows(e, 0)
            take_rows(e, 1)
            take_cols(e, 1)

        @pl.when(k == 1)
        def _():
            take_rows(e, CHUNKS - 1)
            take_rows(e, CHUNKS - 2)
            take_cols(e, 0)

        @pl.when(k == 2)
        def _():
            take_rows(e, CHUNKS // 2)

    def sent(e):
        if not linked:
            return

        def one(c, carry):
            @pl.when(tile > 0)
            def _():
                row_copy(e, 0, c, me - 1).wait_send()

            @pl.when(tile < last_tile)
            def _():
                row_copy(e, 1, c, me + 1).wait_send()

            return carry

        lax.fori_loop(0, CHUNKS, one, 0)
        for edge in range(2):
            col_copy(e, edge, 0, side).wait_send()

            @pl.when(tile > 0)
            def _():
                col_copy(e, edge, 1, side - 1).wait_send()

            @pl.when(tile < last_tile)
            def _():
                col_copy(e, edge, 2, side + 1).wait_send()

    def chunk_of(k):
        return jnp.where(k % 2 == 0, k // 2, CHUNKS - 1 - k // 2)

    def keep(e, y, x0, value):
        windows[e % 2][y + REACH, pl.ds(EDGE + x0, X), :] = value.astype(jnp.float32)
        if linked:
            out_rows[e, y, pl.ds(x0, X), :] = value

    half_cells = ROWS // 2 * X

    def origin(k):
        return pl.multiple_of(chunk_of(k) * X, 16)

    def conv(e, k):
        layer, flipped = ((0, False), (1, False), (1, True), (0, True))[e]
        convolve(windows[e % 2], bands, sums, origin(k), taps_ref, layer, flipped)

    def halves(one):
        def half(q, inner):
            one(q, pl.ds(pl.multiple_of(q * half_cells, 16), half_cells))
            return inner

        lax.fori_loop(0, 2, half, 0)

    def half_of(q):
        return sums[:, pl.ds(pl.multiple_of(q * CELL, CELL), CELL)]

    def row_part(values, p):
        return values[p * X : (p + 1) * X]

    def stacked(read):
        return jnp.concatenate([read(p) for p in range(ROWS // 2)], axis=0)

    def forward_stage(e, layer, keep_norm, keep_slope, finish):
        def normalize(k):
            def one(q, at):
                unit, rstd = normalized(half_of(q))
                keep_norm(k, at, unit, rstd)
                dense = (unit * gain_ref[layer : layer + 1, :]).astype(jnp.bfloat16)
                before[at, :] = dot32(dense, expand_ref[layer])

            halves(one)

        def activate(k, y):
            at = pl.ds(pl.multiple_of(y * X, 16), X)
            value, slope = gelu_pair(before[at, :])
            active[at, :] = value.astype(jnp.bfloat16)
            keep_slope(k, at, slope)

        def close(k):
            def one(q, at):
                finish(k, q, at, dot32(active[at, :], project_ref[layer]))

            halves(one)
            send_chunk(e + 1, k, chunk_of(k))

        def chunk(k, carry):
            take_halo(e, k)
            conv(e, k)
            normalize(k)

            def piece(y, inner):
                send_share(e, k * ROWS + y, CHUNKS * ROWS)
                activate(k, y)
                return inner

            lax.fori_loop(0, ROWS, piece, 0)
            close(k)
            return carry

        lax.fori_loop(0, CHUNKS, chunk, 0)
        sent(e)

    def backward_stage(e, one, after=None):
        def chunk(k, carry):
            take_halo(e, k)
            conv(e, k)

            def part(q, at):
                if e == 2:
                    send_share(e, k * 2 + q, CHUNKS * 2)
                one(k, q, at)

            halves(part)
            if after is not None:
                after(k)
            if e < 3:
                send_chunk(e + 1, k, chunk_of(k))
            return carry

        lax.fori_loop(0, CHUNKS, chunk, 0)
        sent(e)

    half = ALON // 2
    row_number = lax.broadcasted_iota(jnp.int32, (ROWS, CELL), 0)
    land = land_ref[...].astype(jnp.float32).astype(jnp.bfloat16)

    def picked(o):
        return jnp.where(row_number == o, 1.0, 0.0).astype(jnp.bfloat16)

    def spread_mask(o, carry):
        mask_ref[o] = dot_first(land, picked(o)).astype(jnp.bfloat16)
        return carry

    lax.fori_loop(0, ROWS, spread_mask, 0)

    for layer in range(2):
        for u in range(TAPS):
            taps_ref[layer, u * TAPS : (u + 1) * TAPS, :] = kernel_ref[layer, u].astype(jnp.float32)

    def numbers(width):
        return [lax.broadcasted_iota(jnp.int32, (8, width), axis) for axis in range(2)]

    read_row = jnp.where(row_number == 0, surface_read_ref[...], 0.0).astype(jnp.bfloat16)
    for y in range(ROWS):
        at = pl.ds(y * CELL, CELL)
        row, column = numbers(ROWS)
        pick = jnp.where((row == 0) & (column == y), 1.0, 0.0).astype(jnp.bfloat16)
        read_rows_ref[at, :] = dot_first(read_row, pick).astype(jnp.bfloat16)
        row, column = numbers(ROWS * 8)
        pick = jnp.where(column == row + y * 8, 1.0, 0.0).astype(jnp.bfloat16)
        embed_rows_ref[at, :] = dot_first(flux_embed_ref[...], pick).astype(jnp.bfloat16)

    lanes = jnp.concatenate([mask_ref[y] * state_ref[y] for y in range(ROWS)], axis=1)
    high, rest = split(dot32(lanes, read_rows_ref[...]))
    coarse = 0.25 * (dot_first(high, group_ref[...]) + dot_first(rest, group_ref[...]))
    for slot in range(SLOTS):
        total = to_atmosphere_ref[slot, 0] * coarse[0:1]
        for o in range(1, ROWS):
            total = total + to_atmosphere_ref[slot, o] * coarse[o : o + 1]
        first_parts_out[slot] = total
    flux = dot_t(flux_read_ref[...], raw_ref[...])
    first_rows_out[...] = jnp.zeros((2, 8, LANES), jnp.float32)
    first_rows_out[0, :, 0:half] = flux[:, 0:half]
    first_rows_out[1, :, 0:half] = flux[:, half:]
    pl.semaphore_wait(pltpu.get_barrier_semaphore(), DEVICES - 1)
    send_rows(first_rows_out, first_parts_out, first_rows_in, first_parts_in, first_sems)
    spread_taps(bands, taps_ref, 0, False)
    wait_rows(first_rows_out, first_parts_out, first_rows_in, first_parts_in, first_sems)

    for o in range(ROWS):
        total = to_ocean_ref[0, o] * first_rows_in[0]
        for slot in range(1, SLOTS):
            total = total + to_ocean_ref[slot, o] * first_rows_in[slot]
        parts_out[o] = total
    high, rest = split(jnp.concatenate([parts_out[o] for o in range(ROWS)], axis=0))
    flux_cells[0 : ROWS * 8, :] = dot_t(high, group_ref[...])
    flux_cells[ROWS * 8 :, :] = dot_t(rest, group_ref[...])
    flux_embed_twice = jnp.concatenate([flux_embed_ref[...].astype(jnp.float32)] * 2, axis=0)
    flux_embed_twice = flux_embed_twice.astype(jnp.bfloat16)

    def force(o, carry):
        at = pl.multiple_of(o * 8, 8)
        cells = jnp.concatenate(
            [flux_cells[pl.ds(at, 8), :], flux_cells[pl.ds(at + ROWS * 8, 8), :]], axis=0
        ).astype(jnp.bfloat16)
        forcing = dot_first(cells, flux_embed_twice)
        start = (
            state_ref[o].astype(jnp.float32) + mask_ref[o].astype(jnp.float32) * forcing
        ).astype(jnp.bfloat16)
        win_a[o + REACH, EDGE : EDGE + CHUNKS * X, :] = start.astype(jnp.float32)
        out_rows[0, o] = start
        return carry

    lax.fori_loop(0, ROWS, force, 0)

    def first(k, carry):
        send_chunk(0, k, chunk_of(k))
        return carry

    lax.fori_loop(0, CHUNKS, first, 0)

    embed_high, embed_rest = split(surface_embed_ref[...])
    for h in range(2):
        total = first_parts_in[h]
        for k in range(1, 4):
            total = total + first_parts_in[2 * k + h]
        high, rest = split(total)
        blank = jnp.zeros((5, LANES), jnp.float32)
        left = jnp.concatenate(
            [high.astype(jnp.float32), high.astype(jnp.float32), rest.astype(jnp.float32), blank],
            axis=0,
        ).astype(jnp.bfloat16)
        blank = jnp.zeros((5, half_c), jnp.float32)
        right = jnp.concatenate(
            [
                embed_high.astype(jnp.float32),
                embed_rest.astype(jnp.float32),
                embed_high.astype(jnp.float32),
                blank,
            ],
            axis=0,
        ).astype(jnp.bfloat16)
        input_adj_ref[pl.ds(h * half, half), :] = dot_first(left, right)[:half]
    atmosphere_ref[...] = (raw_ref[...].astype(jnp.float32) + input_adj_ref[...]).astype(
        jnp.bfloat16
    )
    spectrum = dot32(wave_t_ref[...], atmosphere_ref[...])
    put_blocks(0, rounded(jnp.concatenate([spectrum[:DEVICES], spectrum[DEVICES:]], axis=1)))

    def mask_of(y, x0):
        return mask_ref[y, pl.ds(x0, X), :].astype(jnp.float32)

    def own(e, y, x0):
        return windows[e % 2][y + REACH, pl.ds(EDGE + x0, X), :]

    def keep_norm_0(k, at, unit, rstd):
        c = chunk_of(k)
        unit_0[c, at, :] = unit
        rstd_0[c, at, :] = jnp.broadcast_to(rstd, unit.shape)

    def keep_slope_0(k, at, slope):
        slope_0[chunk_of(k), at, :] = slope.astype(jnp.bfloat16)

    def finish_0(k, q, at, update):
        x0 = origin(k)
        for p in range(ROWS // 2):
            y = 2 * p + q
            new = own(0, y, x0) + mask_of(y, x0) * row_part(update, p)
            keep(1, y, x0, new.astype(jnp.bfloat16))

    forward_stage(0, 0, keep_norm_0, keep_slope_0, finish_0)
    spectral()
    spread_taps(bands, taps_ref, 1, False)

    def adjoint(e, k, q, at, masked, slope, unit, rstd, layer):
        x0 = origin(k)
        active[at, :] = (slope * dot_t(masked, project_ref[layer])).astype(jnp.bfloat16)
        scaled = dot_t(active[at, :], expand_ref[layer]) * gain_ref[layer : layer + 1, :]
        inner = jnp.mean(scaled * unit, axis=-1, keepdims=True)
        result = rstd * (scaled - jnp.mean(scaled, axis=-1, keepdims=True) - unit * inner)
        for p in range(ROWS // 2):
            keep(e, 2 * p + q, x0, row_part(result, p).astype(jnp.bfloat16))

    def cot_of(y, x0):
        return cot_ref[y, pl.ds(x0, X), :].astype(jnp.float32)

    def keep_norm_1(k, at, unit, rstd):
        unit_1[at, :] = unit
        rstd_1[at, :] = jnp.broadcast_to(rstd, unit.shape)

    def keep_slope_1(k, at, slope):
        before[at, :] = slope

    def finish_1(k, q, at, update):
        x0 = origin(k)
        for p in range(ROWS // 2):
            y = 2 * p + q
            new = own(1, y, x0) + mask_of(y, x0) * row_part(update, p)
            next_ref[y, pl.ds(x0, X), :] = new.astype(jnp.bfloat16)
        masked = stacked(lambda p: mask_of(2 * p + q, x0) * cot_of(2 * p + q, x0))
        adjoint(
            2, k, q, at, masked.astype(jnp.bfloat16), before[at, :], unit_1[at, :], rstd_1[at, :], 1
        )

    forward_stage(1, 1, keep_norm_1, keep_slope_1, finish_1)
    respond()
    spread_taps(bands, taps_ref, 1, True)

    def backward_0(k, q, at):
        c, x0 = (chunk_of(k), origin(k))
        hid = half_of(q)
        parts = []
        for p in range(ROWS // 2):
            y = 2 * p + q
            cot = cot_of(y, x0) + row_part(hid, p)
            grad_ref[y, pl.ds(x0, X), :] = cot
            parts.append(mask_of(y, x0) * cot)
        masked = jnp.concatenate(parts, axis=0).astype(jnp.bfloat16)
        slope = slope_0[c, at, :].astype(jnp.float32)
        adjoint(3, k, q, at, masked, slope, unit_0[c, at, :], rstd_0[c, at, :], 0)

    backward_stage(2, backward_0)
    spectral_back()
    spread_taps(bands, taps_ref, 0, True)

    def last(k, q, at):
        x0 = origin(k)
        hid = half_of(q)
        for p in range(ROWS // 2):
            y = 2 * p + q
            grad_ref[y, pl.ds(x0, X), :] = grad_ref[y, pl.ds(x0, X), :] + row_part(hid, p)

    def gather_flux(k):
        x0 = origin(k)
        lanes = jnp.concatenate(
            [mask_of(y, x0) * grad_ref[y, pl.ds(x0, X), :] for y in range(ROWS)], axis=1
        )
        high, rest = split(lanes)
        flux_rows[pl.ds(x0, X), :] = dot32(high, embed_rows_ref[...]) + dot32(
            rest, embed_rows_ref[...]
        )

    backward_stage(3, last, gather_flux)
    absorb()
    high, rest = split(flux_rows[...])
    flux_by_row = dot_first(high, group_ref[...]) + dot_first(rest, group_ref[...])
    for slot in range(SLOTS):
        total = to_ocean_ref[slot, 0] * flux_by_row[0:8]
        for o in range(1, ROWS):
            total = total + to_ocean_ref[slot, o] * flux_by_row[8 * o : 8 * o + 8]
        parts_out[slot] = total
    embed_high, embed_rest = split(jnp.broadcast_to(surface_embed_ref[...], (8, half_c)))
    rows_out[...] = jnp.zeros((2, 1, LANES), jnp.float32)
    for h in range(2):
        high, rest = split(input_adj_ref[pl.ds(h * half, half), :])
        row = dot_t(embed_high, high) + dot_t(embed_rest, high) + dot_t(embed_high, rest)
        rows_out[h, :, 0:half] = row[0:1]
    send_rows(rows_out, parts_out, rows_in, parts_in, regrid_sems)
    wait_rows(rows_out, parts_out, rows_in, parts_in, regrid_sems)
    for o in range(ROWS):
        total = to_atmosphere_ref[0, o] * rows_in[0]
        for slot in range(1, SLOTS):
            total = total + to_atmosphere_ref[slot, o] * rows_in[slot]
        coarse_rows[o : o + 1, :] = total
    coarse_high, coarse_rest = split(coarse_rows[...])
    read = surface_read_ref[...] * 0.25
    def widen(o, carry):
        pick = picked(o)
        spread = dot32(group_ref[...], dot_first(coarse_high, pick).astype(jnp.bfloat16)) + dot32(
            group_ref[...], dot_first(coarse_rest, pick).astype(jnp.bfloat16)
        )
        grad_ref[o] = grad_ref[o] + mask_ref[o].astype(jnp.float32) * spread * read
        return carry

    lax.fori_loop(0, ROWS, widen, 0)
    flux_read_twice = jnp.concatenate([flux_read_ref[...], flux_read_ref[...]], axis=0)
    for h in range(2):
        total = parts_in[h]
        for k in range(1, 4):
            total = total + parts_in[2 * k + h]
        high, rest = split(total)
        from_flux = dot_first(
            jnp.concatenate([high.astype(jnp.float32), rest.astype(jnp.float32)], axis=0).astype(
                jnp.bfloat16
            ),
            flux_read_twice,
        )
        at = pl.ds(h * half, half)
        input_adj_ref[at, :] = input_adj_ref[at, :] + from_flux[:half]


def ocean(*operands, linked=True):
    vmem = pl.BlockSpec(memory_space=pltpu.VMEM)
    smem = pl.BlockSpec(memory_space=pltpu.SMEM)
    whole = (ROWS, CHUNKS * X, CELL)
    f32, bf16 = (jnp.float32, jnp.bfloat16)
    return pl.pallas_call(
        functools.partial(ocean_kernel, linked),
        out_shape=(
            jax.ShapeDtypeStruct(whole, bf16),
            jax.ShapeDtypeStruct(whole, f32),
            jax.ShapeDtypeStruct((ALON, 3 * CELL), bf16),
            jax.ShapeDtypeStruct((ALON, 3 * CELL), f32),
        ),
        in_specs=[vmem] * 16 + [smem] * 2 + [vmem] * 3,
        out_specs=(vmem,) * 4,
        scratch_shapes=[
            pltpu.VMEM((ROWS + 2 * REACH, WIDE, CELL), f32),
            pltpu.VMEM((ROWS + 2 * REACH, WIDE, CELL), f32),
            pltpu.VMEM((TAPS, 8 * CELL, 2 * CELL), bf16),
            pltpu.VMEM((ROWS // 2 * X, 2 * CELL), f32),
            pltpu.VMEM((CHUNKS, ROWS * X, CELL), f32),
            pltpu.VMEM((CHUNKS, ROWS * X, CELL), f32),
            pltpu.VMEM((CHUNKS, ROWS * X, 4 * CELL), bf16),
            pltpu.VMEM((ROWS * X, CELL), f32),
            pltpu.VMEM((ROWS * X, CELL), f32),
            pltpu.VMEM((ROWS * X, 4 * CELL), f32),
            pltpu.VMEM((ROWS * X, 4 * CELL), bf16),
            pltpu.VMEM((4, ROWS, CHUNKS * X, CELL), bf16),
            pltpu.VMEM((4, 2, REACH, CHUNKS * X, CELL), bf16),
            pltpu.VMEM((4, 2, ROWS + 2 * REACH, EDGE, CELL), f32),
            pltpu.SemaphoreType.DMA((2, 4, 2, CHUNKS)),
            pltpu.SemaphoreType.DMA((2, 4, 2, 3)),
            pltpu.VMEM((4, DEVICES * 8, CELL), f32),
            pltpu.VMEM((4, DEVICES * 8, CELL), f32),
            pltpu.SemaphoreType.DMA((2, 4)),
            pltpu.VMEM((CHUNKS * X, ROWS * SLOTS), f32),
            pltpu.VMEM((ROWS, LANES), f32),
            pltpu.VMEM((2, 1, LANES), f32),
            pltpu.VMEM((SLOTS, 8, LANES), f32),
            pltpu.VMEM((SLOTS, 1, LANES), f32),
            pltpu.VMEM((SLOTS, 8, LANES), f32),
            pltpu.SemaphoreType.DMA((4, SLOTS)),
            pltpu.VMEM(whole, bf16),
            pltpu.VMEM((ALON, 3 * CELL), bf16),
            pltpu.VMEM((2, 8, LANES), f32),
            pltpu.VMEM((SLOTS, 1, LANES), f32),
            pltpu.VMEM((SLOTS, 8, LANES), f32),
            pltpu.VMEM((SLOTS, 1, LANES), f32),
            pltpu.SemaphoreType.DMA((4, SLOTS)),
            pltpu.VMEM((2 * ROWS * 8, CHUNKS * X), f32),
            pltpu.VMEM((2, TAPS * TAPS, CELL), f32),
            pltpu.VMEM((ROWS * CELL, ROWS * 8), bf16),
            pltpu.VMEM((ROWS * CELL, ROWS), bf16),
        ],
        compiler_params=pltpu.CompilerParams(
            collective_id=6 if linked else None, has_side_effects=linked, vmem_limit_bytes=67000000
        ),
        name="ocean",
    )(*operands)


def wave_table():
    place = np.arange(ALON, dtype=np.int32)[:, None] * np.arange(DEVICES, dtype=np.int32)[None, :]
    phase = (place % ALON).astype(np.float32) * np.float32(2.0 * np.pi / ALON)
    both = np.concatenate([np.cos(phase), -np.sin(phase)], axis=1)
    return (both * np.sqrt(np.float32(2.0 / ALON))).astype(jnp.bfloat16)


def slot_weights(bands_row, blocks, group):
    slot = bands_row[:, None] - (2 * group - 2)
    onehot = (slot == jnp.arange(SLOTS, dtype=jnp.int32)[None, :]).astype(jnp.float32)
    return jnp.sum(onehot[:, :, None] * blocks[:, None, :], axis=0)


def per_device(
    atmosphere,
    ocean_state,
    land_mask,
    crossing_bands,
    ocean_regrid,
    atmosphere_regrid,
    surface_read,
    surface_embed,
    flux_read,
    flux_embed,
    legendre_forward,
    legendre_inverse,
    spectral_mix,
    conv_kernel,
    norm_gain,
    expand_weight,
    project_weight,
    atmosphere_cotangent,
    ocean_cotangent,
):
    lon_count = atmosphere.shape[1]
    ocean_lon = ocean_state.shape[1]
    half = lon_count // lax.axis_size("sec")
    ratio = ocean_lon // half
    group = lax.axis_index("tile")
    to_ocean = slot_weights(crossing_bands[0], ocean_regrid[0, :, :, 0], group)
    to_atmosphere = slot_weights(crossing_bands[0], atmosphere_regrid[0, :, 0, :], group)
    table = wave_table()
    grouping = np.arange(ocean_lon)[:, None] // ratio == np.arange(LANES)[None, :]
    grouping = grouping.astype(jnp.bfloat16)
    state, ocean_grad, atmosphere_next, atmosphere_grad = ocean(
        ocean_state,
        land_mask,
        ocean_cotangent,
        conv_kernel,
        norm_gain,
        expand_weight,
        project_weight,
        atmosphere[0],
        atmosphere_cotangent[0],
        jnp.asarray(table),
        jnp.asarray(np.ascontiguousarray(table.T)),
        legendre_forward[0],
        legendre_inverse[0],
        spectral_mix,
        flux_embed,
        jnp.asarray(grouping),
        to_ocean,
        to_atmosphere,
        surface_embed[None, :],
        surface_read.astype(jnp.float32)[None, :],
        flux_read.T,
    )
    return (atmosphere_next[None], state, atmosphere_grad[None], ocean_grad)


def solution(mesh):
    placed = (
        P(SEC_TILE, None, None),
        P(TILE, "sec", None),
        P(TILE, "sec"),
        P(TILE, None),
        P(TILE, None, None, None),
        P(TILE, None, None, None),
        P(),
        P(),
        P(),
        P(),
        P(SEC_TILE, None, None),
        P(SEC_TILE, None, None),
        P(),
        P(),
        P(),
        P(),
        P(),
        P(SEC_TILE, None, None),
        P(TILE, "sec", None),
    )
    return jax.shard_map(
        per_device,
        mesh=mesh,
        in_specs=placed,
        out_specs=(
            P(SEC_TILE, None, None),
            P(TILE, "sec", None),
            P(SEC_TILE, None, None),
            P(TILE, "sec", None),
        ),
        check_vma=False,
    )
```

```python
import functools

import jax
import jax.numpy as jnp
import numpy as np
from jax import lax
from jax.experimental import pallas as pl
from jax.experimental.pallas import tpu as pltpu
from jax.sharding import PartitionSpec as P

SEC_TILE = ("sec", "tile")
TILE = "tile"
LOGICAL = pl.DeviceIdType.LOGICAL
DEVICES = 128
GROUPS = 64
SLOTS = 8
LANES = 256
X = 144
CHUNKS = 5
ROWS = 8
WIDE = 736
EDGE = 8
CELL = 128
TAPS = 7
REACH = 3
ALON = 360


def remote(src, dst, send_sem, recv_sem, device):
    return pltpu.make_async_remote_copy(
        src_ref=src,
        dst_ref=dst,
        send_sem=send_sem,
        recv_sem=recv_sem,
        device_id=device,
        device_id_type=LOGICAL,
    )


def regrid_peers():
    sec = lax.axis_index("sec")
    group = lax.axis_index("tile")
    me = sec * GROUPS + group

    def group_device(k):
        return (k % 2) * GROUPS + (me // 2 + 1 - k // 2 + GROUPS) % GROUPS

    def band_device(slot):
        return (2 * group - 2 + slot + DEVICES) % DEVICES

    return sec, me, group_device, band_device


def send_rows(rows_ref, parts_ref, rows_in, parts_in, sems):
    sec, me, group_device, band_device = regrid_peers()

    for k in range(SLOTS):
        target = group_device(k)
        slot = me % 2 + 2 * (k // 2)

        @pl.when(target != me)
        def _():
            remote(
                rows_ref.at[k % 2], rows_in.at[slot], sems.at[0, k], sems.at[1, slot], target
            ).start()

        @pl.when(target == me)
        def _():
            rows_in[slot] = rows_ref[k % 2]

        band = band_device(k)
        place = (k // 2) * 2 + sec

        @pl.when(band != me)
        def _():
            remote(
                parts_ref.at[k], parts_in.at[place], sems.at[2, k], sems.at[3, place], band
            ).start()

        @pl.when(band == me)
        def _():
            parts_in[place] = parts_ref[k]


def wait_rows(rows_ref, parts_ref, rows_in, parts_in, sems):
    _, me, group_device, band_device = regrid_peers()

    for k in range(SLOTS):

        @pl.when(band_device(k) != me)
        def _():
            remote(rows_ref.at[0], rows_in.at[k], sems.at[0, k], sems.at[1, k], me).wait_recv()
            remote(parts_ref.at[k], parts_in.at[k], sems.at[2, k], sems.at[3, k], me).wait_send()

        @pl.when(group_device(k) != me)
        def _():
            remote(rows_ref.at[0], rows_in.at[k], sems.at[0, k], sems.at[1, k], me).wait_send()
            remote(parts_ref.at[k], parts_in.at[k], sems.at[2, k], sems.at[3, k], me).wait_recv()


def spread_taps(bands, taps_ref, layer, flipped):
    eye = lax.broadcasted_iota(jnp.int32, (CELL, CELL), 0) == lax.broadcasted_iota(
        jnp.int32, (CELL, CELL), 1
    )

    def one(v, carry):
        for u in range(TAPS):
            if flipped:
                row = taps_ref[layer, pl.ds((TAPS - 1 - u) * TAPS + (TAPS - 1) - v, 1), :]
            else:
                row = taps_ref[layer, pl.ds(u * TAPS + v, 1), :]
            block = jnp.where(eye, row, 0.0).astype(jnp.bfloat16)
            for q in range(2):
                bands[v, pl.ds((u + q) * CELL, CELL), pl.ds(q * CELL, CELL)] = block
        return carry

    lax.fori_loop(0, TAPS, one, 0)


VECTOR_TAPS = 2
STRIP = 16


def tap_row(taps_ref, layer, flipped, u, v):
    at = (TAPS - 1 - u) * TAPS + TAPS - 1 - v if flipped else u * TAPS + v
    return taps_ref[layer, at : at + 1, :]


def convolve(window, bands, sums, x0, taps_ref, layer, flipped):
    count = TAPS - VECTOR_TAPS
    strips = X // STRIP
    total = None
    done = 0
    for v in range(count):
        rows = [
            window[r, pl.ds(x0 + EDGE - REACH + v, X), :].astype(jnp.bfloat16)
            for r in range(ROWS + 2 * REACH)
        ]
        left = jnp.concatenate(
            [jnp.concatenate(rows[2 * p : 2 * p + 8], axis=1) for p in range(ROWS // 2)], axis=0
        )
        part = jnp.dot(left, bands[v], preferred_element_type=jnp.float32)
        total = part if total is None else total + part
        upto = strips * (v + 1) // count
        for strip in range(done, upto):
            parts = [None] * ROWS
            for w in range(count, TAPS):
                for r in range(ROWS + 2 * REACH):
                    cells = window[r, pl.ds(x0 + EDGE - REACH + w + strip * STRIP, STRIP), :]
                    for y in range(max(0, r - TAPS + 1), min(ROWS, r + 1)):
                        term = cells * tap_row(taps_ref, layer, flipped, r - y, w)
                        parts[y] = term if parts[y] is None else parts[y] + term
            for y in range(ROWS):
                sums[
                    pl.ds(y // 2 * X + strip * STRIP, STRIP), y % 2 * CELL : (y % 2 + 1) * CELL
                ] = parts[y]
        done = upto
    sums[...] = sums[...] + total


def normalized(hidden):
    center = hidden - jnp.mean(hidden, axis=-1, keepdims=True)
    rstd = lax.rsqrt(jnp.mean(center * center, axis=-1, keepdims=True) + 1e-06)
    return center * rstd, rstd


GELU_A = 0.7978845608028654
GELU_B = GELU_A * 0.044715


def gelu_pair(v):
    square = v * v
    w = 0.5 + 0.5 * jnp.tanh(v * (GELU_A + GELU_B * square))
    value = v * w
    slope = w + value * (1.0 - w) * (2.0 * GELU_A + (6.0 * GELU_B) * square)
    return value, slope


def split(values):
    high = values.astype(jnp.bfloat16)
    return high, (values - high.astype(jnp.float32)).astype(jnp.bfloat16)


def dot32(a, b):
    return jnp.dot(a, b, preferred_element_type=jnp.float32)


def dot_t(a, b):
    return lax.dot_general(a, b, (((1,), (1,)), ((), ())), preferred_element_type=jnp.float32)


def ocean_kernel(
    linked,
    state_ref,
    land_ref,
    cot_ref,
    kernel_ref,
    gain_ref,
    expand_ref,
    project_ref,
    raw_ref,
    atmosphere_cot_ref,
    wave_ref,
    wave_t_ref,
    forward_ref,
    inverse_ref,
    mix_ref,
    flux_embed_ref,
    group_ref,
    to_ocean_ref,
    to_atmosphere_ref,
    surface_embed_ref,
    surface_read_ref,
    flux_read_ref,
    next_ref,
    grad_ref,
    atmosphere_next_ref,
    input_adj_ref,
    win_a,
    win_b,
    bands,
    sums,
    unit_0,
    rstd_0,
    slope_0,
    unit_1,
    rstd_1,
    before,
    active,
    out_rows,
    in_rows,
    in_cols,
    row_sems,
    col_sems,
    leaving,
    landed,
    swap_sems,
    flux_rows,
    coarse_rows,
    rows_out,
    parts_out,
    rows_in,
    parts_in,
    regrid_sems,
    mask_ref,
    atmosphere_ref,
    first_rows_out,
    first_parts_out,
    first_rows_in,
    first_parts_in,
    first_sems,
    flux_cells,
    taps_ref,
    embed_rows_ref,
    read_rows_ref,
):
    sec = lax.axis_index("sec") if linked else 0
    tile = lax.axis_index("tile") if linked else 0
    last_tile = GROUPS - 1 if linked else 0
    me = sec * GROUPS + tile
    side = (1 - sec) * GROUPS + tile
    windows = (win_a, win_b)

    if linked:
        barrier = pltpu.get_barrier_semaphore()

        def greet(i, carry):
            pl.semaphore_signal(
                barrier, inc=1, device_id=(me + i) % DEVICES, device_id_type=LOGICAL
            )
            return carry

        lax.fori_loop(1, DEVICES, greet, 0)

    zero_rows = jnp.zeros((REACH, WIDE, CELL), jnp.float32)

    @pl.when(tile == 0)
    def _():
        for w in windows:
            w[0:REACH] = zero_rows

    @pl.when(tile == last_tile)
    def _():
        for w in windows:
            w[REACH + ROWS :] = zero_rows

    if not linked:
        for w in windows:
            w[:, 0:EDGE] = jnp.zeros((14, EDGE, CELL), jnp.float32)
            w[:, WIDE - EDGE :] = jnp.zeros((14, EDGE, CELL), jnp.float32)
    for v in range(TAPS):
        bands[v, 0:CELL, CELL:] = jnp.zeros((CELL, CELL), jnp.bfloat16)
        bands[v, 7 * CELL :, :CELL] = jnp.zeros((CELL, CELL), jnp.bfloat16)


    def send_block(x, i):
        peer = lax.rem(me + i, DEVICES)
        remote(
            leaving.at[x, pl.ds(pl.multiple_of(peer * 8, 8), 8)],
            landed.at[x, pl.ds(pl.multiple_of(me * 8, 8), 8)],
            swap_sems.at[0, x],
            swap_sems.at[1, x],
            peer,
        ).start()

    def put_blocks(x, values):
        for j in range(6):
            leaving[x, pl.ds(j, DEVICES, stride=8), :] = values[:, j * CELL : (j + 1) * CELL]

        def send(i, carry):
            send_block(x, i)
            return carry

        lax.fori_loop(1, DEVICES, send, 0)
        mine = pl.ds(pl.multiple_of(me * 8, 8), 8)
        landed[x, mine, :] = leaving[x, mine, :]

    def take_blocks(x):
        source = landed
        if linked:
            every = landed.at[x, pl.ds(0, (DEVICES - 1) * 8)]
            pltpu.make_async_copy(every, every, swap_sems.at[1, x]).wait()
            pltpu.make_async_copy(every, every, swap_sems.at[0, x]).wait()
        else:
            source = leaving
        return jnp.concatenate(
            [source[x, pl.ds(j, DEVICES, stride=8), :] for j in range(6)], axis=1
        ).astype(jnp.bfloat16)

    def rounded(values):
        return values.astype(jnp.bfloat16).astype(jnp.float32)

    half_c = 3 * CELL

    def spectral():
        coefficient = dot32(forward_ref[...], take_blocks(0)).astype(jnp.bfloat16)
        real, imag = (coefficient[:, :half_c], coefficient[:, half_c:])
        mixed = jnp.concatenate(
            [
                dot32(real, mix_ref[0]) - dot32(imag, mix_ref[1]),
                dot32(imag, mix_ref[0]) + dot32(real, mix_ref[1]),
            ],
            axis=1,
        ).astype(jnp.bfloat16)
        put_blocks(1, rounded(dot32(inverse_ref[...], mixed)))

    def respond():
        returned = take_blocks(1)
        returned = jnp.concatenate([returned[:, :half_c], returned[:, half_c:]], axis=0)
        parts = []
        for j in range(3):
            cols = pl.ds(j * CELL, CELL)
            response = dot32(wave_ref[...], returned[:, j * CELL : (j + 1) * CELL])
            value, slope = gelu_pair(response)
            atmosphere_next_ref[:, cols] = (
                atmosphere_ref[:, cols].astype(jnp.float32) + value
            ).astype(jnp.bfloat16)
            response_adj = (slope * atmosphere_cot_ref[:, cols].astype(jnp.float32)).astype(
                jnp.bfloat16
            )
            parts.append(dot32(wave_t_ref[...], response_adj))
        put_blocks(
            2,
            rounded(
                jnp.concatenate([p[:DEVICES] for p in parts] + [p[DEVICES:] for p in parts], axis=1)
            ),
        )

    def dot_first(a, b):
        return lax.dot_general(
            a, b, (((0,), (0,)), ((), ())), preferred_element_type=jnp.float32
        )

    def spectral_back():
        mixed_adj = dot_first(inverse_ref[...], take_blocks(2)).astype(jnp.bfloat16)
        real, imag = (mixed_adj[:, :half_c], mixed_adj[:, half_c:])
        coefficient_adj = jnp.concatenate(
            [
                dot_t(real, mix_ref[0]) + dot_t(imag, mix_ref[1]),
                dot_t(imag, mix_ref[0]) - dot_t(real, mix_ref[1]),
            ],
            axis=1,
        ).astype(jnp.bfloat16)
        put_blocks(3, rounded(dot_first(forward_ref[...], coefficient_adj)))

    def absorb():
        spectrum_adj = take_blocks(3)
        spectrum_adj = jnp.concatenate([spectrum_adj[:, :half_c], spectrum_adj[:, half_c:]], axis=0)
        for j in range(3):
            cols = pl.ds(j * CELL, CELL)
            input_adj_ref[:, cols] = atmosphere_cot_ref[:, cols].astype(jnp.float32) + dot32(
                wave_ref[...], spectrum_adj[:, j * CELL : (j + 1) * CELL]
            )

    def row_copy(e, way, c, peer):
        x0 = pl.multiple_of(c * X, 16)
        return remote(
            out_rows.at[e, pl.ds(0 if way == 0 else ROWS - REACH, REACH), pl.ds(x0, X)],
            in_rows.at[e, way, :, pl.ds(x0, X)],
            row_sems.at[0, e, way, c],
            row_sems.at[1, e, way, c],
            peer,
        )

    def col_copy(e, edge, part, peer):
        source = windows[e % 2]
        first, size, place = ((0, ROWS, REACH), (0, REACH, REACH + ROWS), (ROWS - REACH, REACH, 0))[
            part
        ]
        return remote(
            source.at[
                pl.ds(REACH + first, size), pl.ds(EDGE if edge == 0 else WIDE - 2 * EDGE, EDGE)
            ],
            in_cols.at[e, edge, pl.ds(place, size)],
            col_sems.at[0, e, edge, part],
            col_sems.at[1, e, edge, part],
            peer,
        )

    def send_chunk(e, k, c):
        if not linked:
            return

        @pl.when(tile > 0)
        def _():
            row_copy(e, 0, c, me - 1).start()

        @pl.when(tile < last_tile)
        def _():
            row_copy(e, 1, c, me + 1).start()

        for edge in range(2):

            @pl.when(k == edge)
            def _():
                col_copy(e, edge, 0, side).start()

                @pl.when(tile > 0)
                def _():
                    col_copy(e, edge, 1, side - 1).start()

                @pl.when(tile < last_tile)
                def _():
                    col_copy(e, edge, 2, side + 1).start()

    def take_rows(e, c):
        x0 = pl.multiple_of(c * X, 16)
        window = windows[e % 2]

        @pl.when(tile > 0)
        def _():
            row_copy(e, 1, c, me - 1).wait_recv()
            window[0:REACH, pl.ds(EDGE + x0, X), :] = in_rows[e, 1, :, pl.ds(x0, X), :].astype(
                jnp.float32
            )

        @pl.when(tile < last_tile)
        def _():
            row_copy(e, 0, c, me + 1).wait_recv()
            window[REACH + ROWS :, pl.ds(EDGE + x0, X), :] = in_rows[
                e, 0, :, pl.ds(x0, X), :
            ].astype(jnp.float32)

    def take_cols(e, edge):
        window = windows[e % 2]
        at = pl.ds(0 if edge == 1 else WIDE - EDGE, EDGE)
        col_copy(e, edge, 0, side).wait_recv()
        window[pl.ds(REACH, ROWS), at, :] = in_cols[e, edge, pl.ds(REACH, ROWS)]

        @pl.when(tile > 0)
        def _():
            col_copy(e, edge, 2, side - 1).wait_recv()
            window[pl.ds(0, REACH), at, :] = in_cols[e, edge, pl.ds(0, REACH)]

        @pl.when(tile < last_tile)
        def _():
            col_copy(e, edge, 1, side + 1).wait_recv()
            window[pl.ds(REACH + ROWS, REACH), at, :] = in_cols[
                e, edge, pl.ds(REACH + ROWS, REACH)
            ]

    def take_halo(e, k):
        if not linked:
            return

        @pl.when(k == 0)
        def _():
            take_rows(e, 0)
            take_rows(e, 1)
            take_cols(e, 1)

        @pl.when(k == 1)
        def _():
            take_rows(e, CHUNKS - 1)
            take_rows(e, CHUNKS - 2)
            take_cols(e, 0)

        @pl.when(k == 2)
        def _():
            take_rows(e, CHUNKS // 2)

    def sent(e):
        if not linked:
            return

        def one(c, carry):
            @pl.when(tile > 0)
            def _():
                row_copy(e, 0, c, me - 1).wait_send()

            @pl.when(tile < last_tile)
            def _():
                row_copy(e, 1, c, me + 1).wait_send()

            return carry

        lax.fori_loop(0, CHUNKS, one, 0)
        for edge in range(2):
            col_copy(e, edge, 0, side).wait_send()

            @pl.when(tile > 0)
            def _():
                col_copy(e, edge, 1, side - 1).wait_send()

            @pl.when(tile < last_tile)
            def _():
                col_copy(e, edge, 2, side + 1).wait_send()

    def chunk_of(k):
        return jnp.where(k % 2 == 0, k // 2, CHUNKS - 1 - k // 2)

    def keep(e, y, x0, value):
        windows[e % 2][y + REACH, pl.ds(EDGE + x0, X), :] = value.astype(jnp.float32)
        if linked:
            out_rows[e, y, pl.ds(x0, X), :] = value

    half_cells = ROWS // 2 * X

    def origin(k):
        return pl.multiple_of(chunk_of(k) * X, 16)

    def conv(e, k):
        layer, flipped = ((0, False), (1, False), (1, True), (0, True))[e]
        convolve(windows[e % 2], bands, sums, origin(k), taps_ref, layer, flipped)

    def halves(one):
        def half(q, inner):
            one(q, pl.ds(pl.multiple_of(q * half_cells, 16), half_cells))
            return inner

        lax.fori_loop(0, 2, half, 0)

    def half_of(q):
        return sums[:, pl.ds(pl.multiple_of(q * CELL, CELL), CELL)]

    def row_part(values, p):
        return values[p * X : (p + 1) * X]

    def stacked(read):
        return jnp.concatenate([read(p) for p in range(ROWS // 2)], axis=0)

    def forward_stage(e, layer, keep_norm, keep_slope, finish):
        def normalize(k):
            def one(q, at):
                unit, rstd = normalized(half_of(q))
                keep_norm(k, at, unit, rstd)
                dense = (unit * gain_ref[layer : layer + 1, :]).astype(jnp.bfloat16)
                before[at, :] = dot32(dense, expand_ref[layer])

            halves(one)

        def activate(k, y):
            at = pl.ds(pl.multiple_of(y * X, 16), X)
            value, slope = gelu_pair(before[at, :])
            active[at, :] = value.astype(jnp.bfloat16)
            keep_slope(k, at, slope)

        def close(k):
            def one(q, at):
                finish(k, q, at, dot32(active[at, :], project_ref[layer]))

            halves(one)
            send_chunk(e + 1, k, chunk_of(k))

        def chunk(k, carry):
            take_halo(e, k)
            conv(e, k)
            normalize(k)

            def piece(y, inner):
                activate(k, y)
                return inner

            lax.fori_loop(0, ROWS, piece, 0)
            close(k)
            return carry

        lax.fori_loop(0, CHUNKS, chunk, 0)
        sent(e)

    def backward_stage(e, one, after=None):
        def chunk(k, carry):
            take_halo(e, k)
            conv(e, k)
            halves(lambda q, at: one(k, q, at))
            if after is not None:
                after(k)
            if e < 3:
                send_chunk(e + 1, k, chunk_of(k))
            return carry

        lax.fori_loop(0, CHUNKS, chunk, 0)
        sent(e)

    half = ALON // 2
    row_number = lax.broadcasted_iota(jnp.int32, (ROWS, CELL), 0)
    land = land_ref[...].astype(jnp.float32).astype(jnp.bfloat16)

    def picked(o):
        return jnp.where(row_number == o, 1.0, 0.0).astype(jnp.bfloat16)

    def spread_mask(o, carry):
        mask_ref[o] = dot_first(land, picked(o)).astype(jnp.bfloat16)
        return carry

    lax.fori_loop(0, ROWS, spread_mask, 0)

    for layer in range(2):
        for u in range(TAPS):
            taps_ref[layer, u * TAPS : (u + 1) * TAPS, :] = kernel_ref[layer, u].astype(jnp.float32)

    def numbers(width):
        return [lax.broadcasted_iota(jnp.int32, (8, width), axis) for axis in range(2)]

    read_row = jnp.where(row_number == 0, surface_read_ref[...], 0.0).astype(jnp.bfloat16)
    for y in range(ROWS):
        at = pl.ds(y * CELL, CELL)
        row, column = numbers(ROWS)
        pick = jnp.where((row == 0) & (column == y), 1.0, 0.0).astype(jnp.bfloat16)
        read_rows_ref[at, :] = dot_first(read_row, pick).astype(jnp.bfloat16)
        row, column = numbers(ROWS * 8)
        pick = jnp.where(column == row + y * 8, 1.0, 0.0).astype(jnp.bfloat16)
        embed_rows_ref[at, :] = dot_first(flux_embed_ref[...], pick).astype(jnp.bfloat16)

    lanes = jnp.concatenate([mask_ref[y] * state_ref[y] for y in range(ROWS)], axis=1)
    high, rest = split(dot32(lanes, read_rows_ref[...]))
    coarse = 0.25 * (dot_first(high, group_ref[...]) + dot_first(rest, group_ref[...]))
    for slot in range(SLOTS):
        total = to_atmosphere_ref[slot, 0] * coarse[0:1]
        for o in range(1, ROWS):
            total = total + to_atmosphere_ref[slot, o] * coarse[o : o + 1]
        first_parts_out[slot] = total
    flux = dot_t(flux_read_ref[...], raw_ref[...])
    first_rows_out[...] = jnp.zeros((2, 8, LANES), jnp.float32)
    first_rows_out[0, :, 0:half] = flux[:, 0:half]
    first_rows_out[1, :, 0:half] = flux[:, half:]
    pl.semaphore_wait(pltpu.get_barrier_semaphore(), DEVICES - 1)
    send_rows(first_rows_out, first_parts_out, first_rows_in, first_parts_in, first_sems)
    spread_taps(bands, taps_ref, 0, False)
    wait_rows(first_rows_out, first_parts_out, first_rows_in, first_parts_in, first_sems)

    for o in range(ROWS):
        total = to_ocean_ref[0, o] * first_rows_in[0]
        for slot in range(1, SLOTS):
            total = total + to_ocean_ref[slot, o] * first_rows_in[slot]
        parts_out[o] = total
    high, rest = split(jnp.concatenate([parts_out[o] for o in range(ROWS)], axis=0))
    flux_cells[0 : ROWS * 8, :] = dot_t(high, group_ref[...])
    flux_cells[ROWS * 8 :, :] = dot_t(rest, group_ref[...])
    flux_embed_twice = jnp.concatenate([flux_embed_ref[...].astype(jnp.float32)] * 2, axis=0)
    flux_embed_twice = flux_embed_twice.astype(jnp.bfloat16)

    def force(o, carry):
        at = pl.multiple_of(o * 8, 8)
        cells = jnp.concatenate(
            [flux_cells[pl.ds(at, 8), :], flux_cells[pl.ds(at + ROWS * 8, 8), :]], axis=0
        ).astype(jnp.bfloat16)
        forcing = dot_first(cells, flux_embed_twice)
        start = (
            state_ref[o].astype(jnp.float32) + mask_ref[o].astype(jnp.float32) * forcing
        ).astype(jnp.bfloat16)
        win_a[o + REACH, EDGE : EDGE + CHUNKS * X, :] = start.astype(jnp.float32)
        out_rows[0, o] = start
        return carry

    lax.fori_loop(0, ROWS, force, 0)

    def first(k, carry):
        send_chunk(0, k, chunk_of(k))
        return carry

    lax.fori_loop(0, CHUNKS, first, 0)

    embed_high, embed_rest = split(surface_embed_ref[...])
    for h in range(2):
        total = first_parts_in[h]
        for k in range(1, 4):
            total = total + first_parts_in[2 * k + h]
        high, rest = split(total)
        blank = jnp.zeros((5, LANES), jnp.float32)
        left = jnp.concatenate(
            [high.astype(jnp.float32), high.astype(jnp.float32), rest.astype(jnp.float32), blank],
            axis=0,
        ).astype(jnp.bfloat16)
        blank = jnp.zeros((5, half_c), jnp.float32)
        right = jnp.concatenate(
            [
                embed_high.astype(jnp.float32),
                embed_rest.astype(jnp.float32),
                embed_high.astype(jnp.float32),
                blank,
            ],
            axis=0,
        ).astype(jnp.bfloat16)
        input_adj_ref[pl.ds(h * half, half), :] = dot_first(left, right)[:half]
    atmosphere_ref[...] = (raw_ref[...].astype(jnp.float32) + input_adj_ref[...]).astype(
        jnp.bfloat16
    )
    spectrum = dot32(wave_t_ref[...], atmosphere_ref[...])
    put_blocks(0, rounded(jnp.concatenate([spectrum[:DEVICES], spectrum[DEVICES:]], axis=1)))

    def mask_of(y, x0):
        return mask_ref[y, pl.ds(x0, X), :].astype(jnp.float32)

    def own(e, y, x0):
        return windows[e % 2][y + REACH, pl.ds(EDGE + x0, X), :]

    def keep_norm_0(k, at, unit, rstd):
        c = chunk_of(k)
        unit_0[c, at, :] = unit
        rstd_0[c, at, :] = jnp.broadcast_to(rstd, unit.shape)

    def keep_slope_0(k, at, slope):
        slope_0[chunk_of(k), at, :] = slope.astype(jnp.bfloat16)

    def finish_0(k, q, at, update):
        x0 = origin(k)
        for p in range(ROWS // 2):
            y = 2 * p + q
            new = own(0, y, x0) + mask_of(y, x0) * row_part(update, p)
            keep(1, y, x0, new.astype(jnp.bfloat16))

    forward_stage(0, 0, keep_norm_0, keep_slope_0, finish_0)
    spectral()
    spread_taps(bands, taps_ref, 1, False)

    def adjoint(e, k, q, at, masked, slope, unit, rstd, layer):
        x0 = origin(k)
        active[at, :] = (slope * dot_t(masked, project_ref[layer])).astype(jnp.bfloat16)
        scaled = dot_t(active[at, :], expand_ref[layer]) * gain_ref[layer : layer + 1, :]
        inner = jnp.mean(scaled * unit, axis=-1, keepdims=True)
        result = rstd * (scaled - jnp.mean(scaled, axis=-1, keepdims=True) - unit * inner)
        for p in range(ROWS // 2):
            keep(e, 2 * p + q, x0, row_part(result, p).astype(jnp.bfloat16))

    def cot_of(y, x0):
        return cot_ref[y, pl.ds(x0, X), :].astype(jnp.float32)

    def keep_norm_1(k, at, unit, rstd):
        unit_1[at, :] = unit
        rstd_1[at, :] = jnp.broadcast_to(rstd, unit.shape)

    def keep_slope_1(k, at, slope):
        before[at, :] = slope

    def finish_1(k, q, at, update):
        x0 = origin(k)
        for p in range(ROWS // 2):
            y = 2 * p + q
            new = own(1, y, x0) + mask_of(y, x0) * row_part(update, p)
            next_ref[y, pl.ds(x0, X), :] = new.astype(jnp.bfloat16)
        masked = stacked(lambda p: mask_of(2 * p + q, x0) * cot_of(2 * p + q, x0))
        adjoint(
            2, k, q, at, masked.astype(jnp.bfloat16), before[at, :], unit_1[at, :], rstd_1[at, :], 1
        )

    forward_stage(1, 1, keep_norm_1, keep_slope_1, finish_1)
    respond()
    spread_taps(bands, taps_ref, 1, True)

    def backward_0(k, q, at):
        c, x0 = (chunk_of(k), origin(k))
        hid = half_of(q)
        parts = []
        for p in range(ROWS // 2):
            y = 2 * p + q
            cot = cot_of(y, x0) + row_part(hid, p)
            grad_ref[y, pl.ds(x0, X), :] = cot
            parts.append(mask_of(y, x0) * cot)
        masked = jnp.concatenate(parts, axis=0).astype(jnp.bfloat16)
        slope = slope_0[c, at, :].astype(jnp.float32)
        adjoint(3, k, q, at, masked, slope, unit_0[c, at, :], rstd_0[c, at, :], 0)

    backward_stage(2, backward_0)
    spectral_back()
    spread_taps(bands, taps_ref, 0, True)

    def last(k, q, at):
        x0 = origin(k)
        hid = half_of(q)
        for p in range(ROWS // 2):
            y = 2 * p + q
            grad_ref[y, pl.ds(x0, X), :] = grad_ref[y, pl.ds(x0, X), :] + row_part(hid, p)

    def gather_flux(k):
        x0 = origin(k)
        lanes = jnp.concatenate(
            [mask_of(y, x0) * grad_ref[y, pl.ds(x0, X), :] for y in range(ROWS)], axis=1
        )
        high, rest = split(lanes)
        flux_rows[pl.ds(x0, X), :] = dot32(high, embed_rows_ref[...]) + dot32(
            rest, embed_rows_ref[...]
        )

    backward_stage(3, last, gather_flux)
    absorb()
    high, rest = split(flux_rows[...])
    flux_by_row = dot_first(high, group_ref[...]) + dot_first(rest, group_ref[...])
    for slot in range(SLOTS):
        total = to_ocean_ref[slot, 0] * flux_by_row[0:8]
        for o in range(1, ROWS):
            total = total + to_ocean_ref[slot, o] * flux_by_row[8 * o : 8 * o + 8]
        parts_out[slot] = total
    embed_high, embed_rest = split(jnp.broadcast_to(surface_embed_ref[...], (8, half_c)))
    rows_out[...] = jnp.zeros((2, 1, LANES), jnp.float32)
    for h in range(2):
        high, rest = split(input_adj_ref[pl.ds(h * half, half), :])
        row = dot_t(embed_high, high) + dot_t(embed_rest, high) + dot_t(embed_high, rest)
        rows_out[h, :, 0:half] = row[0:1]
    send_rows(rows_out, parts_out, rows_in, parts_in, regrid_sems)
    wait_rows(rows_out, parts_out, rows_in, parts_in, regrid_sems)
    for o in range(ROWS):
        total = to_atmosphere_ref[0, o] * rows_in[0]
        for slot in range(1, SLOTS):
            total = total + to_atmosphere_ref[slot, o] * rows_in[slot]
        coarse_rows[o : o + 1, :] = total
    coarse_high, coarse_rest = split(coarse_rows[...])
    read = surface_read_ref[...] * 0.25
    def widen(o, carry):
        pick = picked(o)
        spread = dot32(group_ref[...], dot_first(coarse_high, pick).astype(jnp.bfloat16)) + dot32(
            group_ref[...], dot_first(coarse_rest, pick).astype(jnp.bfloat16)
        )
        grad_ref[o] = grad_ref[o] + mask_ref[o].astype(jnp.float32) * spread * read
        return carry

    lax.fori_loop(0, ROWS, widen, 0)
    flux_read_twice = jnp.concatenate([flux_read_ref[...], flux_read_ref[...]], axis=0)
    for h in range(2):
        total = parts_in[h]
        for k in range(1, 4):
            total = total + parts_in[2 * k + h]
        high, rest = split(total)
        from_flux = dot_first(
            jnp.concatenate([high.astype(jnp.float32), rest.astype(jnp.float32)], axis=0).astype(
                jnp.bfloat16
            ),
            flux_read_twice,
        )
        at = pl.ds(h * half, half)
        input_adj_ref[at, :] = input_adj_ref[at, :] + from_flux[:half]


def ocean(*operands, linked=True):
    vmem = pl.BlockSpec(memory_space=pltpu.VMEM)
    smem = pl.BlockSpec(memory_space=pltpu.SMEM)
    whole = (ROWS, CHUNKS * X, CELL)
    f32, bf16 = (jnp.float32, jnp.bfloat16)
    return pl.pallas_call(
        functools.partial(ocean_kernel, linked),
        out_shape=(
            jax.ShapeDtypeStruct(whole, bf16),
            jax.ShapeDtypeStruct(whole, f32),
            jax.ShapeDtypeStruct((ALON, 3 * CELL), bf16),
            jax.ShapeDtypeStruct((ALON, 3 * CELL), f32),
        ),
        in_specs=[vmem] * 16 + [smem] * 2 + [vmem] * 3,
        out_specs=(vmem,) * 4,
        scratch_shapes=[
            pltpu.VMEM((ROWS + 2 * REACH, WIDE, CELL), f32),
            pltpu.VMEM((ROWS + 2 * REACH, WIDE, CELL), f32),
            pltpu.VMEM((TAPS, 8 * CELL, 2 * CELL), bf16),
            pltpu.VMEM((ROWS // 2 * X, 2 * CELL), f32),
            pltpu.VMEM((CHUNKS, ROWS * X, CELL), f32),
            pltpu.VMEM((CHUNKS, ROWS * X, CELL), f32),
            pltpu.VMEM((CHUNKS, ROWS * X, 4 * CELL), bf16),
            pltpu.VMEM((ROWS * X, CELL), f32),
            pltpu.VMEM((ROWS * X, CELL), f32),
            pltpu.VMEM((ROWS * X, 4 * CELL), f32),
            pltpu.VMEM((ROWS * X, 4 * CELL), bf16),
            pltpu.VMEM((4, ROWS, CHUNKS * X, CELL), bf16),
            pltpu.VMEM((4, 2, REACH, CHUNKS * X, CELL), bf16),
            pltpu.VMEM((4, 2, ROWS + 2 * REACH, EDGE, CELL), f32),
            pltpu.SemaphoreType.DMA((2, 4, 2, CHUNKS)),
            pltpu.SemaphoreType.DMA((2, 4, 2, 3)),
            pltpu.VMEM((4, DEVICES * 8, CELL), f32),
            pltpu.VMEM((4, DEVICES * 8, CELL), f32),
            pltpu.SemaphoreType.DMA((2, 4)),
            pltpu.VMEM((CHUNKS * X, ROWS * SLOTS), f32),
            pltpu.VMEM((ROWS, LANES), f32),
            pltpu.VMEM((2, 1, LANES), f32),
            pltpu.VMEM((SLOTS, 8, LANES), f32),
            pltpu.VMEM((SLOTS, 1, LANES), f32),
            pltpu.VMEM((SLOTS, 8, LANES), f32),
            pltpu.SemaphoreType.DMA((4, SLOTS)),
            pltpu.VMEM(whole, bf16),
            pltpu.VMEM((ALON, 3 * CELL), bf16),
            pltpu.VMEM((2, 8, LANES), f32),
            pltpu.VMEM((SLOTS, 1, LANES), f32),
            pltpu.VMEM((SLOTS, 8, LANES), f32),
            pltpu.VMEM((SLOTS, 1, LANES), f32),
            pltpu.SemaphoreType.DMA((4, SLOTS)),
            pltpu.VMEM((2 * ROWS * 8, CHUNKS * X), f32),
            pltpu.VMEM((2, TAPS * TAPS, CELL), f32),
            pltpu.VMEM((ROWS * CELL, ROWS * 8), bf16),
            pltpu.VMEM((ROWS * CELL, ROWS), bf16),
        ],
        compiler_params=pltpu.CompilerParams(
            collective_id=6 if linked else None, has_side_effects=linked, vmem_limit_bytes=67000000
        ),
        name="ocean",
    )(*operands)


def wave_table():
    place = np.arange(ALON, dtype=np.int32)[:, None] * np.arange(DEVICES, dtype=np.int32)[None, :]
    phase = (place % ALON).astype(np.float32) * np.float32(2.0 * np.pi / ALON)
    both = np.concatenate([np.cos(phase), -np.sin(phase)], axis=1)
    return (both * np.sqrt(np.float32(2.0 / ALON))).astype(jnp.bfloat16)


def slot_weights(bands_row, blocks, group):
    slot = bands_row[:, None] - (2 * group - 2)
    onehot = (slot == jnp.arange(SLOTS, dtype=jnp.int32)[None, :]).astype(jnp.float32)
    return jnp.sum(onehot[:, :, None] * blocks[:, None, :], axis=0)


def per_device(
    atmosphere,
    ocean_state,
    land_mask,
    crossing_bands,
    ocean_regrid,
    atmosphere_regrid,
    surface_read,
    surface_embed,
    flux_read,
    flux_embed,
    legendre_forward,
    legendre_inverse,
    spectral_mix,
    conv_kernel,
    norm_gain,
    expand_weight,
    project_weight,
    atmosphere_cotangent,
    ocean_cotangent,
):
    lon_count = atmosphere.shape[1]
    ocean_lon = ocean_state.shape[1]
    half = lon_count // lax.axis_size("sec")
    ratio = ocean_lon // half
    group = lax.axis_index("tile")
    to_ocean = slot_weights(crossing_bands[0], ocean_regrid[0, :, :, 0], group)
    to_atmosphere = slot_weights(crossing_bands[0], atmosphere_regrid[0, :, 0, :], group)
    table = wave_table()
    grouping = np.arange(ocean_lon)[:, None] // ratio == np.arange(LANES)[None, :]
    grouping = grouping.astype(jnp.bfloat16)
    state, ocean_grad, atmosphere_next, atmosphere_grad = ocean(
        ocean_state,
        land_mask,
        ocean_cotangent,
        conv_kernel,
        norm_gain,
        expand_weight,
        project_weight,
        atmosphere[0],
        atmosphere_cotangent[0],
        jnp.asarray(table),
        jnp.asarray(np.ascontiguousarray(table.T)),
        legendre_forward[0],
        legendre_inverse[0],
        spectral_mix,
        flux_embed,
        jnp.asarray(grouping),
        to_ocean,
        to_atmosphere,
        surface_embed[None, :],
        surface_read.astype(jnp.float32)[None, :],
        flux_read.T,
    )
    return (atmosphere_next[None], state, atmosphere_grad[None], ocean_grad)


def solution(mesh):
    placed = (
        P(SEC_TILE, None, None),
        P(TILE, "sec", None),
        P(TILE, "sec"),
        P(TILE, None),
        P(TILE, None, None, None),
        P(TILE, None, None, None),
        P(),
        P(),
        P(),
        P(),
        P(SEC_TILE, None, None),
        P(SEC_TILE, None, None),
        P(),
        P(),
        P(),
        P(),
        P(),
        P(SEC_TILE, None, None),
        P(TILE, "sec", None),
    )
    return jax.shard_map(
        per_device,
        mesh=mesh,
        in_specs=placed,
        out_specs=(
            P(SEC_TILE, None, None),
            P(TILE, "sec", None),
            P(SEC_TILE, None, None),
            P(TILE, "sec", None),
        ),
        check_vma=False,
    )
```
